8 devices in a mesh: heads: 1 (over z), cpo: 2 (over y), cp: 4 (over x, core).
Axes of the slice: x: 2, y: 2, z: 1, core: 2. Of those that a mesh axis runs over, the one named last changes fastest.
Arguments:
- queries: bfloat16 [24, 64, 128, 128], P(None, ('cpo', 'cp'), 'heads')
- attn_out: bfloat16 [24, 64, 128, 128], P(None, ('cpo', 'cp'), 'heads')
- grad_out: bfloat16 [24, 64, 128, 128], P(None, ('cpo', 'cp'), 'heads')
- log_sum_exp: float32 [24, 64, 128], P(None, ('cpo', 'cp'), 'heads')
- key_cache: bfloat16 [9728, 8, 128], P(('cpo', 'cp'), 'heads')
- value_cache: bfloat16 [9728, 8, 128], P(('cpo', 'cp'), 'heads')
Outputs:
- output 1: bfloat16 [24, 64, 128, 128], P(None, ('cpo', 'cp'), 'heads')
- output 2: float32 [9728, 8, 128], P(('cpo', 'cp'), 'heads')
- output 3: float32 [9728, 8, 128], P(('cpo', 'cp'), 'heads')
All inputs are finite; a program needn't handle non-finite values.
Results may differ from the reference program's by a relative error of at most 0.001.
Values are sent between devices in bfloat16 or wider.
A program may use at most 1 GiB of HBM per device.

```python
import jax
import jax.numpy as jnp
from jax import lax

N_SLICES = 24
SLICE_LEN = 64
PREFIX_BASE = 8192
Q_HEADS = 128
KV_HEADS = 8
HEAD_DIM = 128
ROW_BLOCK = 8


def slice_lse(queries_f, keys_f, slice_idx):
    group_size = Q_HEADS // KV_HEADS
    softmax_scale = HEAD_DIM ** -0.5
    limit_len = PREFIX_BASE + (slice_idx + 1) * SLICE_LEN
    key_part = keys_f[:limit_len]
    key_pos = jnp.arange(limit_len)
    n_blocks = SLICE_LEN // ROW_BLOCK
    q_blocks = queries_f.reshape(n_blocks, ROW_BLOCK, KV_HEADS, group_size, HEAD_DIM)
    row_starts = PREFIX_BASE + slice_idx * SLICE_LEN + ROW_BLOCK * jnp.arange(n_blocks)

    def one_block(operand):
        q_blk, row_start = operand
        scores = jnp.einsum('rhgd,khd->rhgk', q_blk, key_part) * softmax_scale
        q_pos = row_start + jnp.arange(ROW_BLOCK)
        visible = (key_pos[None, :] <= q_pos[:, None])[:, None, None, :]
        scores = jnp.where(visible, scores, -jnp.inf)
        return jax.nn.logsumexp(scores, axis=-1).reshape(ROW_BLOCK, Q_HEADS)

    return lax.map(one_block, (q_blocks, row_starts)).reshape(SLICE_LEN, Q_HEADS)


def setup_inputs(seed: int = 0, part: int = 0) -> dict:
    base_key = jax.random.fold_in(jax.random.key(seed), part)
    key_q, key_k, key_v, key_o, key_g = jax.random.split(base_key, 5)
    total_len = PREFIX_BASE + N_SLICES * SLICE_LEN
    row_shape = (N_SLICES, SLICE_LEN, Q_HEADS, HEAD_DIM)
    cache_shape = (total_len, KV_HEADS, HEAD_DIM)
    queries = jax.random.normal(key_q, row_shape, jnp.float32).astype(jnp.bfloat16)
    key_cache = jax.random.normal(key_k, cache_shape, jnp.float32).astype(jnp.bfloat16)
    value_cache = jax.random.normal(key_v, cache_shape, jnp.float32).astype(jnp.bfloat16)
    out_val = jax.random.normal(key_o, row_shape, jnp.float32)
    grad_out = (0.1 * out_val + jax.random.normal(key_g, row_shape, jnp.float32)).astype(jnp.bfloat16)
    attn_out = out_val.astype(jnp.bfloat16)
    queries_f = queries.astype(jnp.float32)
    keys_f = key_cache.astype(jnp.float32)
    log_sum_exp = jnp.stack([slice_lse(queries_f[slice_idx], keys_f, slice_idx) for slice_idx in range(N_SLICES)])
    return {'queries': queries, 'attn_out': attn_out, 'grad_out': grad_out, 'log_sum_exp': log_sum_exp, 'key_cache': key_cache, 'value_cache': value_cache}


def reference(queries, attn_out, grad_out, log_sum_exp, key_cache, value_cache):
    group_size = Q_HEADS // KV_HEADS
    softmax_scale = HEAD_DIM ** -0.5
    total_len = PREFIX_BASE + N_SLICES * SLICE_LEN
    n_blocks = SLICE_LEN // ROW_BLOCK
    blk_shape = (n_blocks, ROW_BLOCK, KV_HEADS, group_size)
    keys_f = key_cache.astype(jnp.float32)
    values_f = value_cache.astype(jnp.float32)
    row_delta = jnp.sum(grad_out.astype(jnp.float32) * attn_out.astype(jnp.float32), axis=-1)
    grad_key = jnp.zeros((total_len, KV_HEADS, HEAD_DIM), jnp.float32)
    grad_value = jnp.zeros((total_len, KV_HEADS, HEAD_DIM), jnp.float32)
    dq_list = []
    for slice_idx in reversed(range(N_SLICES)):
        limit_len = PREFIX_BASE + (slice_idx + 1) * SLICE_LEN
        key_part = keys_f[:limit_len]
        value_part = values_f[:limit_len]
        key_pos = jnp.arange(limit_len)
        operands = (
            queries[slice_idx].astype(jnp.float32).reshape(blk_shape + (HEAD_DIM,)),
            grad_out[slice_idx].astype(jnp.float32).reshape(blk_shape + (HEAD_DIM,)),
            log_sum_exp[slice_idx].reshape(blk_shape),
            row_delta[slice_idx].reshape(blk_shape),
            PREFIX_BASE + slice_idx * SLICE_LEN + ROW_BLOCK * jnp.arange(n_blocks),
        )

        def one_block(carry_acc, operand):
            key_acc, value_acc = carry_acc
            q_blk, g_blk, lse_blk, delta_blk, row_start = operand
            scores = jnp.einsum('rhgd,khd->rhgk', q_blk, key_part) * softmax_scale
            q_pos = row_start + jnp.arange(ROW_BLOCK)
            visible = (key_pos[None, :] <= q_pos[:, None])[:, None, None, :]
            attn_prob = jnp.where(visible, jnp.exp(scores - lse_blk[..., None]), 0.0)
            prob_bf = attn_prob.astype(jnp.bfloat16).astype(jnp.float32)
            value_acc = value_acc + jnp.einsum('rhgk,rhgd->khd', prob_bf, g_blk)
            grad_prob = jnp.einsum('rhgd,khd->rhgk', g_blk, value_part)
            grad_scores = attn_prob * (grad_prob - delta_blk[..., None])
            grad_scores = grad_scores.astype(jnp.bfloat16).astype(jnp.float32)
            dq_blk = jnp.einsum('rhgk,khd->rhgd', grad_scores, key_part) * softmax_scale
            key_acc = key_acc + softmax_scale * jnp.einsum('rhgk,rhgd->khd', grad_scores, q_blk)
            return (key_acc, value_acc), dq_blk.astype(jnp.bfloat16)

        start_acc = (grad_key[:limit_len], grad_value[:limit_len])
        (key_acc, value_acc), dq_blocks = lax.scan(one_block, start_acc, operands)
        grad_key = lax.dynamic_update_slice(grad_key, key_acc, (0, 0, 0))
        grad_value = lax.dynamic_update_slice(grad_value, value_acc, (0, 0, 0))
        dq_list.append(dq_blocks.reshape(SLICE_LEN, Q_HEADS, HEAD_DIM))
    grad_query = jnp.stack(dq_list[::-1])
    return grad_query, grad_key, grad_value
```

```python
import functools
import math

import jax
import jax.numpy as jnp
from jax import lax
from jax.experimental import pallas as pl
from jax.experimental.pallas import tpu as pltpu
from jax.sharding import PartitionSpec as P

CP_AXES = ('cpo', 'cp')
MESH = pl.DeviceIdType.MESH
BF16 = jnp.bfloat16
F32 = jnp.float32

N_DEV = 8
N_SLICES = 24
ROWS_DEV = 8
GROUP = 16
DIM = 128
KEYS = 9728
KEYS_DEV = KEYS // N_DEV
PREFIX = 8192
N_GRP = 3
RB = 1024
CB = 512
NKB = KEYS // CB
CHUNK = 64
SCALE = DIM ** -0.5
EXP_SCALE = SCALE * math.log2(math.e)

PASS_1, PASS_2, PASS_3, PASS_B, N_OUTER = 19, 25, 31, 40, 58


def dg(a, b, ca, cb):
    return lax.dot_general(a, b, (((ca,), (cb,)), ((), ())), preferred_element_type=F32)


def quo(a, b):
    return lax.div(a, jnp.int32(b))


def rem(a, b):
    return lax.rem(a, jnp.int32(b))


def pick(cond, a, b):
    return jnp.where(cond, jnp.int32(a), jnp.int32(b))


def xor3(a, b):
    out = jnp.int32(0)
    for bit in (1, 2, 4):
        out = out + bit * rem(rem(quo(a, bit), 2) + rem(quo(b, bit), 2), 2)
    return out


def kernel(q_h, do_h, st_h, k_h, v_h, dq_o, dk_o, dv_o,
           q_v, do_v, qt_v, dot_v, st_v, kn_v, v_v, kt_v, dqt, dkt, dvt, p0, d0, p1, d1, x_v, okv, odq,
           rows_ss, keys_ss, rows_rs, keys_rs, kv_ss, kv_rs, dq_ss, dq_rs):
    me = lax.axis_index('cpo') * 4 + lax.axis_index('cp')
    chip = quo(me, 2)
    first_kb = 5 * chip

    def dev(e):
        return {'cpo': quo(e, 4), 'cp': rem(e, 4)}

    barrier = pltpu.get_barrier_semaphore()
    for m in range(1, N_DEV):
        pl.semaphore_signal(barrier, inc=1, device_id=dev(xor3(me, jnp.int32(m))), device_id_type=MESH)
    pl.semaphore_wait(barrier, N_DEV - 1)

    def row_copies(m, g):
        e = xor3(me, jnp.int32(m))
        heads = pl.ds(pl.multiple_of(e * GROUP, GROUP), GROUP)
        pairs = ((st_h.at[e, g], st_v.at[m, g], 2),
                 (q_h.at[pl.ds(8 * g, 8), :, heads, :], q_v.at[m, g], 0),
                 (do_h.at[pl.ds(8 * g, 8), :, heads, :], do_v.at[m, g], 1))
        for src, dst, t in pairs:
            if m == 0:
                yield pltpu.make_async_copy(src, dst, rows_rs.at[m, g, t])
            else:
                yield pltpu.make_async_remote_copy(src, dst, rows_ss.at[m, g, t], rows_rs.at[m, g, t],
                                                   device_id=dev(e), device_id_type=MESH)

    def key_copies(e, m, local=False):
        rows = pl.ds(pl.multiple_of(me * KEYS_DEV, CHUNK), KEYS_DEV)
        for src, dst, t in ((k_h.at[e], kn_v.at[rows, :], 0), (v_h.at[e], v_v.at[rows, :], 1)):
            if local:
                yield pltpu.make_async_copy(src, dst, keys_rs.at[m, t])
            else:
                yield pltpu.make_async_remote_copy(src, dst, keys_ss.at[m, t], keys_rs.at[m, t],
                                                   device_id=dev(e), device_id_type=MESH)

    for c in key_copies(me, jnp.int32(0), local=True):
        c.start()
    for c in key_copies(xor3(me, jnp.int32(1)), jnp.int32(1)):
        c.start()
    for g in range(N_GRP):
        for m in (0, 1):
            for c in row_copies(m, g):
                c.start()
    for back in (1, 2, 3):
        for core in (0, 1):
            e = 2 * rem(chip + 4 - back, 4) + core
            for c in key_copies(e, xor3(me, e)):
                c.start()
    for ms in ((2, 3, 4, 5), (6, 7)):
        for g in range(N_GRP):
            for m in ms:
                for c in row_copies(m, g):
                    c.start()

    def zero_keys(i, c):
        dkt[i] = jnp.zeros((DIM, CB), F32)
        dvt[i] = jnp.zeros((DIM, CB), F32)
        return c
    lax.fori_loop(0, NKB, zero_keys, 0)

    def zero_rows(i, c):
        dqt[i] = jnp.zeros((DIM, RB), F32)
        return c
    lax.fori_loop(0, N_DEV * N_GRP, zero_rows, 0)
    p1[...] = jnp.zeros((RB, CB), BF16)
    d1[...] = jnp.zeros((RB, CB), BF16)
    x_v[...] = (lax.broadcasted_iota(jnp.int32, (DIM, CB), 1)
                - lax.broadcasted_iota(jnp.int32, (DIM, CB), 0) // GROUP)

    def tile(kb, m, g, kb_p, rg_p, p_ref, d_ref, pp_ref, dp_ref, masked):
        lane16 = lax.broadcasted_iota(jnp.int32, (DIM, DIM), 1) // 16
        l_rows = lax.broadcasted_iota(jnp.int32, (DIM, CB), 0) % 16
        pick_l = jnp.where(l_rows < 3, 1.0, 0.0).astype(BF16)
        d_lanes = lax.broadcasted_iota(jnp.int32, (CB, DIM), 1) % 16
        pick_d = jnp.where((d_lanes >= 3) & (d_lanes < 6), 1.0, 0.0).astype(BF16)
        keys = pl.ds(pl.multiple_of(kb * CB, CB), CB)
        rhs_s = jnp.concatenate([kt_v[kb], pick_l], axis=0)
        rhs_d = jnp.concatenate([v_v[keys, :], pick_d], axis=1)
        stats = st_v[m, g]
        limit = PREFIX + CB * g + ROWS_DEV * xor3(me, m) - CB * kb

        def scores(rc):
            zero = jnp.zeros((), BF16)
            aug = jnp.concatenate([jnp.where(lane16 == 2 * rc, stats, zero),
                                   jnp.where(lane16 == 2 * rc + 1, stats, zero)], axis=0)
            two = pl.ds(2 * rc, 2)
            s = dg(jnp.concatenate([q_v[m, g, two].reshape(256, DIM), aug], axis=1), rhs_s, 1, 0)
            dp = dg(jnp.concatenate([do_v[m, g, two].reshape(256, DIM), aug], axis=1), rhs_d, 1, 1)
            p = jnp.exp2(s * EXP_SCALE)
            if masked:
                p = jnp.concatenate([jnp.where(x_v[...] <= limit + 64 * (2 * rc), p[:DIM], 0.0),
                                     jnp.where(x_v[...] <= limit + 64 * (2 * rc + 1), p[DIM:], 0.0)], axis=0)
            rows = pl.ds(256 * rc, 256)
            p_ref[rows, :] = p.astype(BF16)
            d_ref[rows, :] = (p * dp).astype(BF16)

        scores(0)
        dvt[kb_p] += dg(dot_v[rg_p], pp_ref[...], 1, 0)
        scores(1)
        dqt[rg_p, :, 0:512] += dg(kt_v[kb_p], dp_ref[0:512, :], 1, 1)
        scores(2)
        dkt[kb_p] += dg(qt_v[rg_p], dp_ref[...], 1, 0)
        scores(3)
        dqt[rg_p, :, 512:1024] += dg(kt_v[kb_p], dp_ref[512:1024, :], 1, 1)

    def flush(kb_p, rg_p):
        dvt[kb_p] += dg(dot_v[rg_p], p1[...], 1, 0)
        dkt[kb_p] += dg(qt_v[rg_p], d1[...], 1, 0)
        dqt[rg_p] += dg(kt_v[kb_p], d1[...], 1, 1)

    def wait_local(ref, sem):
        pltpu.make_async_copy(ref, ref, sem).wait()

    def prepare_rows(m, g):
        wait_local(st_v.at[m, g], rows_rs.at[m, g, 2])
        wait_local(q_v.at[m, g], rows_rs.at[m, g, 0])
        wait_local(do_v.at[m, g], rows_rs.at[m, g, 1])
        rg = m * N_GRP + g
        st_v[m, g] = st_v[m, g].T
        qt_v[rg] = q_v[m, g].reshape(RB, DIM).T
        dot_v[rg] = do_v[m, g].reshape(RB, DIM).T

    def wait_keys(k):
        for core in (0, 1):
            e = 2 * k + core
            m = xor3(me, e)
            rows = pl.ds(pl.multiple_of(e * KEYS_DEV, CHUNK), KEYS_DEV)
            wait_local(kn_v.at[rows, :], keys_rs.at[m, 0])
            wait_local(v_v.at[rows, :], keys_rs.at[m, 1])

    def stage_dq(m, g, par):
        odq[par] = (dqt[m * N_GRP + g].T * SCALE).astype(BF16).reshape(8, ROWS_DEV, GROUP, DIM)

    def send_dq(m, g, par):
        e = xor3(me, m)
        dst = dq_o.at[pl.ds(pl.multiple_of(8 * g, 8), 8), :, pl.ds(pl.multiple_of(me * GROUP, GROUP), GROUP), :]

        @pl.when(m == 0)
        def _():
            pltpu.make_async_copy(odq.at[par], dst, dq_ss.at[par]).start()

        @pl.when(m != 0)
        def _():
            pltpu.make_async_remote_copy(odq.at[par], dst, dq_ss.at[par], dq_rs.at[m],
                                         device_id=dev(e), device_id_type=MESH).start()

    def stage_kv(kb, par):
        okv[par, 0] = dkt[kb].T * SCALE
        okv[par, 1] = dvt[kb].T

    def send_kv(kb, par):
        def piece(j, c):
            ck = 8 * kb + j
            e = quo(ck, KEYS_DEV // CHUNK)
            off = pl.multiple_of(CHUNK * rem(ck, KEYS_DEV // CHUNK), CHUNK)
            m = xor3(me, e)
            src_rows = pl.ds(pl.multiple_of(CHUNK * j, CHUNK), CHUNK)
            for t, out in ((0, dk_o), (1, dv_o)):
                src = okv.at[par, t, src_rows, :]
                dst = out.at[me, pl.ds(off, CHUNK), :]

                @pl.when(m == 0)
                def _():
                    pltpu.make_async_copy(src, dst, kv_ss.at[par, t]).start()

                @pl.when(m != 0)
                def _():
                    pltpu.make_async_remote_copy(src, dst, kv_ss.at[par, t], kv_rs.at[m, t],
                                                 device_id=dev(e), device_id_type=MESH).start()
            return c
        lax.fori_loop(0, CB // CHUNK, piece, 0)

    def wait_kv(par):
        for t in (0, 1):
            wait_local(okv.at[par, t], kv_ss.at[par, t])

    def wait_dq(par):
        wait_local(odq.at[par], dq_ss.at[par])

    def block_of(o):
        i = jnp.where(o < PASS_1, o, jnp.where(o < PASS_2, o - PASS_1 + 4, jnp.where(o < PASS_3, o - PASS_2 + 4, o - PASS_3 + 10)))
        return rem(first_kb + i, NKB)

    def last_rows(n):
        return pick(n < 6, 6, pick(n < 12, 2, 4)) + rem(n, 2), quo(rem(n, 6), 2)

    def outer(o, carry):
        by_rows = o >= PASS_B
        kb = block_of(o)
        m_r, g_r = last_rows(jnp.maximum(o - PASS_B, 0))
        m_lo = pick(o < PASS_1, 0, pick((o >= PASS_2) & (o < PASS_3), 6, 2))
        n_m = pick((o >= PASS_1) & (o < PASS_2), 2, pick((o >= PASS_3), 3, 1))
        g_lo = jnp.maximum(kb - 16, 0)
        count = jnp.where(by_rows, pick((chip == 3) & (g_r == 0), 1, 2), (N_GRP - g_lo) * n_m)
        masked = jnp.where(by_rows, chip == 3, kb >= 16)
        first = (o == 0) | (o == PASS_1) | (o == PASS_2)

        @pl.when(o == 0)
        def _():
            wait_keys(chip)

        new = pick(kb == 0, 0, pick(kb == 4, 1, pick(kb == 9, 2, pick(kb == 14, 3, 4))))

        @pl.when((o < PASS_1) & (new < 4) & (new != chip))
        def _():
            wait_keys(new)

        @pl.when(o < PASS_1)
        def _():
            kt_v[kb] = kn_v[pl.ds(pl.multiple_of(kb * CB, CB), CB), :].T

        def pair(is_masked, j, c):
            kb_p, rg_p = c
            g = jnp.where(by_rows, g_r, g_lo + lax.div(j, n_m))
            m_a = jnp.where(by_rows, m_r, m_lo + 2 * lax.rem(j, n_m))
            m_b = jnp.where(by_rows, m_r, m_a + 1)
            kb_a = jnp.where(by_rows, first_kb + 2 * j, kb)
            kb_b = jnp.where(by_rows, first_kb + 2 * j + 1, kb)
            if not is_masked:
                @pl.when(first)
                def _():
                    prepare_rows(m_a, g)
                    prepare_rows(m_b, g)
            tile(kb_a, m_a, g, kb_p, rg_p, p0, d0, p1, d1, is_masked)
            tile(kb_b, m_b, g, kb_a, m_a * N_GRP + g, p1, d1, p0, d0, is_masked)
            return kb_b, m_b * N_GRP + g

        carry = lax.fori_loop(0, jnp.where(masked, 0, count), functools.partial(pair, False), carry)
        carry = lax.fori_loop(0, jnp.where(masked, count, 0), functools.partial(pair, True), carry)

        par = rem(o, 2)
        own = (o >= PASS_1 + 1) & (o < PASS_1 + 7)
        late = o >= PASS_B + 1
        r = o - (PASS_1 + 1)
        m_l, g_l = last_rows(jnp.maximum(o - PASS_B - 1, 0))
        m_s = jnp.where(own, rem(jnp.maximum(r, 0), 2), m_l)
        g_s = jnp.where(own, quo(jnp.maximum(r, 0), 2), g_l)

        own_b = (o >= PASS_1 + 2) & (o < PASS_1 + 8)
        m_l, g_l = last_rows(jnp.maximum(o - PASS_B - 2, 0))
        m_t = jnp.where(own_b, rem(jnp.maximum(r - 1, 0), 2), m_l)
        g_t = jnp.where(own_b, quo(jnp.maximum(r - 1, 0), 2), g_l)

        @pl.when(own_b | (o >= PASS_B + 2))
        def _():
            send_dq(m_t, g_t, 1 - par)

        @pl.when((o >= PASS_2 + 2) & (o <= PASS_B + 1))
        def _():
            send_kv(block_of(o - 2), 1 - par)

        @pl.when((own & (o >= PASS_1 + 3)) | late)
        def _():
            wait_dq(par)

        @pl.when(own | late)
        def _():
            stage_dq(m_s, g_s, par)

        @pl.when((o >= PASS_2 + 3) & (o <= PASS_B))
        def _():
            wait_kv(par)

        @pl.when((o >= PASS_2 + 1) & (o <= PASS_B))
        def _():
            stage_kv(block_of(o - 1), par)
        return carry

    m_0 = jnp.int32(0)
    kb_p, rg_p = lax.fori_loop(0, N_OUTER, outer, (first_kb, m_0))
    flush(kb_p, rg_p)

    m_t, g_t = last_rows(jnp.int32(16))
    m_s, g_s = last_rows(jnp.int32(17))
    end = N_OUTER % 2
    send_dq(m_t, g_t, 1 - end)
    wait_dq(end)
    stage_dq(m_s, g_s, end)

    def last_blocks(i, c):
        par = rem(i, 2)

        @pl.when(i > 0)
        def _():
            send_kv(first_kb + i - 1, 1 - par)

        @pl.when(i < 4)
        def _():
            wait_kv(par)
            stage_kv(first_kb + i, par)
        return c
    lax.fori_loop(0, 5, last_blocks, 0)
    send_dq(m_s, g_s, end)

    for par in (0, 1):
        wait_dq(par)
        wait_kv(par)
    for m in range(1, N_DEV):
        for g in range(N_GRP):
            wait_local(st_v.at[m, g], rows_ss.at[m, g, 2])
            wait_local(q_v.at[m, g], rows_ss.at[m, g, 0])
            wait_local(do_v.at[m, g], rows_ss.at[m, g, 1])
        wait_local(kn_v.at[pl.ds(0, KEYS_DEV), :], keys_ss.at[m, 0])
        wait_local(v_v.at[pl.ds(0, KEYS_DEV), :], keys_ss.at[m, 1])
        heads = pl.ds(0, GROUP)
        wait_local(dq_o.at[:, :, heads, :], dq_rs.at[m])
        wait_local(dk_o.at[0], kv_rs.at[m, 0])
        wait_local(dv_o.at[0], kv_rs.at[m, 1])


def split3(x):
    hi = lax.reduce_precision(x, 8, 7)
    mid = lax.reduce_precision(x - hi, 8, 7)
    lo = (x - hi) - mid
    return [hi, mid, lo]


def solution(mesh):
    row_spec = P(None, CP_AXES, 'heads', None)
    stat_spec = P(None, CP_AXES, 'heads')
    key_spec = P(CP_AXES, 'heads', None)
    any_ = pl.BlockSpec(memory_space=pl.ANY)

    def local_grads(queries, attn_out, grad_out, log_sum_exp, key_cache, value_cache):
        row_delta = jnp.sum(grad_out.astype(F32) * attn_out.astype(F32), axis=-1)
        parts = split3(log_sum_exp * (-1.0 / SCALE)) + split3(-row_delta)
        parts = parts + [jnp.zeros_like(row_delta)] * 10
        stats = jnp.stack(parts, axis=0).astype(BF16)
        stats = stats.reshape(16, N_GRP, 8, ROWS_DEV, N_DEV, GROUP)
        stats = jnp.transpose(stats, (4, 1, 2, 0, 3, 5)).reshape(N_DEV, N_GRP, DIM, DIM)
        keys = jnp.transpose(key_cache, (1, 0, 2))
        values = jnp.transpose(value_cache, (1, 0, 2))
        dma = pltpu.SemaphoreType.DMA
        rows_shape = (N_DEV, N_GRP, 8, ROWS_DEV, GROUP, DIM)
        n_rg = N_DEV * N_GRP
        grad_query, grad_key, grad_value = pl.pallas_call(
            kernel,
            name='attn_bwd',
            out_shape=(jax.ShapeDtypeStruct((N_SLICES, ROWS_DEV, N_DEV * GROUP, DIM), BF16),
                       jax.ShapeDtypeStruct((N_DEV, KEYS_DEV, DIM), F32),
                       jax.ShapeDtypeStruct((N_DEV, KEYS_DEV, DIM), F32)),
            in_specs=[any_] * 5,
            out_specs=[any_] * 3,
            scratch_shapes=[
                pltpu.VMEM(rows_shape, BF16), pltpu.VMEM(rows_shape, BF16),
                pltpu.VMEM((n_rg, DIM, RB), BF16), pltpu.VMEM((n_rg, DIM, RB), BF16),
                pltpu.VMEM((N_DEV, N_GRP, DIM, DIM), BF16),
                pltpu.VMEM((KEYS, DIM), BF16), pltpu.VMEM((KEYS, DIM), BF16),
                pltpu.VMEM((NKB, DIM, CB), BF16),
                pltpu.VMEM((n_rg, DIM, RB), F32),
                pltpu.VMEM((NKB, DIM, CB), F32), pltpu.VMEM((NKB, DIM, CB), F32),
                pltpu.VMEM((RB, CB), BF16), pltpu.VMEM((RB, CB), BF16),
                pltpu.VMEM((RB, CB), BF16), pltpu.VMEM((RB, CB), BF16),
                pltpu.VMEM((DIM, CB), jnp.int32),
                pltpu.VMEM((2, 2, CB, DIM), F32),
                pltpu.VMEM((2, 8, ROWS_DEV, GROUP, DIM), BF16),
                dma((N_DEV, N_GRP, 3)), dma((N_DEV, 2)), dma((N_DEV, N_GRP, 3)), dma((N_DEV, 2)),
                dma((2, 2)), dma((N_DEV, 2)), dma((2,)), dma((N_DEV,)),
            ],
            compiler_params=pltpu.CompilerParams(collective_id=0, has_side_effects=True, vmem_limit_bytes=67043328),
        )(queries, grad_out, stats, keys, values)
        return grad_query, jnp.transpose(grad_key, (1, 0, 2)), jnp.transpose(grad_value, (1, 0, 2))

    return jax.shard_map(local_grads, mesh=mesh, in_specs=(row_spec, row_spec, row_spec, stat_spec, key_spec, key_spec),
                         out_specs=(row_spec, key_spec, key_spec), check_vma=False)
```

```python
import functools
import math

import jax
import jax.numpy as jnp
from jax import lax
from jax.experimental import pallas as pl
from jax.experimental.pallas import tpu as pltpu
from jax.sharding import PartitionSpec as P

CP_AXES = ('cpo', 'cp')
MESH = pl.DeviceIdType.MESH
BF16 = jnp.bfloat16
F32 = jnp.float32

N_DEV = 8
N_SLICES = 24
ROWS_DEV = 8
GROUP = 16
DIM = 128
KEYS = 9728
KEYS_DEV = KEYS // N_DEV
PREFIX = 8192
N_GRP = 3
RB = 1024
CB = 512
NKB = KEYS // CB
CHUNK = 64
SCALE = DIM ** -0.5
EXP_SCALE = SCALE * math.log2(math.e)

UNROLL = 6
N_BUF = 3

PASS_1, PASS_2, PASS_D, PASS_3, PASS_B, PASS_C, N_OUTER = 17, 23, 38, 40, 49, 53, 54


def dg(a, b, ca, cb):
    return lax.dot_general(a, b, (((ca,), (cb,)), ((), ())), preferred_element_type=F32)


def quo(a, b):
    return lax.div(a, jnp.int32(b))


def rem(a, b):
    return lax.rem(a, jnp.int32(b))


def pick(cond, a, b):
    return jnp.where(cond, jnp.int32(a), jnp.int32(b))


def xor3(a, b):
    out = jnp.int32(0)
    for bit in (1, 2, 4):
        out = out + bit * rem(rem(quo(a, bit), 2) + rem(quo(b, bit), 2), 2)
    return out


def kernel(q_h, do_h, st_h, k_h, v_h, dq_o, dk_o, dv_o,
           q_v, do_v, qt_v, dot_v, st_v, aug_v, k_v, v_v, dqt, dkt, dvt, p0, d0, p1, d1, x_v, okv, odq,
           rows_ss, keys_ss, rows_rs, keys_rs, kv_ss, kv_rs, dq_ss, dq_rs):
    me = lax.axis_index('cpo') * 4 + lax.axis_index('cp')
    chip = quo(me, 2)
    first_kb = 5 * chip

    def dev(e):
        return {'cpo': quo(e, 4), 'cp': rem(e, 4)}

    barrier = pltpu.get_barrier_semaphore()
    for m in range(1, N_DEV):
        pl.semaphore_signal(barrier, inc=1, device_id=dev(xor3(me, jnp.int32(m))), device_id_type=MESH)

    def zero_keys(i, c):
        dkt[i] = jnp.zeros((DIM, CB), F32)
        dvt[i] = jnp.zeros((DIM, CB), F32)
        return c
    lax.fori_loop(0, NKB, zero_keys, 0)

    def zero_rows(i, c):
        dqt[i] = jnp.zeros((DIM, RB), F32)
        return c
    lax.fori_loop(0, N_DEV * N_GRP, zero_rows, 0)
    p1[...] = jnp.zeros((RB, CB), BF16)
    d1[...] = jnp.zeros((RB, CB), BF16)
    x_v[...] = (lax.broadcasted_iota(jnp.int32, (DIM, CB), 1)
                - lax.broadcasted_iota(jnp.int32, (DIM, CB), 0) // GROUP)

    pl.semaphore_wait(barrier, N_DEV - 1)

    def row_copies(m, g):
        e = xor3(me, jnp.int32(m))
        heads = pl.ds(pl.multiple_of(e * GROUP, GROUP), GROUP)
        pairs = ((st_h.at[e, g], st_v.at[m, g], 2),
                 (q_h.at[pl.ds(8 * g, 8), :, heads, :], q_v.at[m, g], 0),
                 (do_h.at[pl.ds(8 * g, 8), :, heads, :], do_v.at[m, g], 1))
        for src, dst, t in pairs:
            if m == 0:
                yield pltpu.make_async_copy(src, dst, rows_rs.at[m, g, t])
            else:
                yield pltpu.make_async_remote_copy(src, dst, rows_ss.at[m, g, t], rows_rs.at[m, g, t],
                                                   device_id=dev(e), device_id_type=MESH)

    def key_copies(e, m, local=False):
        rows = pl.ds(pl.multiple_of(me * KEYS_DEV, CHUNK), KEYS_DEV)
        for src, dst, t in ((k_h.at[e], k_v.at[rows, :], 0), (v_h.at[e], v_v.at[rows, :], 1)):
            if local:
                yield pltpu.make_async_copy(src, dst, keys_rs.at[m, t])
            else:
                yield pltpu.make_async_remote_copy(src, dst, keys_ss.at[m, t], keys_rs.at[m, t],
                                                   device_id=dev(e), device_id_type=MESH)

    for c in key_copies(me, jnp.int32(0), local=True):
        c.start()
    for c in key_copies(xor3(me, jnp.int32(1)), jnp.int32(1)):
        c.start()
    for g in range(N_GRP):
        for m in (0, 1):
            for c in row_copies(m, g):
                c.start()
    for back in (1, 2, 3):
        for core in (0, 1):
            e = 2 * rem(chip + 4 - back, 4) + core
            for c in key_copies(e, xor3(me, e)):
                c.start()
    for ms in ((2, 3, 4, 5), (6, 7)):
        for g in range(N_GRP):
            for m in ms:
                for c in row_copies(m, g):
                    c.start()

    def keys_t(ref, kb):
        return jnp.concatenate([ref[pl.ds(pl.multiple_of(kb * CB + DIM * i, DIM), DIM), :] for i in range(CB // DIM)], axis=1)

    def tile(kb, m, g, kb_p, rg_p, p_ref, d_ref, pp_ref, dp_ref, masked):
        slice_of = lax.broadcasted_iota(jnp.int32, (DIM, DIM), 1) % 8
        part_row = lax.broadcasted_iota(jnp.int32, (DIM, CB), 0)
        pick_l = jnp.where(part_row < 24, 1.0, 0.0).astype(BF16)
        pick_d = jnp.where((part_row >= 24) & (part_row < 48), 1.0, 0.0).astype(BF16)
        rhs_s = jnp.concatenate([keys_t(k_v, kb), pick_l], axis=0)
        rhs_d = jnp.concatenate([keys_t(v_v, kb), pick_d], axis=0)
        stats = aug_v[m, g]
        limit = PREFIX + CB * g + ROWS_DEV * xor3(me, m) - CB * kb

        def lhs(ref, rc):
            zero = jnp.zeros((), BF16)
            aug = jnp.concatenate([jnp.where(slice_of == 2 * rc, stats, zero),
                                   jnp.where(slice_of == 2 * rc + 1, stats, zero)], axis=0)
            return jnp.concatenate([ref[m, g, pl.ds(2 * rc, 2)].reshape(256, DIM), aug], axis=1)

        def score(rc):
            return dg(lhs(q_v, rc), rhs_s, 1, 0)

        def grad(rc):
            return dg(lhs(do_v, rc), rhs_d, 1, 0)

        def finish(rc, s, dp):
            p = jnp.exp2(s * EXP_SCALE)
            if masked:
                p = jnp.concatenate([jnp.where(x_v[...] <= limit + 64 * (2 * rc), p[:DIM], 0.0),
                                     jnp.where(x_v[...] <= limit + 64 * (2 * rc + 1), p[DIM:], 0.0)], axis=0)
            rows = pl.ds(256 * rc, 256)
            p_ref[rows, :] = p.astype(BF16)
            d_ref[rows, :] = (p * dp).astype(BF16)

        def dq_half(h, k):
            cols = slice(256 * k, 256 * k + 256)
            return dg(keys_t(k_v, kb_p)[:, cols], dp_ref[512 * h:512 * h + 512, cols], 1, 1)

        def dv_part(i):
            return dg(dot_v[rg_p][:, 256 * i:256 * i + 256], pp_ref[256 * i:256 * i + 256, :], 1, 0)

        def dk_part(i):
            return dg(qt_v[rg_p][:, 256 * i:256 * i + 256], dp_ref[256 * i:256 * i + 256, :], 1, 0)

        def put_dq(h, x):
            dqt[rg_p, :, 512 * h:512 * h + 512] = x + dqt[rg_p, :, 512 * h:512 * h + 512]

        s = score(0)
        dq = dq_half(0, 0)
        dp = grad(0)
        finish(0, s, dp)
        put_dq(0, dq_half(0, 1) + dq)
        s = score(1)
        dv = dv_part(0)
        dv = dv_part(1) + dv
        dp = grad(1)
        finish(1, s, dp)
        dv = dv_part(2) + dv
        dv = dv_part(3) + dv
        dvt[kb_p] = dv + dvt[kb_p]
        s = score(2)
        dq = dq_half(1, 0)
        dp = grad(2)
        finish(2, s, dp)
        put_dq(1, dq_half(1, 1) + dq)
        s = score(3)
        dk = dk_part(0)
        dk = dk_part(1) + dk
        dp = grad(3)
        finish(3, s, dp)
        dk = dk_part(2) + dk
        dk = dk_part(3) + dk
        dkt[kb_p] = dk + dkt[kb_p]

    def flush(kb_p, rg_p):
        dvt[kb_p] += dg(dot_v[rg_p], p1[...], 1, 0)
        dkt[kb_p] += dg(qt_v[rg_p], d1[...], 1, 0)
        dqt[rg_p] += dg(keys_t(k_v, kb_p), d1[...], 1, 1)

    def wait_local(ref, sem):
        pltpu.make_async_copy(ref, ref, sem).wait()

    def prepare_rows(m, g):
        wait_local(st_v.at[m, g], rows_rs.at[m, g, 2])
        wait_local(q_v.at[m, g], rows_rs.at[m, g, 0])
        wait_local(do_v.at[m, g], rows_rs.at[m, g, 1])
        rg = m * N_GRP + g
        x = st_v[m, g]
        hi = x.astype(BF16).astype(F32)
        mid = (x - hi).astype(BF16).astype(F32)
        lo = (x - hi) - mid
        parts = [y[8 * t:8 * t + 8] for t in (0, 1) for y in (hi, mid, lo)]
        aug_v[m, g] = jnp.concatenate(parts + [jnp.zeros((80, DIM), F32)], axis=0).T.astype(BF16)
        qt_v[rg] = q_v[m, g].reshape(RB, DIM).T
        dot_v[rg] = do_v[m, g].reshape(RB, DIM).T

    def wait_keys(k):
        for core in (0, 1):
            e = 2 * k + core
            m = xor3(me, e)
            rows = pl.ds(pl.multiple_of(e * KEYS_DEV, CHUNK), KEYS_DEV)
            wait_local(k_v.at[rows, :], keys_rs.at[m, 0])
            wait_local(v_v.at[rows, :], keys_rs.at[m, 1])

    def prepare_keys(kb):
        for i in range(CB // DIM):
            rows = pl.ds(pl.multiple_of(kb * CB + DIM * i, DIM), DIM)
            k_v[rows, :] = k_v[rows, :].T
            v_v[rows, :] = v_v[rows, :].T

    def stage_dq(m, par):
        for g in range(N_GRP):
            odq[par, g] = (dqt[m * N_GRP + g].T * SCALE).astype(BF16).reshape(8, ROWS_DEV, GROUP, DIM)

    def send_dq(m, par):
        e = xor3(me, m)
        heads = pl.ds(pl.multiple_of(me * GROUP, GROUP), GROUP)
        for g in range(N_GRP):
            dst = dq_o.at[pl.ds(8 * g, 8), :, heads, :]

            @pl.when(m == 0)
            def _():
                pltpu.make_async_copy(odq.at[par, g], dst, dq_ss.at[par, g]).start()

            @pl.when(m != 0)
            def _():
                pltpu.make_async_remote_copy(odq.at[par, g], dst, dq_ss.at[par, g], dq_rs.at[m],
                                             device_id=dev(e), device_id_type=MESH).start()

    def stage_kv(kb, buf):
        okv[buf, 0] = dkt[kb].T * SCALE
        okv[buf, 1] = dvt[kb].T

    def send_kv(kb, buf):
        def piece(j, c):
            ck = 8 * kb + j
            e = quo(ck, KEYS_DEV // CHUNK)
            off = pl.multiple_of(CHUNK * rem(ck, KEYS_DEV // CHUNK), CHUNK)
            m = xor3(me, e)
            src_rows = pl.ds(pl.multiple_of(CHUNK * j, CHUNK), CHUNK)
            for t, out in ((0, dk_o), (1, dv_o)):
                src = okv.at[buf, t, src_rows, :]
                dst = out.at[me, pl.ds(off, CHUNK), :]

                @pl.when(m == 0)
                def _():
                    pltpu.make_async_copy(src, dst, kv_ss.at[buf, t]).start()

                @pl.when(m != 0)
                def _():
                    pltpu.make_async_remote_copy(src, dst, kv_ss.at[buf, t], kv_rs.at[m, t],
                                                 device_id=dev(e), device_id_type=MESH).start()
            return c
        lax.fori_loop(0, CB // CHUNK, piece, 0)

    def wait_kv(buf):
        for t in (0, 1):
            wait_local(okv.at[buf, t], kv_ss.at[buf, t])

    def wait_dq(par):
        for g in range(N_GRP):
            wait_local(odq.at[par, g], dq_ss.at[par, g])

    def between(o, lo, hi):
        return (o >= lo) & (o < hi)

    def block_of(o):
        n = jnp.where(o < PASS_2, o - PASS_1, jnp.where(o < PASS_D, o - PASS_2, o - PASS_3 + 6))
        n = jnp.maximum(n, 0)
        other = 4 + 5 * rem(n, 3) + quo(n, 3)
        i = jnp.where(o < PASS_1, jnp.where(o < 2, o, o + 2), other)
        return rem(first_kb + i, NKB)

    def rows_of(o):
        n = jnp.maximum(o - PASS_B, 0)
        return jnp.where(o < PASS_B, 6 + o - PASS_D, 2 + 2 * rem(n, 2) + quo(n, 2))

    def kv_event(o):
        return jnp.where(o < PASS_D, o - PASS_2, 6 + o - PASS_3)

    def outer(o, carry):
        ends = between(o, PASS_D, PASS_3) | between(o, PASS_B, PASS_C)
        last = o >= PASS_C
        kb = block_of(o)
        m_r = rows_of(o)
        m_lo = pick(o < PASS_1, 0, pick(between(o, PASS_2, PASS_D), 6, 2))
        n_m = pick((o < PASS_1) | between(o, PASS_2, PASS_D), 2, 4)
        g_lo = jnp.maximum(kb - 16, 0)
        masked = jnp.where(ends | last, chip == 3, kb >= 16)
        n_full = jnp.where(ends | last, 2, quo(n_m, 2))
        n_pairs = jnp.where(ends, 5, jnp.where(last, 4, (N_GRP - g_lo) * quo(n_m, 2)))
        first = (o == 0) | (o == PASS_1) | (o == PASS_2)

        @pl.when(o == 0)
        def _():
            wait_keys(chip)

        new = pick(kb == 0, 0, pick(kb == 4, 1, pick(kb == 9, 2, pick(kb == 14, 3, 4))))

        @pl.when((o < PASS_1) & (new < 4) & (new != chip))
        def _():
            wait_keys(new)

        @pl.when(o < PASS_1)
        def _():
            prepare_keys(kb)

        @pl.when(o < 2)
        def _():
            prepare_keys(kb + 2)

        def index(n):
            g = jnp.where(ends | last, quo(n, 4), lax.div(n, n_m))
            m = jnp.where(ends, m_r, jnp.where(last, rem(quo(n, 2), 2), m_lo + lax.rem(n, n_m)))
            k = jnp.where(ends, first_kb + rem(n, 4), jnp.where(last, first_kb + 2 + rem(n, 2), kb))
            return k, m, g

        def six(j, c):
            @pl.when(first)
            def _():
                def one(t, c):
                    _, m, g = index(UNROLL * j + t)
                    prepare_rows(m, g)
                    return c
                lax.fori_loop(0, UNROLL, one, 0)
            kb_p, rg_p = c
            for t in range(UNROLL):
                k, m, g = index(UNROLL * j + t)
                bufs = (p0, d0, p1, d1) if t % 2 == 0 else (p1, d1, p0, d0)
                tile(k, m, g, kb_p, rg_p, *bufs, False)
                kb_p, rg_p = k, m * N_GRP + g
            return kb_p, rg_p

        def pair(j, c):
            kb_p, rg_p = c
            n2 = quo(n_m, 2)
            g = jnp.where(ends, quo(j + 1, 2), jnp.where(last, 1 + quo(j, 2), g_lo + lax.div(j, n2)))
            half = jnp.where(ends, jnp.where(j == 0, 0, rem(j + 1, 2)), 1)
            m_a = jnp.where(ends, m_r, jnp.where(last, rem(j, 2), m_lo + 2 * lax.rem(j, n2)))
            m_b = jnp.where(ends | last, m_a, m_a + 1)
            k_a = jnp.where(ends | last, first_kb + 2 * half, kb)
            k_b = jnp.where(ends | last, k_a + 1, kb)
            tile(k_a, m_a, g, kb_p, rg_p, p0, d0, p1, d1, True)
            tile(k_b, m_b, g, k_a, m_a * N_GRP + g, p1, d1, p0, d0, True)
            return k_b, m_b * N_GRP + g

        carry = lax.fori_loop(0, jnp.where(masked, 0, n_full), six, carry)
        carry = lax.fori_loop(0, jnp.where(masked, n_pairs, 0), pair, carry)

        par = rem(o, 2)

        @pl.when(between(o, PASS_D + 2, PASS_3 + 2) | between(o, PASS_B + 2, PASS_C + 2))
        def _():
            send_dq(rows_of(o - 2), 1 - par)

        @pl.when(between(o, PASS_2 + 2, PASS_2 + 8) | between(o, PASS_3 + 2, PASS_B + 2))
        def _():
            send_kv(block_of(o - 2), rem(kv_event(o - 2), N_BUF))

        @pl.when(between(o, PASS_D + 1, PASS_3 + 1) | between(o, PASS_B + 1, PASS_C + 1))
        def _():
            @pl.when(o > PASS_3)
            def _():
                wait_dq(par)
            stage_dq(rows_of(o - 1), par)

        @pl.when(between(o, PASS_2 + 1, PASS_2 + 7) | between(o, PASS_3 + 1, PASS_B + 1))
        def _():
            ev = kv_event(o - 1)

            @pl.when(ev >= N_BUF)
            def _():
                wait_kv(rem(ev, N_BUF))
            stage_kv(block_of(o - 1), rem(ev, N_BUF))
        return carry

    kb_p, rg_p = lax.fori_loop(0, N_OUTER, outer, (first_kb, jnp.int32(0)))
    flush(kb_p, rg_p)

    send_dq(rows_of(jnp.int32(PASS_C - 1)), (N_OUTER - 1) % 2)

    def last_parts(i, c):
        @pl.when((i > 0) & (i < 5))
        def _():
            send_kv(first_kb + i - 1, rem(14 + i, N_BUF))

        @pl.when(i < 4)
        def _():
            wait_kv(rem(15 + i, N_BUF))
            stage_kv(first_kb + i, rem(15 + i, N_BUF))

        @pl.when(i > 1)
        def _():
            par = rem(i, 2)

            @pl.when(i < 4)
            def _():
                wait_dq(par)
                stage_dq(i - 2, par)

            @pl.when(i > 2)
            def _():
                send_dq(i - 3, 1 - par)
        return c
    lax.fori_loop(0, 5, last_parts, 0)

    for par in (0, 1):
        wait_dq(par)
    for buf in range(N_BUF):
        wait_kv(buf)
    for m in range(1, N_DEV):
        for g in range(N_GRP):
            wait_local(st_v.at[m, g], rows_ss.at[m, g, 2])
            wait_local(q_v.at[m, g], rows_ss.at[m, g, 0])
            wait_local(do_v.at[m, g], rows_ss.at[m, g, 1])
        wait_local(k_v.at[pl.ds(0, KEYS_DEV), :], keys_ss.at[m, 0])
        wait_local(v_v.at[pl.ds(0, KEYS_DEV), :], keys_ss.at[m, 1])
        heads = pl.ds(0, GROUP)
        wait_local(dq_o.at[:, :, heads, :], dq_rs.at[m])
        wait_local(dk_o.at[0], kv_rs.at[m, 0])
        wait_local(dv_o.at[0], kv_rs.at[m, 1])


def solution(mesh):
    row_spec = P(None, CP_AXES, 'heads', None)
    stat_spec = P(None, CP_AXES, 'heads')
    key_spec = P(CP_AXES, 'heads', None)
    any_ = pl.BlockSpec(memory_space=pl.ANY)

    def local_grads(queries, attn_out, grad_out, log_sum_exp, key_cache, value_cache):
        row_delta = jnp.sum(grad_out.astype(F32) * attn_out.astype(F32), axis=-1)
        stats = jnp.stack([log_sum_exp * (-1.0 / SCALE), -row_delta], axis=0)
        stats = stats.reshape(2, N_GRP, 8, ROWS_DEV, N_DEV, GROUP)
        stats = jnp.transpose(stats, (4, 1, 0, 2, 3, 5)).reshape(N_DEV, N_GRP, 16, DIM)
        keys = jnp.transpose(key_cache, (1, 0, 2))
        values = jnp.transpose(value_cache, (1, 0, 2))
        dma = pltpu.SemaphoreType.DMA
        rows_shape = (N_DEV, N_GRP, 8, ROWS_DEV, GROUP, DIM)
        n_rg = N_DEV * N_GRP
        grad_query, grad_key, grad_value = pl.pallas_call(
            kernel,
            name='attn_bwd',
            out_shape=(jax.ShapeDtypeStruct((N_SLICES, ROWS_DEV, N_DEV * GROUP, DIM), BF16),
                       jax.ShapeDtypeStruct((N_DEV, KEYS_DEV, DIM), F32),
                       jax.ShapeDtypeStruct((N_DEV, KEYS_DEV, DIM), F32)),
            in_specs=[any_] * 5,
            out_specs=[any_] * 3,
            scratch_shapes=[
                pltpu.VMEM(rows_shape, BF16), pltpu.VMEM(rows_shape, BF16),
                pltpu.VMEM((n_rg, DIM, RB), BF16), pltpu.VMEM((n_rg, DIM, RB), BF16),
                pltpu.VMEM((N_DEV, N_GRP, 16, DIM), F32), pltpu.VMEM((N_DEV, N_GRP, DIM, DIM), BF16),
                pltpu.VMEM((KEYS, DIM), BF16), pltpu.VMEM((KEYS, DIM), BF16),
                pltpu.VMEM((n_rg, DIM, RB), F32),
                pltpu.VMEM((NKB, DIM, CB), F32), pltpu.VMEM((NKB, DIM, CB), F32),
                pltpu.VMEM((RB, CB), BF16), pltpu.VMEM((RB, CB), BF16),
                pltpu.VMEM((RB, CB), BF16), pltpu.VMEM((RB, CB), BF16),
                pltpu.VMEM((DIM, CB), jnp.int32),
                pltpu.VMEM((N_BUF, 2, CB, DIM), F32),
                pltpu.VMEM((2, N_GRP, 8, ROWS_DEV, GROUP, DIM), BF16),
                dma((N_DEV, N_GRP, 3)), dma((N_DEV, 2)), dma((N_DEV, N_GRP, 3)), dma((N_DEV, 2)),
                dma((N_BUF, 2)), dma((N_DEV, 2)), dma((2, N_GRP)), dma((N_DEV,)),
            ],
            compiler_params=pltpu.CompilerParams(collective_id=0, has_side_effects=True, vmem_limit_bytes=67043328),
        )(queries, grad_out, stats, keys, values)
        return grad_query, jnp.transpose(grad_key, (1, 0, 2)), jnp.transpose(grad_value, (1, 0, 2))

    return jax.shard_map(local_grads, mesh=mesh, in_specs=(row_spec, row_spec, row_spec, stat_spec, key_spec, key_spec),
                         out_specs=(row_spec, key_spec, key_spec), check_vma=False)
```

```python
import functools
import math

import jax
import jax.numpy as jnp
from jax import lax
from jax.experimental import pallas as pl
from jax.experimental.pallas import tpu as pltpu
from jax.sharding import PartitionSpec as P

CP_AXES = ('cpo', 'cp')
MESH = pl.DeviceIdType.MESH
BF16 = jnp.bfloat16
F32 = jnp.float32

N_DEV = 8
N_SLICES = 24
ROWS_DEV = 8
GROUP = 16
DIM = 128
KEYS = 9728
KEYS_DEV = KEYS // N_DEV
PREFIX = 8192
N_GRP = 3
RB = 1024
CB = 512
NKB = KEYS // CB
CHUNK = 64
SCALE = DIM ** -0.5
EXP_SCALE = SCALE * math.log2(math.e)

UNROLL = 6
N_BUF = 3

PASS_1, PASS_2, PASS_D, PASS_3, PASS_B, PASS_C, N_OUTER = 17, 23, 38, 40, 49, 53, 54


def dg(a, b, ca, cb):
    return lax.dot_general(a, b, (((ca,), (cb,)), ((), ())), preferred_element_type=F32)


def quo(a, b):
    return lax.div(a, jnp.int32(b))


def rem(a, b):
    return lax.rem(a, jnp.int32(b))


def pick(cond, a, b):
    return jnp.where(cond, jnp.int32(a), jnp.int32(b))


def xor3(a, b):
    out = jnp.int32(0)
    for bit in (1, 2, 4):
        out = out + bit * rem(rem(quo(a, bit), 2) + rem(quo(b, bit), 2), 2)
    return out


def kernel(q_h, do_h, st_h, k_h, v_h, dq_o, dk_o, dv_o,
           q_v, do_v, qt_v, dot_v, st_v, aug_v, k_v, v_v, dqt, dkt, dvt, p0, d0, p1, d1, x_v, okv, odq,
           rows_ss, keys_ss, rows_rs, keys_rs, kv_ss, kv_rs, dq_ss, dq_rs):
    me = lax.axis_index('cpo') * 4 + lax.axis_index('cp')
    chip = quo(me, 2)
    first_kb = 5 * chip

    def dev(e):
        return {'cpo': quo(e, 4), 'cp': rem(e, 4)}

    barrier = pltpu.get_barrier_semaphore()
    for m in range(1, N_DEV):
        pl.semaphore_signal(barrier, inc=1, device_id=dev(xor3(me, jnp.int32(m))), device_id_type=MESH)

    def zero_keys(i, c):
        dkt[i] = jnp.zeros((DIM, CB), F32)
        dvt[i] = jnp.zeros((DIM, CB), F32)
        return c
    lax.fori_loop(0, NKB, zero_keys, 0)

    def zero_rows(i, c):
        dqt[i] = jnp.zeros((DIM, RB), F32)
        return c
    lax.fori_loop(0, N_DEV * N_GRP, zero_rows, 0)
    p1[...] = jnp.zeros((RB, CB), BF16)
    d1[...] = jnp.zeros((RB, CB), BF16)
    x_v[...] = (lax.broadcasted_iota(jnp.int32, (DIM, CB), 1)
                - lax.broadcasted_iota(jnp.int32, (DIM, CB), 0) // GROUP)

    with jax.named_scope('barrier'):
        pl.semaphore_wait(barrier, N_DEV - 1)

    def row_copies(m, g):
        e = xor3(me, jnp.int32(m))
        heads = pl.ds(pl.multiple_of(e * GROUP, GROUP), GROUP)
        pairs = ((st_h.at[e, g], st_v.at[m, g], 2),
                 (q_h.at[pl.ds(8 * g, 8), :, heads, :], q_v.at[m, g], 0),
                 (do_h.at[pl.ds(8 * g, 8), :, heads, :], do_v.at[m, g], 1))
        for src, dst, t in pairs:
            if m == 0:
                yield pltpu.make_async_copy(src, dst, rows_rs.at[m, g, t])
            else:
                yield pltpu.make_async_remote_copy(src, dst, rows_ss.at[m, g, t], rows_rs.at[m, g, t],
                                                   device_id=dev(e), device_id_type=MESH)

    def key_copies(e, m, local=False):
        rows = pl.ds(pl.multiple_of(me * KEYS_DEV, CHUNK), KEYS_DEV)
        for src, dst, t in ((k_h.at[e], k_v.at[rows, :], 0), (v_h.at[e], v_v.at[rows, :], 1)):
            if local:
                yield pltpu.make_async_copy(src, dst, keys_rs.at[m, t])
            else:
                yield pltpu.make_async_remote_copy(src, dst, keys_ss.at[m, t], keys_rs.at[m, t],
                                                   device_id=dev(e), device_id_type=MESH)

    for c in key_copies(me, jnp.int32(0), local=True):
        c.start()
    for c in key_copies(xor3(me, jnp.int32(1)), jnp.int32(1)):
        c.start()
    for g in range(N_GRP):
        for m in (0, 1):
            for c in row_copies(m, g):
                c.start()
    for back in (1, 2, 3):
        for core in (0, 1):
            e = 2 * rem(chip + 4 - back, 4) + core
            for c in key_copies(e, xor3(me, e)):
                c.start()
    for ms in ((2, 3, 4, 5), (6, 7)):
        for g in range(N_GRP):
            for m in ms:
                for c in row_copies(m, g):
                    c.start()

    def keys_t(ref, kb):
        return jnp.concatenate([ref[pl.ds(pl.multiple_of(kb * CB + DIM * i, DIM), DIM), :] for i in range(CB // DIM)], axis=1)

    def tile(kb, m, g, kb_p, rg_p, p_ref, d_ref, pp_ref, dp_ref, masked):
        slice_of = lax.broadcasted_iota(jnp.int32, (DIM, DIM), 1) % 8
        part_row = lax.broadcasted_iota(jnp.int32, (DIM, CB), 0)
        pick_l = jnp.where(part_row < 24, 1.0, 0.0).astype(BF16)
        pick_d = jnp.where((part_row >= 24) & (part_row < 48), 1.0, 0.0).astype(BF16)
        rhs_s = jnp.concatenate([keys_t(k_v, kb), pick_l], axis=0)
        rhs_d = jnp.concatenate([keys_t(v_v, kb), pick_d], axis=0)
        stats = aug_v[m, g]
        limit = PREFIX + CB * g + ROWS_DEV * xor3(me, m) - CB * kb

        def lhs(ref, rc):
            zero = jnp.zeros((), BF16)
            aug = jnp.concatenate([jnp.where(slice_of == 2 * rc, stats, zero),
                                   jnp.where(slice_of == 2 * rc + 1, stats, zero)], axis=0)
            return jnp.concatenate([ref[m, g, pl.ds(2 * rc, 2)].reshape(256, DIM), aug], axis=1)

        def score(rc):
            return dg(lhs(q_v, rc), rhs_s, 1, 0)

        def grad(rc):
            return dg(lhs(do_v, rc), rhs_d, 1, 0)

        def finish(rc, s, dp):
            p = jnp.exp2(s * EXP_SCALE)
            if masked:
                p = jnp.concatenate([jnp.where(x_v[...] <= limit + 64 * (2 * rc), p[:DIM], 0.0),
                                     jnp.where(x_v[...] <= limit + 64 * (2 * rc + 1), p[DIM:], 0.0)], axis=0)
            rows = pl.ds(256 * rc, 256)
            p_ref[rows, :] = p.astype(BF16)
            d_ref[rows, :] = (p * dp).astype(BF16)

        def dq_half(h, k):
            cols = slice(256 * k, 256 * k + 256)
            return dg(keys_t(k_v, kb_p)[:, cols], dp_ref[512 * h:512 * h + 512, cols], 1, 1)

        def dv_part(i):
            return dg(dot_v[rg_p][:, 256 * i:256 * i + 256], pp_ref[256 * i:256 * i + 256, :], 1, 0)

        def dk_part(i):
            return dg(qt_v[rg_p][:, 256 * i:256 * i + 256], dp_ref[256 * i:256 * i + 256, :], 1, 0)

        def put_dq(h, x):
            dqt[rg_p, :, 512 * h:512 * h + 512] = x + dqt[rg_p, :, 512 * h:512 * h + 512]

        s = score(0)
        dq = dq_half(0, 0)
        dp = grad(0)
        finish(0, s, dp)
        put_dq(0, dq_half(0, 1) + dq)
        s = score(1)
        dv = dv_part(0)
        dv = dv_part(1) + dv
        dp = grad(1)
        finish(1, s, dp)
        dv = dv_part(2) + dv
        dv = dv_part(3) + dv
        dvt[kb_p] = dv + dvt[kb_p]
        s = score(2)
        dq = dq_half(1, 0)
        dp = grad(2)
        finish(2, s, dp)
        put_dq(1, dq_half(1, 1) + dq)
        s = score(3)
        dk = dk_part(0)
        dk = dk_part(1) + dk
        dp = grad(3)
        finish(3, s, dp)
        dk = dk_part(2) + dk
        dk = dk_part(3) + dk
        dkt[kb_p] = dk + dkt[kb_p]

    def flush(kb_p, rg_p):
        dvt[kb_p] += dg(dot_v[rg_p], p1[...], 1, 0)
        dkt[kb_p] += dg(qt_v[rg_p], d1[...], 1, 0)
        dqt[rg_p] += dg(keys_t(k_v, kb_p), d1[...], 1, 1)

    def wait_local(ref, sem):
        pltpu.make_async_copy(ref, ref, sem).wait()

    def prepare_rows(m, g):
        with jax.named_scope('w_rows'):
            wait_local(st_v.at[m, g], rows_rs.at[m, g, 2])
            wait_local(q_v.at[m, g], rows_rs.at[m, g, 0])
            wait_local(do_v.at[m, g], rows_rs.at[m, g, 1])
        rg = m * N_GRP + g
        x = st_v[m, g]
        hi = x.astype(BF16).astype(F32)
        mid = (x - hi).astype(BF16).astype(F32)
        lo = (x - hi) - mid
        parts = [y[8 * t:8 * t + 8] for t in (0, 1) for y in (hi, mid, lo)]
        aug_v[m, g] = jnp.concatenate(parts + [jnp.zeros((80, DIM), F32)], axis=0).T.astype(BF16)
        qt_v[rg] = q_v[m, g].reshape(RB, DIM).T
        dot_v[rg] = do_v[m, g].reshape(RB, DIM).T

    def wait_keys(k):
        with jax.named_scope('w_keys'):
            for core in (0, 1):
                e = 2 * k + core
                m = xor3(me, e)
                rows = pl.ds(pl.multiple_of(e * KEYS_DEV, CHUNK), KEYS_DEV)
                wait_local(k_v.at[rows, :], keys_rs.at[m, 0])
                wait_local(v_v.at[rows, :], keys_rs.at[m, 1])

    def prepare_keys(kb):
        for i in range(CB // DIM):
            rows = pl.ds(pl.multiple_of(kb * CB + DIM * i, DIM), DIM)
            k_v[rows, :] = k_v[rows, :].T
            v_v[rows, :] = v_v[rows, :].T

    def stage_dq(m, par):
        with jax.named_scope('s_dq'):
            for g in range(N_GRP):
                odq[par, g] = (dqt[m * N_GRP + g].T * SCALE).astype(BF16).reshape(8, ROWS_DEV, GROUP, DIM)

    def send_dq(m, par):
        e = xor3(me, m)
        heads = pl.ds(pl.multiple_of(me * GROUP, GROUP), GROUP)
        for g in range(N_GRP):
            dst = dq_o.at[pl.ds(8 * g, 8), :, heads, :]

            @pl.when(m == 0)
            def _():
                pltpu.make_async_copy(odq.at[par, g], dst, dq_ss.at[par, g]).start()

            @pl.when(m != 0)
            def _():
                pltpu.make_async_remote_copy(odq.at[par, g], dst, dq_ss.at[par, g], dq_rs.at[m],
                                             device_id=dev(e), device_id_type=MESH).start()

    def stage_kv(kb, buf):
        with jax.named_scope('s_kv'):
            okv[buf, 0] = dkt[kb].T * SCALE
            okv[buf, 1] = dvt[kb].T

    def send_kv(kb, buf):
        def piece(j, c):
            ck = 8 * kb + j
            e = quo(ck, KEYS_DEV // CHUNK)
            off = pl.multiple_of(CHUNK * rem(ck, KEYS_DEV // CHUNK), CHUNK)
            m = xor3(me, e)
            src_rows = pl.ds(pl.multiple_of(CHUNK * j, CHUNK), CHUNK)
            for t, out in ((0, dk_o), (1, dv_o)):
                src = okv.at[buf, t, src_rows, :]
                dst = out.at[pl.ds(off, CHUNK), me, 0, :]

                @pl.when(m == 0)
                def _():
                    pltpu.make_async_copy(src, dst, kv_ss.at[buf, t]).start()

                @pl.when(m != 0)
                def _():
                    pltpu.make_async_remote_copy(src, dst, kv_ss.at[buf, t], kv_rs.at[m, t],
                                                 device_id=dev(e), device_id_type=MESH).start()
            return c
        lax.fori_loop(0, CB // CHUNK, piece, 0)

    def wait_kv(buf):
        with jax.named_scope('w_kv'):
            for t in (0, 1):
                wait_local(okv.at[buf, t], kv_ss.at[buf, t])

    def wait_dq(par):
        with jax.named_scope('w_dq'):
            for g in range(N_GRP):
                wait_local(odq.at[par, g], dq_ss.at[par, g])

    def between(o, lo, hi):
        return (o >= lo) & (o < hi)

    def block_of(o):
        n = jnp.where(o < PASS_2, o - PASS_1, jnp.where(o < PASS_D, o - PASS_2, o - PASS_3 + 6))
        n = jnp.maximum(n, 0)
        other = 4 + 5 * rem(n, 3) + quo(n, 3)
        i = jnp.where(o < PASS_1, jnp.where(o < 2, o, o + 2), other)
        return rem(first_kb + i, NKB)

    def rows_of(o):
        n = jnp.maximum(o - PASS_B, 0)
        return jnp.where(o < PASS_B, 6 + o - PASS_D, 2 + 2 * rem(n, 2) + quo(n, 2))

    def kv_event(o):
        return jnp.where(o < PASS_D, o - PASS_2, 6 + o - PASS_3)

    def outer(o, carry):
        ends = between(o, PASS_D, PASS_3) | between(o, PASS_B, PASS_C)
        last = o >= PASS_C
        kb = block_of(o)
        m_r = rows_of(o)
        m_lo = pick(o < PASS_1, 0, pick(between(o, PASS_2, PASS_D), 6, 2))
        n_m = pick((o < PASS_1) | between(o, PASS_2, PASS_D), 2, 4)
        g_lo = jnp.maximum(kb - 16, 0)
        masked = jnp.where(ends | last, chip == 3, kb >= 16)
        n_full = jnp.where(ends | last, 2, quo(n_m, 2))
        odd = jnp.where(o < PASS_3, o - PASS_D, rem(jnp.maximum(o - PASS_B, 0), 2))
        n_pairs = jnp.where(ends, 4 + odd, jnp.where(last, 3, (N_GRP - g_lo) * quo(n_m, 2)))
        first = (o == 0) | (o == PASS_1) | (o == PASS_2)

        @pl.when(o == 0)
        def _():
            wait_keys(chip)

        new = pick(kb == 0, 0, pick(kb == 4, 1, pick(kb == 9, 2, pick(kb == 14, 3, 4))))

        @pl.when((o < PASS_1) & (new < 4) & (new != chip))
        def _():
            wait_keys(new)

        @pl.when(o < PASS_1)
        def _():
            prepare_keys(kb)

        @pl.when(o < 2)
        def _():
            prepare_keys(kb + 2)

        def index(n):
            g = jnp.where(ends | last, quo(n, 4), lax.div(n, n_m))
            m = jnp.where(ends, m_r, jnp.where(last, rem(quo(n, 2), 2), m_lo + lax.rem(n, n_m)))
            k = jnp.where(ends, first_kb + rem(n, 4), jnp.where(last, first_kb + 2 + rem(n, 2), kb))
            return k, m, g

        def six(j, c):
            @pl.when(first)
            def _():
                def one(t, c):
                    _, m, g = index(UNROLL * j + t)
                    prepare_rows(m, g)
                    return c
                lax.fori_loop(0, UNROLL, one, 0)
            kb_p, rg_p = c
            for t in range(UNROLL):
                k, m, g = index(UNROLL * j + t)
                bufs = (p0, d0, p1, d1) if t % 2 == 0 else (p1, d1, p0, d0)
                tile(k, m, g, kb_p, rg_p, *bufs, False)
                kb_p, rg_p = k, m * N_GRP + g
            return kb_p, rg_p

        def index_masked(n):
            n2 = quo(n, 2)
            half = quo(n_m, 2)
            g = g_lo + lax.div(n2, half)
            m = m_lo + 2 * lax.rem(n2, half) + rem(n, 2)
            k = kb
            e = n - odd
            e_m = jnp.where(e < 0, rows_of(o - 1), m_r)
            e = jnp.where(e < 0, 8, e)
            e_g = pick(e < 2, 0, pick(e < 5, 1, 2))
            e_k = 15 + e - pick(e < 2, 0, pick(e < 5, 2, 5))
            f = rem(n, 3)
            f_g = pick(f > 0, 2, 1)
            f_k = pick(f == 2, 18, 17)
            g = jnp.where(ends, e_g, jnp.where(last, f_g, g))
            m = jnp.where(ends, e_m, jnp.where(last, quo(n, 3), m))
            k = jnp.where(ends, e_k, jnp.where(last, f_k, k))
            return k, m, g

        def pair(j, c):
            kb_p, rg_p = c
            k_a, m_a, g_a = index_masked(2 * j)
            k_b, m_b, g_b = index_masked(2 * j + 1)
            tile(k_a, m_a, g_a, kb_p, rg_p, p0, d0, p1, d1, True)
            tile(k_b, m_b, g_b, k_a, m_a * N_GRP + g_a, p1, d1, p0, d0, True)
            return k_b, m_b * N_GRP + g_b

        with jax.named_scope('tiles'):
            carry = lax.fori_loop(0, jnp.where(masked, 0, n_full), six, carry)
            carry = lax.fori_loop(0, jnp.where(masked, n_pairs, 0), pair, carry)

        par = rem(o, 2)

        @pl.when(between(o, PASS_D + 2, PASS_3 + 2) | between(o, PASS_B + 2, PASS_C + 2))
        def _():
            send_dq(rows_of(o - 2), 1 - par)

        @pl.when(between(o, PASS_2 + 2, PASS_2 + 8) | between(o, PASS_3 + 2, PASS_B + 2))
        def _():
            send_kv(block_of(o - 2), rem(kv_event(o - 2), N_BUF))

        @pl.when(between(o, PASS_D + 1, PASS_3 + 1) | between(o, PASS_B + 1, PASS_C + 1))
        def _():
            @pl.when(o > PASS_3)
            def _():
                wait_dq(par)
            stage_dq(rows_of(o - 1), par)

        @pl.when(between(o, PASS_2 + 1, PASS_2 + 7) | between(o, PASS_3 + 1, PASS_B + 1))
        def _():
            ev = kv_event(o - 1)

            @pl.when(ev >= N_BUF)
            def _():
                wait_kv(rem(ev, N_BUF))
            stage_kv(block_of(o - 1), rem(ev, N_BUF))
        return carry

    kb_p, rg_p = lax.fori_loop(0, N_OUTER, outer, (first_kb, jnp.int32(0)))
    with jax.named_scope('flush'):
        flush(kb_p, rg_p)

    send_dq(rows_of(jnp.int32(PASS_C - 1)), (N_OUTER - 1) % 2)

    def last_parts(i, c):
        @pl.when((i > 0) & (i < 5))
        def _():
            send_kv(first_kb + i - 1, rem(14 + i, N_BUF))

        @pl.when(i < 4)
        def _():
            wait_kv(rem(15 + i, N_BUF))
            stage_kv(first_kb + i, rem(15 + i, N_BUF))

        @pl.when(i > 1)
        def _():
            par = rem(i, 2)

            @pl.when(i < 4)
            def _():
                wait_dq(par)
                stage_dq(i - 2, par)

            @pl.when(i > 2)
            def _():
                send_dq(i - 3, 1 - par)
        return c
    lax.fori_loop(0, 5, last_parts, 0)

    for par in (0, 1):
        wait_dq(par)
    for buf in range(N_BUF):
        wait_kv(buf)
    with jax.named_scope('drain'):
        for m in range(1, N_DEV):
            for g in range(N_GRP):
                wait_local(st_v.at[m, g], rows_ss.at[m, g, 2])
                wait_local(q_v.at[m, g], rows_ss.at[m, g, 0])
                wait_local(do_v.at[m, g], rows_ss.at[m, g, 1])
            wait_local(k_v.at[pl.ds(0, KEYS_DEV), :], keys_ss.at[m, 0])
            wait_local(v_v.at[pl.ds(0, KEYS_DEV), :], keys_ss.at[m, 1])
            heads = pl.ds(0, GROUP)
            wait_local(dq_o.at[:, :, heads, :], dq_rs.at[m])
            wait_local(dk_o.at[:, 0, 0, :], kv_rs.at[m, 0])
            wait_local(dv_o.at[:, 0, 0, :], kv_rs.at[m, 1])


def solution(mesh):
    row_spec = P(None, CP_AXES, 'heads', None)
    stat_spec = P(None, CP_AXES, 'heads')
    key_spec = P(CP_AXES, 'heads', None)
    any_ = pl.BlockSpec(memory_space=pl.ANY)

    def local_grads(queries, attn_out, grad_out, log_sum_exp, key_cache, value_cache):
        row_delta = jnp.sum(grad_out.astype(F32) * attn_out.astype(F32), axis=-1)
        stats = jnp.stack([log_sum_exp * (-1.0 / SCALE), -row_delta], axis=0)
        stats = stats.reshape(2, N_GRP, 8, ROWS_DEV, N_DEV, GROUP)
        stats = jnp.transpose(stats, (4, 1, 0, 2, 3, 5)).reshape(N_DEV, N_GRP, 16, DIM)
        keys = jnp.transpose(key_cache, (1, 0, 2))
        values = jnp.transpose(value_cache, (1, 0, 2))
        dma = pltpu.SemaphoreType.DMA
        rows_shape = (N_DEV, N_GRP, 8, ROWS_DEV, GROUP, DIM)
        n_rg = N_DEV * N_GRP
        grad_query, grad_key, grad_value = pl.pallas_call(
            kernel,
            name='attn_bwd',
            out_shape=(jax.ShapeDtypeStruct((N_SLICES, ROWS_DEV, N_DEV * GROUP, DIM), BF16),
                       jax.ShapeDtypeStruct((KEYS_DEV, N_DEV, 1, DIM), F32),
                       jax.ShapeDtypeStruct((KEYS_DEV, N_DEV, 1, DIM), F32)),
            in_specs=[any_] * 5,
            out_specs=[any_] * 3,
            scratch_shapes=[
                pltpu.VMEM(rows_shape, BF16), pltpu.VMEM(rows_shape, BF16),
                pltpu.VMEM((n_rg, DIM, RB), BF16), pltpu.VMEM((n_rg, DIM, RB), BF16),
                pltpu.VMEM((N_DEV, N_GRP, 16, DIM), F32), pltpu.VMEM((N_DEV, N_GRP, DIM, DIM), BF16),
                pltpu.VMEM((KEYS, DIM), BF16), pltpu.VMEM((KEYS, DIM), BF16),
                pltpu.VMEM((n_rg, DIM, RB), F32),
                pltpu.VMEM((NKB, DIM, CB), F32), pltpu.VMEM((NKB, DIM, CB), F32),
                pltpu.VMEM((RB, CB), BF16), pltpu.VMEM((RB, CB), BF16),
                pltpu.VMEM((RB, CB), BF16), pltpu.VMEM((RB, CB), BF16),
                pltpu.VMEM((DIM, CB), jnp.int32),
                pltpu.VMEM((N_BUF, 2, CB, DIM), F32),
                pltpu.VMEM((2, N_GRP, 8, ROWS_DEV, GROUP, DIM), BF16),
                dma((N_DEV, N_GRP, 3)), dma((N_DEV, 2)), dma((N_DEV, N_GRP, 3)), dma((N_DEV, 2)),
                dma((N_BUF, 2)), dma((N_DEV, 2)), dma((2, N_GRP)), dma((N_DEV,)),
            ],
            compiler_params=pltpu.CompilerParams(collective_id=0, has_side_effects=True, vmem_limit_bytes=67043328),
        )(queries, grad_out, stats, keys, values)
        return grad_query, grad_key.reshape(KEYS_DEV, N_DEV, DIM), grad_value.reshape(KEYS_DEV, N_DEV, DIM)

    return jax.shard_map(local_grads, mesh=mesh, in_specs=(row_spec, row_spec, row_spec, stat_spec, key_spec, key_spec),
                         out_specs=(row_spec, key_spec, key_spec), check_vma=False)
```

```python
import functools
import math

import jax
import jax.numpy as jnp
from jax import lax
from jax.experimental import pallas as pl
from jax.experimental.pallas import tpu as pltpu
from jax.sharding import PartitionSpec as P

CP_AXES = ('cpo', 'cp')
MESH = pl.DeviceIdType.MESH
BF16 = jnp.bfloat16
F32 = jnp.float32

N_DEV = 8
N_SLICES = 24
ROWS_DEV = 8
GROUP = 16
DIM = 128
KEYS = 9728
KEYS_DEV = KEYS // N_DEV
PREFIX = 8192
N_GRP = 3
RB = 1024
CB = 512
NKB = KEYS // CB
CHUNK = 64
SCALE = DIM ** -0.5
EXP_SCALE = SCALE * math.log2(math.e)

UNROLL = 6
N_BUF = 3
N_DQ = 6

PASS_1, PASS_2, PASS_D, PASS_3, PASS_B, PASS_C, N_OUTER = 17, 23, 38, 40, 49, 53, 55


def dg(a, b, ca, cb):
    return lax.dot_general(a, b, (((ca,), (cb,)), ((), ())), preferred_element_type=F32)


def quo(a, b):
    return lax.div(a, jnp.int32(b))


def rem(a, b):
    return lax.rem(a, jnp.int32(b))


def pick(cond, a, b):
    return jnp.where(cond, jnp.int32(a), jnp.int32(b))


def xor3(a, b):
    out = jnp.int32(0)
    for bit in (1, 2, 4):
        out = out + bit * rem(rem(quo(a, bit), 2) + rem(quo(b, bit), 2), 2)
    return out


def kernel(q_h, do_h, st_h, k_h, v_h, dq_o, dkv_o,
           q_v, do_v, qt_v, dot_v, st_v, aug_v, k_v, v_v, dqt, dkt, dvt, p0, d0, p1, d1, x_v, okv, odq,
           rows_ss, keys_ss, rows_rs, keys_rs, kv_ss, kv_rs, dq_ss, dq_rs):
    me = lax.axis_index('cpo') * 4 + lax.axis_index('cp')
    chip = quo(me, 2)
    first_kb = 5 * chip
    chips = [chip] + [quo(xor3(me, jnp.int32(2 * i)), 2) for i in (1, 2, 3)]

    def dev(e):
        return {'cpo': quo(e, 4), 'cp': rem(e, 4)}

    barrier = pltpu.get_barrier_semaphore()
    for m in range(1, N_DEV):
        pl.semaphore_signal(barrier, inc=1, device_id=dev(xor3(me, jnp.int32(m))), device_id_type=MESH)

    def zero_keys(i, c):
        dkt[i] = jnp.zeros((DIM, CB), F32)
        dvt[i] = jnp.zeros((DIM, CB), F32)
        return c
    lax.fori_loop(0, NKB, zero_keys, 0)

    def zero_rows(i, c):
        dqt[i] = jnp.zeros((DIM, RB), F32)
        return c
    lax.fori_loop(0, N_DEV * N_GRP, zero_rows, 0)
    p1[...] = jnp.zeros((RB, CB), BF16)
    d1[...] = jnp.zeros((RB, CB), BF16)
    x_v[...] = (lax.broadcasted_iota(jnp.int32, (DIM, CB), 1)
                - lax.broadcasted_iota(jnp.int32, (DIM, CB), 0) // GROUP)

    with jax.named_scope('barrier'):
        pl.semaphore_wait(barrier, N_DEV - 1)

    def row_copies(m, g):
        e = xor3(me, jnp.int32(m))
        heads = pl.ds(pl.multiple_of(e * GROUP, GROUP), GROUP)
        pairs = ((st_h.at[e, g], st_v.at[m, g], 2),
                 (q_h.at[pl.ds(8 * g, 8), :, heads, :], q_v.at[m, g], 0),
                 (do_h.at[pl.ds(8 * g, 8), :, heads, :], do_v.at[m, g], 1))
        for src, dst, t in pairs:
            if m == 0:
                yield pltpu.make_async_copy(src, dst, rows_rs.at[m, g, t])
            else:
                yield pltpu.make_async_remote_copy(src, dst, rows_ss.at[m, g, t], rows_rs.at[m, g, t],
                                                   device_id=dev(e), device_id_type=MESH)

    def key_copies(e, m, local=False):
        rows = pl.ds(pl.multiple_of(me * KEYS_DEV, CHUNK), KEYS_DEV)
        for src, dst, t in ((k_h.at[e], k_v.at[rows, :], 0), (v_h.at[e], v_v.at[rows, :], 1)):
            if local:
                yield pltpu.make_async_copy(src, dst, keys_rs.at[m, t])
            else:
                yield pltpu.make_async_remote_copy(src, dst, keys_ss.at[m, t], keys_rs.at[m, t],
                                                   device_id=dev(e), device_id_type=MESH)

    for c in key_copies(me, jnp.int32(0), local=True):
        c.start()
    for c in key_copies(xor3(me, jnp.int32(1)), jnp.int32(1)):
        c.start()
    for g in range(N_GRP):
        for m in (0, 1):
            for c in row_copies(m, g):
                c.start()
    for ms in ((2, 4, 3, 5), (6, 7)):
        pairs = [list(key_copies(xor3(me, jnp.int32(m)), jnp.int32(m))) for m in ms]
        for t in (0, 1):
            for pair in pairs:
                pair[t].start()
    for ms in ((2, 4, 3, 5), (6, 7)):
        for g in range(N_GRP):
            for m in ms:
                for c in row_copies(m, g):
                    c.start()

    def keys_t(ref, kb):
        return jnp.concatenate([ref[pl.ds(pl.multiple_of(kb * CB + DIM * i, DIM), DIM), :] for i in range(CB // DIM)], axis=1)

    def tile(kb, m, g, kb_p, rg_p, p_ref, d_ref, pp_ref, dp_ref, masked):
        slice_of = lax.broadcasted_iota(jnp.int32, (DIM, DIM), 1) % 8
        part_row = lax.broadcasted_iota(jnp.int32, (DIM, CB), 0)
        pick_l = jnp.where(part_row < 24, 1.0, 0.0).astype(BF16)
        pick_d = jnp.where((part_row >= 24) & (part_row < 48), 1.0, 0.0).astype(BF16)
        rhs_s = jnp.concatenate([keys_t(k_v, kb), pick_l], axis=0)
        rhs_d = jnp.concatenate([keys_t(v_v, kb), pick_d], axis=0)
        stats = aug_v[m, g]
        limit = PREFIX + CB * g + ROWS_DEV * xor3(me, m) - CB * kb

        def lhs(ref, rc):
            zero = jnp.zeros((), BF16)
            aug = jnp.concatenate([jnp.where(slice_of == 2 * rc, stats, zero),
                                   jnp.where(slice_of == 2 * rc + 1, stats, zero)], axis=0)
            return jnp.concatenate([ref[m, g, pl.ds(2 * rc, 2)].reshape(256, DIM), aug], axis=1)

        def score(rc):
            return dg(lhs(q_v, rc), rhs_s, 1, 0)

        def grad(rc):
            return dg(lhs(do_v, rc), rhs_d, 1, 0)

        def finish(rc, s, dp):
            p = jnp.exp2(s * EXP_SCALE)
            if masked:
                p = jnp.concatenate([jnp.where(x_v[...] <= limit + 64 * (2 * rc), p[:DIM], 0.0),
                                     jnp.where(x_v[...] <= limit + 64 * (2 * rc + 1), p[DIM:], 0.0)], axis=0)
            rows = pl.ds(256 * rc, 256)
            p_ref[rows, :] = p.astype(BF16)
            d_ref[rows, :] = (p * dp).astype(BF16)

        def dq_half(h, k):
            cols = slice(256 * k, 256 * k + 256)
            return dg(keys_t(k_v, kb_p)[:, cols], dp_ref[512 * h:512 * h + 512, cols], 1, 1)

        def dv_part(i):
            return dg(dot_v[rg_p][:, 256 * i:256 * i + 256], pp_ref[256 * i:256 * i + 256, :], 1, 0)

        def dk_part(i):
            return dg(qt_v[rg_p][:, 256 * i:256 * i + 256], dp_ref[256 * i:256 * i + 256, :], 1, 0)

        def put_dq(h, x):
            dqt[rg_p, :, 512 * h:512 * h + 512] = x + dqt[rg_p, :, 512 * h:512 * h + 512]

        s = score(0)
        dq = dq_half(0, 0)
        dp = grad(0)
        finish(0, s, dp)
        put_dq(0, dq_half(0, 1) + dq)
        s = score(1)
        dv = dv_part(0)
        dv = dv_part(1) + dv
        dp = grad(1)
        finish(1, s, dp)
        dv = dv_part(2) + dv
        dv = dv_part(3) + dv
        dvt[kb_p] = dv + dvt[kb_p]
        s = score(2)
        dq = dq_half(1, 0)
        dp = grad(2)
        finish(2, s, dp)
        put_dq(1, dq_half(1, 1) + dq)
        s = score(3)
        dk = dk_part(0)
        dk = dk_part(1) + dk
        dp = grad(3)
        finish(3, s, dp)
        dk = dk_part(2) + dk
        dk = dk_part(3) + dk
        dkt[kb_p] = dk + dkt[kb_p]

    def flush(kb_p, rg_p):
        dvt[kb_p] += dg(dot_v[rg_p], p1[...], 1, 0)
        dkt[kb_p] += dg(qt_v[rg_p], d1[...], 1, 0)
        dqt[rg_p] += dg(keys_t(k_v, kb_p), d1[...], 1, 1)

    def wait_local(ref, sem):
        pltpu.make_async_copy(ref, ref, sem).wait()

    def prepare_rows(m, g):
        with jax.named_scope('w_rows'):
            wait_local(st_v.at[m, g], rows_rs.at[m, g, 2])
            wait_local(q_v.at[m, g], rows_rs.at[m, g, 0])
            wait_local(do_v.at[m, g], rows_rs.at[m, g, 1])
        rg = m * N_GRP + g
        x = st_v[m, g]
        hi = x.astype(BF16).astype(F32)
        mid = (x - hi).astype(BF16).astype(F32)
        lo = (x - hi) - mid
        parts = [y[8 * t:8 * t + 8] for t in (0, 1) for y in (hi, mid, lo)]
        aug_v[m, g] = jnp.concatenate(parts + [jnp.zeros((80, DIM), F32)], axis=0).T.astype(BF16)
        qt_v[rg] = q_v[m, g].reshape(RB, DIM).T
        dot_v[rg] = do_v[m, g].reshape(RB, DIM).T

    def wait_keys(k):
        with jax.named_scope('w_keys'):
            for core in (0, 1):
                e = 2 * k + core
                m = xor3(me, e)
                rows = pl.ds(pl.multiple_of(e * KEYS_DEV, CHUNK), KEYS_DEV)
                wait_local(k_v.at[rows, :], keys_rs.at[m, 0])
                wait_local(v_v.at[rows, :], keys_rs.at[m, 1])

    def prepare_keys(kb):
        for i in range(CB // DIM):
            rows = pl.ds(pl.multiple_of(kb * CB + DIM * i, DIM), DIM)
            k_v[rows, :] = k_v[rows, :].T
            v_v[rows, :] = v_v[rows, :].T

    def stage_dq(m, g, slot):
        with jax.named_scope('s_dq'):
            odq[slot] = (dqt[m * N_GRP + g].T * SCALE).astype(BF16).reshape(8, ROWS_DEV, GROUP, DIM)

    def send_dq(m, g, slot):
        e = xor3(me, m)
        dst = dq_o.at[pl.ds(pl.multiple_of(8 * g, 8), 8), :, pl.ds(pl.multiple_of(me * GROUP, GROUP), GROUP), :]

        @pl.when(m == 0)
        def _():
            pltpu.make_async_copy(odq.at[slot], dst, dq_ss.at[slot]).start()

        @pl.when(m != 0)
        def _():
            pltpu.make_async_remote_copy(odq.at[slot], dst, dq_ss.at[slot], dq_rs.at[m],
                                         device_id=dev(e), device_id_type=MESH).start()

    def stage_kv(kb, buf):
        with jax.named_scope('s_kv'):
            okv[buf, 0] = dkt[kb].T * SCALE
            okv[buf, 1] = dvt[kb].T

    def send_kv(kb, buf):
        n_dev = KEYS_DEV // CHUNK
        e_lo = quo(8 * kb, n_dev)

        def piece(j, c):
            ck = 8 * kb + j
            over = ck >= n_dev * (e_lo + 1)
            e = jnp.where(over, e_lo + 1, e_lo)
            off = pl.multiple_of(CHUNK * (ck - n_dev * e), CHUNK)
            m = xor3(me, e)
            src = okv.at[buf, :, pl.ds(pl.multiple_of(CHUNK * j, CHUNK), CHUNK), :]
            dst = dkv_o.at[:, pl.ds(off, CHUNK), me, 0, :]

            @pl.when(m == 0)
            def _():
                pltpu.make_async_copy(src, dst, kv_ss.at[buf]).start()

            @pl.when(m != 0)
            def _():
                pltpu.make_async_remote_copy(src, dst, kv_ss.at[buf], kv_rs.at[m],
                                             device_id=dev(e), device_id_type=MESH).start()
            return c
        lax.fori_loop(0, CB // CHUNK, piece, 0)

    def wait_kv(buf):
        with jax.named_scope('w_kv'):
            wait_local(okv.at[buf], kv_ss.at[buf])

    def wait_dq(slot):
        with jax.named_scope('w_dq'):
            wait_local(odq.at[slot], dq_ss.at[slot])

    def between(o, lo, hi):
        return (o >= lo) & (o < hi)

    def chip_at(d):
        return jnp.where(d == 0, chips[0], jnp.where(d == 1, chips[1], jnp.where(d == 2, chips[2], chips[3])))

    def block_at(i):
        return jnp.where(i < 16, 5 * chip_at(quo(i, 4)) + rem(i, 4), 5 * (i - 16) + 4)

    def block_of(o):
        n = jnp.where(o < PASS_2, o - PASS_1, jnp.where(o < PASS_D, o - PASS_2, o - PASS_3 + 6))
        n = jnp.clip(n, 0, 14)
        other = jnp.where(n < 12, 4 + 4 * rem(n, 3) + quo(n, 3), n + 4)
        return block_at(jnp.where(o < PASS_1, jnp.where(o < 2, o, o + 2), other))

    def rows_d(r):
        return 6 + rem(r, 2), quo(r, 2)

    def rows_b(r):
        return 2 + 2 * rem(r, 2) + quo(rem(r, 4), 2), quo(r, 4)

    def rows_at(o, r):
        d_m, d_g = rows_d(r)
        b_m, b_g = rows_b(r)
        return jnp.where(o < PASS_B, d_m, b_m), jnp.where(o < PASS_B, d_g, b_g)

    def done_dq(o, act):
        for lo, n, rows in ((PASS_D, 6, rows_d), (PASS_B, 12, rows_b)):
            for t in range(3):
                r = 3 * (o - lo) - 1 + t

                @pl.when((r >= 0) & (r < n))
                def _():
                    m, g = rows(r)
                    act(m, g, r + (0 if lo == PASS_D else 6))

    def done_kv(o, act):
        ev = jnp.where(o <= PASS_2 + 6, o - PASS_2 - 1, jnp.where(o <= PASS_B, 6 + o - PASS_3 - 1, 15 + o - PASS_C))

        @pl.when(between(o, PASS_2 + 1, PASS_2 + 7) | between(o, PASS_3 + 1, PASS_B + 1) | (o >= PASS_C))
        def _():
            act(jnp.where(o >= PASS_C, first_kb + o - PASS_C, block_of(o - 1)), rem(ev, N_BUF), ev)

    def outer(o, carry):
        ends = between(o, PASS_D, PASS_3) | between(o, PASS_B, PASS_C)
        last = o >= PASS_C
        kb = block_of(o)
        m_lo = pick(o < PASS_1, 0, pick(between(o, PASS_2, PASS_D), 6, 2))
        n_m = pick((o < PASS_1) | between(o, PASS_2, PASS_D), 2, 4)
        g_lo = jnp.maximum(kb - 16, 0)
        masked = jnp.where(ends | last, chip == 3, kb >= 16)
        n_full = jnp.where(ends, 2, jnp.where(last, 1, quo(n_m, 2)))
        it = jnp.where(o < PASS_B, o - PASS_D, o - PASS_B)
        skip = jnp.where(o < PASS_B, 6 * it, it * (it + 5))
        n_pairs = jnp.where(ends, jnp.where(o < PASS_B, 3 + 3 * it, 3 + it),
                            jnp.where(last, 2 - (o - PASS_C), (N_GRP - g_lo) * quo(n_m, 2)))
        first = (o == 0) | (o == PASS_1) | (o == PASS_2)

        done_dq(o - 1, lambda m, g, r: send_dq(m, g, rem(r, N_DQ)))
        done_kv(o - 1, lambda k, buf, ev: send_kv(k, buf))

        @pl.when(o == 0)
        def _():
            wait_keys(chip)

        d = quo(o + 2, 4)

        @pl.when((o >= 2) & (rem(o + 2, 4) == 0) & (d < 4))
        def _():
            wait_keys(chip_at(d))

        @pl.when(o < PASS_1)
        def _():
            prepare_keys(kb)

        @pl.when(o < 2)
        def _():
            prepare_keys(kb + 2)

        def index(n):
            e_m, e_g = rows_at(o, 3 * it + quo(n, 4))
            own = n + 6 * (o - PASS_C)
            g = jnp.where(ends, e_g, jnp.where(last, quo(own, 4), lax.div(n, n_m)))
            m = jnp.where(ends, e_m, jnp.where(last, rem(quo(own, 2), 2), m_lo + lax.rem(n, n_m)))
            k = jnp.where(ends, first_kb + rem(n, 4), jnp.where(last, first_kb + 2 + rem(n, 2), kb))
            return k, m, g

        def six(j, c):
            @pl.when(first)
            def _():
                def one(t, c):
                    _, m, g = index(UNROLL * j + t)
                    prepare_rows(m, g)
                    return c
                lax.fori_loop(0, UNROLL, one, 0)
            kb_p, rg_p = c
            for t in range(UNROLL):
                k, m, g = index(UNROLL * j + t)
                bufs = (p0, d0, p1, d1) if t % 2 == 0 else (p1, d1, p0, d0)
                tile(k, m, g, kb_p, rg_p, *bufs, False)
                kb_p, rg_p = k, m * N_GRP + g
            return kb_p, rg_p

        def index_masked(n):
            n2 = quo(n, 2)
            half = quo(n_m, 2)
            e = n + skip
            w = pick(o < PASS_B, 2, 4)
            a = e - 2 * w
            b = e - 5 * w
            e_r = jnp.where(a < 0, quo(e, 2), jnp.where(b < 0, w + quo(jnp.maximum(a, 0), 3), 2 * w + quo(jnp.maximum(b, 0), 4)))
            e_k = jnp.where(a < 0, rem(e, 2), jnp.where(b < 0, rem(jnp.maximum(a, 0), 3), rem(jnp.maximum(b, 0), 4)))
            e_m, e_g = rows_at(o, e_r)
            f = n + 4 * (o - PASS_C)
            f3 = rem(f, 3)
            g = jnp.where(ends, e_g, jnp.where(last, pick(f3 > 0, 2, 1), g_lo + lax.div(n2, half)))
            m = jnp.where(ends, e_m, jnp.where(last, quo(f, 3), m_lo + 2 * lax.rem(n2, half) + rem(n, 2)))
            k = jnp.where(ends, 15 + e_k, jnp.where(last, pick(f3 == 2, 18, 17), kb))
            return k, m, g

        def pair(j, c):
            kb_p, rg_p = c
            k_a, m_a, g_a = index_masked(2 * j)
            k_b, m_b, g_b = index_masked(2 * j + 1)
            tile(k_a, m_a, g_a, kb_p, rg_p, p0, d0, p1, d1, True)
            tile(k_b, m_b, g_b, k_a, m_a * N_GRP + g_a, p1, d1, p0, d0, True)
            return k_b, m_b * N_GRP + g_b

        with jax.named_scope('tiles'):
            carry = lax.fori_loop(0, jnp.where(masked, 0, n_full), six, carry)
            carry = lax.fori_loop(0, jnp.where(masked, n_pairs, 0), pair, carry)

        def put_kv(k, buf, ev):
            @pl.when(ev >= N_BUF)
            def _():
                wait_kv(buf)
            stage_kv(k, buf)
        done_kv(o, put_kv)

        def put_dq(m, g, r):
            @pl.when(r >= N_DQ)
            def _():
                wait_dq(rem(r, N_DQ))
            stage_dq(m, g, rem(r, N_DQ))
        done_dq(o, put_dq)
        return carry

    kb_p, rg_p = lax.fori_loop(0, N_OUTER, outer, (first_kb, jnp.int32(0)))
    done_kv(jnp.int32(N_OUTER - 1), lambda k, buf, ev: send_kv(k, buf))
    with jax.named_scope('flush'):
        flush(kb_p, rg_p)

    n_kv = 15 + N_OUTER - PASS_C
    for i in (0, 1):
        wait_kv((n_kv + i) % N_BUF)
        stage_kv(first_kb + 2 + i, (n_kv + i) % N_BUF)
    for r in range(2 * N_GRP):
        slot = (18 + r) % N_DQ
        wait_dq(slot)
        stage_dq(jnp.int32(1 - r % 2), jnp.int32(r // 2), slot)
        if r < 2:
            send_kv(first_kb + 2 + r, (n_kv + r) % N_BUF)
        if r > 0:
            send_dq(jnp.int32(1 - (r - 1) % 2), jnp.int32((r - 1) // 2), (17 + r) % N_DQ)
    send_dq(jnp.int32(0), jnp.int32(N_GRP - 1), (18 + 2 * N_GRP - 1) % N_DQ)

    for slot in range(N_DQ):
        wait_dq(slot)
    for buf in range(N_BUF):
        wait_kv(buf)
    with jax.named_scope('drain'):
        for m in range(1, N_DEV):
            for g in range(N_GRP):
                wait_local(st_v.at[m, g], rows_ss.at[m, g, 2])
                wait_local(q_v.at[m, g], rows_ss.at[m, g, 0])
                wait_local(do_v.at[m, g], rows_ss.at[m, g, 1])
            wait_local(k_v.at[pl.ds(0, KEYS_DEV), :], keys_ss.at[m, 0])
            wait_local(v_v.at[pl.ds(0, KEYS_DEV), :], keys_ss.at[m, 1])
            heads = pl.ds(0, GROUP)
            wait_local(dq_o.at[:, :, heads, :], dq_rs.at[m])
            wait_local(dkv_o.at[:, :, 0, 0, :], kv_rs.at[m])


def solution(mesh):
    row_spec = P(None, CP_AXES, 'heads', None)
    stat_spec = P(None, CP_AXES, 'heads')
    key_spec = P(CP_AXES, 'heads', None)
    any_ = pl.BlockSpec(memory_space=pl.ANY)

    def local_grads(queries, attn_out, grad_out, log_sum_exp, key_cache, value_cache):
        row_delta = jnp.sum(grad_out.astype(F32) * attn_out.astype(F32), axis=-1)
        stats = jnp.stack([log_sum_exp * (-1.0 / SCALE), -row_delta], axis=0)
        stats = stats.reshape(2, N_GRP, 8, ROWS_DEV, N_DEV, GROUP)
        stats = jnp.transpose(stats, (4, 1, 0, 2, 3, 5)).reshape(N_DEV, N_GRP, 16, DIM)
        keys = jnp.transpose(key_cache, (1, 0, 2))
        values = jnp.transpose(value_cache, (1, 0, 2))
        dma = pltpu.SemaphoreType.DMA
        rows_shape = (N_DEV, N_GRP, 8, ROWS_DEV, GROUP, DIM)
        n_rg = N_DEV * N_GRP
        grad_query, grad_keys = pl.pallas_call(
            kernel,
            name='attn_bwd',
            out_shape=(jax.ShapeDtypeStruct((N_SLICES, ROWS_DEV, N_DEV * GROUP, DIM), BF16),
                       jax.ShapeDtypeStruct((2, KEYS_DEV, N_DEV, 1, DIM), F32)),
            in_specs=[any_] * 5,
            out_specs=[any_] * 2,
            scratch_shapes=[
                pltpu.VMEM(rows_shape, BF16), pltpu.VMEM(rows_shape, BF16),
                pltpu.VMEM((n_rg, DIM, RB), BF16), pltpu.VMEM((n_rg, DIM, RB), BF16),
                pltpu.VMEM((N_DEV, N_GRP, 16, DIM), F32), pltpu.VMEM((N_DEV, N_GRP, DIM, DIM), BF16),
                pltpu.VMEM((KEYS, DIM), BF16), pltpu.VMEM((KEYS, DIM), BF16),
                pltpu.VMEM((n_rg, DIM, RB), F32),
                pltpu.VMEM((NKB, DIM, CB), F32), pltpu.VMEM((NKB, DIM, CB), F32),
                pltpu.VMEM((RB, CB), BF16), pltpu.VMEM((RB, CB), BF16),
                pltpu.VMEM((RB, CB), BF16), pltpu.VMEM((RB, CB), BF16),
                pltpu.VMEM((DIM, CB), jnp.int32),
                pltpu.VMEM((N_BUF, 2, CB, DIM), F32),
                pltpu.VMEM((N_DQ, 8, ROWS_DEV, GROUP, DIM), BF16),
                dma((N_DEV, N_GRP, 3)), dma((N_DEV, 2)), dma((N_DEV, N_GRP, 3)), dma((N_DEV, 2)),
                dma((N_BUF,)), dma((N_DEV,)), dma((N_DQ,)), dma((N_DEV,)),
            ],
            compiler_params=pltpu.CompilerParams(collective_id=0, has_side_effects=True, vmem_limit_bytes=67043328),
        )(queries, grad_out, stats, keys, values)
        grad_keys = grad_keys.reshape(2, KEYS_DEV, N_DEV, DIM)
        return grad_query, grad_keys[0], grad_keys[1]

    return jax.shard_map(local_grads, mesh=mesh, in_specs=(row_spec, row_spec, row_spec, stat_spec, key_spec, key_spec),
                         out_specs=(row_spec, key_spec, key_spec), check_vma=False)
```

```python
import functools
import math

import jax
import jax.numpy as jnp
from jax import lax
from jax.experimental import pallas as pl
from jax.experimental.pallas import tpu as pltpu
from jax.sharding import PartitionSpec as P

CP_AXES = ('cpo', 'cp')
MESH = pl.DeviceIdType.MESH
BF16 = jnp.bfloat16
F32 = jnp.float32

N_DEV = 8
N_SLICES = 24
ROWS_DEV = 8
GROUP = 16
DIM = 128
KEYS = 9728
KEYS_DEV = KEYS // N_DEV
PREFIX = 8192
N_GRP = 3
RB = 1024
CB = 512
NKB = KEYS // CB
CHUNK = 64
SCALE = DIM ** -0.5
EXP_SCALE = SCALE * math.log2(math.e)

UNROLL = 6
N_BUF = 3
N_DQ = 6

PASS_1, PASS_2, PASS_D, PASS_3, PASS_B, PASS_C, N_OUTER = 18, 24, 39, 41, 50, 54, 55


def dg(a, b, ca, cb):
    return lax.dot_general(a, b, (((ca,), (cb,)), ((), ())), preferred_element_type=F32)


def quo(a, b):
    return lax.div(a, jnp.int32(b))


def rem(a, b):
    return lax.rem(a, jnp.int32(b))


def pick(cond, a, b):
    return jnp.where(cond, jnp.int32(a), jnp.int32(b))


def xor3(a, b):
    out = jnp.int32(0)
    for bit in (1, 2, 4):
        out = out + bit * rem(rem(quo(a, bit), 2) + rem(quo(b, bit), 2), 2)
    return out


def kernel(q_h, do_h, o_h, l_h, k_h, v_h, dq_o, dkv_o,
           q_v, do_v, qt_v, dot_v, st_v, aug_v, k_v, v_v, dqt, dkt, dvt, p0, d0, p1, d1, x_v, okv, odq, nd_v,
           rows_ss, keys_ss, rows_rs, keys_rs, kv_ss, kv_rs, dq_ss, dq_rs):
    me = lax.axis_index('cpo') * 4 + lax.axis_index('cp')
    chip = quo(me, 2)
    first_kb = 5 * chip
    chips = [chip] + [quo(xor3(me, jnp.int32(2 * i)), 2) for i in (1, 2, 3)]

    def dev(e):
        return {'cpo': quo(e, 4), 'cp': rem(e, 4)}

    barrier = pltpu.get_barrier_semaphore()
    for m in range(1, N_DEV):
        pl.semaphore_signal(barrier, inc=1, device_id=dev(xor3(me, jnp.int32(m))), device_id_type=MESH)

    def zero_keys(i, c):
        dkt[i] = jnp.zeros((DIM, CB), F32)
        dvt[i] = jnp.zeros((DIM, CB), F32)
        return c
    lax.fori_loop(0, NKB, zero_keys, 0)

    def zero_rows(i, c):
        dqt[i] = jnp.zeros((DIM, RB), F32)
        return c
    lax.fori_loop(0, N_DEV * N_GRP, zero_rows, 0)
    p1[...] = jnp.zeros((RB, CB), BF16)
    d1[...] = jnp.zeros((RB, CB), BF16)
    x_v[...] = (lax.broadcasted_iota(jnp.int32, (DIM, CB), 1)
                - lax.broadcasted_iota(jnp.int32, (DIM, CB), 0) // GROUP)

    with jax.named_scope('barrier'):
        pl.semaphore_wait(barrier, N_DEV - 1)

    def row_copies(m, g):
        e = xor3(me, jnp.int32(m))
        heads = pl.ds(pl.multiple_of(e * GROUP, GROUP), GROUP)
        pairs = ((l_h.at[e, g], st_v.at[m, g, pl.ds(0, 8), :], 2),
                 (q_h.at[pl.ds(8 * g, 8), :, heads, :], q_v.at[m, g], 0),
                 (do_h.at[pl.ds(8 * g, 8), :, heads, :], do_v.at[m, g], 1))
        for src, dst, t in pairs:
            if m == 0:
                yield pltpu.make_async_copy(src, dst, rows_rs.at[m, g, t])
            else:
                yield pltpu.make_async_remote_copy(src, dst, rows_ss.at[m, g, t], rows_rs.at[m, g, t],
                                                   device_id=dev(e), device_id_type=MESH)

    def key_copies(e, m, local=False):
        rows = pl.ds(pl.multiple_of(me * KEYS_DEV, CHUNK), KEYS_DEV)
        for src, dst, t in ((k_h.at[e], k_v.at[rows, :], 0), (v_h.at[e], v_v.at[rows, :], 1)):
            if local:
                yield pltpu.make_async_copy(src, dst, keys_rs.at[m, t])
            else:
                yield pltpu.make_async_remote_copy(src, dst, keys_ss.at[m, t], keys_rs.at[m, t],
                                                   device_id=dev(e), device_id_type=MESH)

    for c in key_copies(me, jnp.int32(0), local=True):
        c.start()
    for c in key_copies(xor3(me, jnp.int32(1)), jnp.int32(1)):
        c.start()
    for g in range(N_GRP):
        for m in (0, 1):
            for c in row_copies(m, g):
                c.start()
    for ms in ((2, 4, 3, 5), (6, 7)):
        pairs = [list(key_copies(xor3(me, jnp.int32(m)), jnp.int32(m))) for m in ms]
        for t in (0, 1):
            for pair in pairs:
                pair[t].start()

    def block_copies(c):
        e = xor3(me, quo(c, N_GRP))
        src = (pl.ds(pl.multiple_of(8 * rem(c, N_GRP), 8), 8), slice(None), pl.ds(pl.multiple_of(e * GROUP, GROUP), GROUP), slice(None))
        for t, ref in ((0, o_h), (3, do_h)):
            slot = rem(c, 3) + t
            yield pltpu.make_async_copy(ref.at[src], odq.at[slot], dq_ss.at[slot])

    def delta(c, carry):
        @pl.when(c + 2 < N_DEV * N_GRP)
        def _():
            for copy in block_copies(c + 2):
                copy.start()
        for copy in block_copies(c):
            copy.wait()
        x = odq[rem(c, 3)].reshape(RB, DIM).astype(F32) * odq[rem(c, 3) + 3].reshape(RB, DIM).astype(F32)
        hi = x.astype(BF16)
        lo = (x - hi.astype(F32)).astype(BF16)
        row = lax.broadcasted_iota(jnp.int32, (16, 2 * DIM), 0)
        acc = None
        for i in range(8):
            one = jnp.where(row == i, 1.0, 0.0).astype(BF16)
            part = dg(one, jnp.concatenate([hi[DIM * i:DIM * i + DIM], lo[DIM * i:DIM * i + DIM]], axis=1), 1, 1)
            acc = part if acc is None else part + acc
        nd = 0.0 - acc[:8]
        m, g = quo(c, N_GRP), rem(c, N_GRP)
        nd_v[m, g] = nd

        @pl.when(m == 0)
        def _():
            st_v[0, g, 8:16, :] = nd
        return carry

    for c in (0, 1):
        for copy in block_copies(jnp.int32(c)):
            copy.start()
    with jax.named_scope('delta'):
        lax.fori_loop(0, N_DEV * N_GRP, delta, 0)
    for m in range(1, N_DEV):
        for g in range(N_GRP):
            pltpu.make_async_remote_copy(nd_v.at[m, g], st_v.at[m, g, pl.ds(8, 8), :], rows_ss.at[m, g, 3], rows_rs.at[m, g, 3],
                                         device_id=dev(xor3(me, jnp.int32(m))), device_id_type=MESH).start()
    for ms in ((2, 4, 3, 5), (6, 7)):
        for g in range(N_GRP):
            for m in ms:
                for c in row_copies(m, g):
                    c.start()

    def keys_t(ref, kb):
        return jnp.concatenate([ref[pl.ds(pl.multiple_of(kb * CB + DIM * i, DIM), DIM), :] for i in range(CB // DIM)], axis=1)

    def tile(kb, m, g, kb_p, rg_p, p_ref, d_ref, pp_ref, dp_ref, masked):
        slice_of = lax.broadcasted_iota(jnp.int32, (DIM, DIM), 1) % 8
        part_row = lax.broadcasted_iota(jnp.int32, (DIM, CB), 0)
        pick_l = jnp.where(part_row < 24, 1.0, 0.0).astype(BF16)
        pick_d = jnp.where((part_row >= 24) & (part_row < 48), 1.0, 0.0).astype(BF16)
        rhs_s = jnp.concatenate([keys_t(k_v, kb), pick_l], axis=0)
        rhs_d = jnp.concatenate([keys_t(v_v, kb), pick_d], axis=0)
        stats = aug_v[m, g]
        limit = PREFIX + CB * g + ROWS_DEV * xor3(me, m) - CB * kb

        def lhs(ref, rc):
            zero = jnp.zeros((), BF16)
            aug = jnp.concatenate([jnp.where(slice_of == 2 * rc, stats, zero),
                                   jnp.where(slice_of == 2 * rc + 1, stats, zero)], axis=0)
            return jnp.concatenate([ref[m, g, pl.ds(2 * rc, 2)].reshape(256, DIM), aug], axis=1)

        def score(rc):
            return dg(lhs(q_v, rc), rhs_s, 1, 0)

        def grad(rc):
            return dg(lhs(do_v, rc), rhs_d, 1, 0)

        def finish(rc, s, dp):
            p = jnp.exp2(s * EXP_SCALE)
            if masked:
                p = jnp.concatenate([jnp.where(x_v[...] <= limit + 64 * (2 * rc), p[:DIM], 0.0),
                                     jnp.where(x_v[...] <= limit + 64 * (2 * rc + 1), p[DIM:], 0.0)], axis=0)
            rows = pl.ds(256 * rc, 256)
            p_ref[rows, :] = p.astype(BF16)
            d_ref[rows, :] = (p * dp).astype(BF16)

        def dq_half(h, k):
            cols = slice(256 * k, 256 * k + 256)
            return dg(keys_t(k_v, kb_p)[:, cols], dp_ref[512 * h:512 * h + 512, cols], 1, 1)

        def dv_part(i):
            return dg(dot_v[rg_p][:, 256 * i:256 * i + 256], pp_ref[256 * i:256 * i + 256, :], 1, 0)

        def dk_part(i):
            return dg(qt_v[rg_p][:, 256 * i:256 * i + 256], dp_ref[256 * i:256 * i + 256, :], 1, 0)

        def put_dq(h, x):
            dqt[rg_p, :, 512 * h:512 * h + 512] = x + dqt[rg_p, :, 512 * h:512 * h + 512]

        s = score(0)
        dq = dq_half(0, 0)
        dp = grad(0)
        finish(0, s, dp)
        put_dq(0, dq_half(0, 1) + dq)
        s = score(1)
        dv = dv_part(0)
        dv = dv_part(1) + dv
        dp = grad(1)
        finish(1, s, dp)
        dv = dv_part(2) + dv
        dv = dv_part(3) + dv
        dvt[kb_p] = dv + dvt[kb_p]
        s = score(2)
        dq = dq_half(1, 0)
        dp = grad(2)
        finish(2, s, dp)
        put_dq(1, dq_half(1, 1) + dq)
        s = score(3)
        dk = dk_part(0)
        dk = dk_part(1) + dk
        dp = grad(3)
        finish(3, s, dp)
        dk = dk_part(2) + dk
        dk = dk_part(3) + dk
        dkt[kb_p] = dk + dkt[kb_p]

    def flush(kb_p, rg_p):
        dvt[kb_p] += dg(dot_v[rg_p], p1[...], 1, 0)
        dkt[kb_p] += dg(qt_v[rg_p], d1[...], 1, 0)
        dqt[rg_p] += dg(keys_t(k_v, kb_p), d1[...], 1, 1)

    def wait_local(ref, sem):
        pltpu.make_async_copy(ref, ref, sem).wait()

    def wait_rows(m, g):
        wait_local(st_v.at[m, g, pl.ds(0, 8), :], rows_rs.at[m, g, 2])
        wait_local(q_v.at[m, g], rows_rs.at[m, g, 0])
        wait_local(do_v.at[m, g], rows_rs.at[m, g, 1])

        @pl.when(m != 0)
        def _():
            wait_local(st_v.at[m, g, pl.ds(8, 8), :], rows_rs.at[m, g, 3])

    def prepare_rows(m, g):
        rg = m * N_GRP + g
        x = st_v[m, g]
        hi = x.astype(BF16).astype(F32)
        mid = (x - hi).astype(BF16).astype(F32)
        lo = (x - hi) - mid
        parts = [y[8 * t:8 * t + 8] for t in (0, 1) for y in (hi, mid, lo)]
        aug_v[m, g] = jnp.concatenate(parts + [jnp.zeros((80, DIM), F32)], axis=0).T.astype(BF16)
        qt_v[rg] = q_v[m, g].reshape(RB, DIM).T
        dot_v[rg] = do_v[m, g].reshape(RB, DIM).T

    def wait_keys(k):
        with jax.named_scope('w_keys'):
            for core in (0, 1):
                e = 2 * k + core
                m = xor3(me, e)
                rows = pl.ds(pl.multiple_of(e * KEYS_DEV, CHUNK), KEYS_DEV)
                wait_local(k_v.at[rows, :], keys_rs.at[m, 0])
                wait_local(v_v.at[rows, :], keys_rs.at[m, 1])

    def prepare_keys(kb):
        for i in range(CB // DIM):
            rows = pl.ds(pl.multiple_of(kb * CB + DIM * i, DIM), DIM)
            k_v[rows, :] = k_v[rows, :].T
            v_v[rows, :] = v_v[rows, :].T

    def stage_dq(m, g, slot):
        with jax.named_scope('s_dq'):
            odq[slot] = (dqt[m * N_GRP + g].T * SCALE).astype(BF16).reshape(8, ROWS_DEV, GROUP, DIM)

    def send_dq(m, g, slot):
        e = xor3(me, m)
        dst = dq_o.at[pl.ds(pl.multiple_of(8 * g, 8), 8), :, pl.ds(pl.multiple_of(me * GROUP, GROUP), GROUP), :]

        @pl.when(m == 0)
        def _():
            pltpu.make_async_copy(odq.at[slot], dst, dq_ss.at[slot]).start()

        @pl.when(m != 0)
        def _():
            pltpu.make_async_remote_copy(odq.at[slot], dst, dq_ss.at[slot], dq_rs.at[m],
                                         device_id=dev(e), device_id_type=MESH).start()

    def stage_kv(kb, buf):
        with jax.named_scope('s_kv'):
            okv[buf, 0] = dkt[kb].T * SCALE
            okv[buf, 1] = dvt[kb].T

    def send_kv(kb, buf):
        n_dev = KEYS_DEV // CHUNK
        e_lo = quo(8 * kb, n_dev)

        def piece(j, c):
            ck = 8 * kb + j
            over = ck >= n_dev * (e_lo + 1)
            e = jnp.where(over, e_lo + 1, e_lo)
            off = pl.multiple_of(CHUNK * (ck - n_dev * e), CHUNK)
            m = xor3(me, e)
            src = okv.at[buf, :, pl.ds(pl.multiple_of(CHUNK * j, CHUNK), CHUNK), :]
            dst = dkv_o.at[:, pl.ds(off, CHUNK), me, 0, :]

            @pl.when(m == 0)
            def _():
                pltpu.make_async_copy(src, dst, kv_ss.at[buf]).start()

            @pl.when(m != 0)
            def _():
                pltpu.make_async_remote_copy(src, dst, kv_ss.at[buf], kv_rs.at[m],
                                             device_id=dev(e), device_id_type=MESH).start()
            return c
        lax.fori_loop(0, CB // CHUNK, piece, 0)

    def wait_kv(buf):
        with jax.named_scope('w_kv'):
            wait_local(okv.at[buf], kv_ss.at[buf])

    def wait_dq(slot):
        with jax.named_scope('w_dq'):
            wait_local(odq.at[slot], dq_ss.at[slot])

    def between(o, lo, hi):
        return (o >= lo) & (o < hi)

    def chip_at(d):
        return jnp.where(d == 0, chips[0], jnp.where(d == 1, chips[1], jnp.where(d == 2, chips[2], chips[3])))

    def block_at(i):
        return jnp.where(i < 16, 5 * chip_at(quo(i, 4)) + rem(i, 4), 5 * (i - 16) + 4)

    def block_of(o):
        n = jnp.where(o < PASS_2, o - PASS_1, jnp.where(o < PASS_D, o - PASS_2, o - PASS_3 + 6))
        n = jnp.clip(n, 0, 14)
        other = jnp.where(n < 12, 4 + 4 * rem(n, 3) + quo(n, 3), n + 4)
        return block_at(jnp.where(o < PASS_1, jnp.where(o < 3, o, o + 1), other))

    def rows_d(r):
        return 6 + rem(r, 2), quo(r, 2)

    def rows_b(r):
        return 2 + 2 * rem(r, 2) + quo(rem(r, 4), 2), quo(r, 4)

    def rows_at(o, r):
        d_m, d_g = rows_d(r)
        b_m, b_g = rows_b(r)
        return jnp.where(o < PASS_B, d_m, b_m), jnp.where(o < PASS_B, d_g, b_g)

    def done_dq(o, act):
        for lo, n, rows in ((PASS_D, 6, rows_d), (PASS_B, 12, rows_b)):
            for t in range(3):
                r = 3 * (o - lo) - 1 + t

                @pl.when((r >= 0) & (r < n))
                def _():
                    m, g = rows(r)
                    act(m, g, r + (0 if lo == PASS_D else 6))

    def done_kv(o, act):
        ev = jnp.where(o <= PASS_2 + 6, o - PASS_2 - 1, jnp.where(o <= PASS_B, 6 + o - PASS_3 - 1, 15 + o - PASS_C))

        @pl.when(between(o, PASS_2 + 1, PASS_2 + 7) | between(o, PASS_3 + 1, PASS_B + 1) | (o >= PASS_C))
        def _():
            act(jnp.where(o >= PASS_C, first_kb + o - PASS_C, block_of(o - 1)), rem(ev, N_BUF), ev)

    def outer(o, carry):
        ends = between(o, PASS_D, PASS_3) | between(o, PASS_B, PASS_C)
        last = o >= PASS_C
        kb = block_of(o)
        m_lo = pick(o < PASS_1, 0, pick(between(o, PASS_2, PASS_D), 6, 2))
        n_m = pick((o < PASS_1) | between(o, PASS_2, PASS_D), 2, 4)
        g_lo = jnp.maximum(kb - 16, 0)
        masked = jnp.where(ends | last, chip == 3, kb >= 16)
        n_full = jnp.where(ends, 2, jnp.where(last, 1, quo(n_m, 2)))
        it = jnp.where(o < PASS_B, o - PASS_D, o - PASS_B)
        skip = jnp.where(o < PASS_B, 6 * it, it * (it + 5))
        n_pairs = jnp.where(ends, jnp.where(o < PASS_B, 3 + 3 * it, 3 + it),
                            jnp.where(last, 1, (N_GRP - g_lo) * quo(n_m, 2)))
        first = (o == 0) | (o == PASS_1) | (o == PASS_2)

        done_dq(o - 1, lambda m, g, r: send_dq(m, g, rem(r, N_DQ)))
        done_kv(o - 1, lambda k, buf, ev: send_kv(k, buf))

        @pl.when(o == 0)
        def _():
            wait_keys(chip)

        d = quo(o + 1, 4)

        @pl.when((rem(o + 1, 4) == 0) & (d < 4))
        def _():
            wait_keys(chip_at(d))

        @pl.when(o < PASS_1)
        def _():
            prepare_keys(kb)

        @pl.when(o == 0)
        def _():
            prepare_keys(kb + 3)

        def index(n):
            e_m, e_g = rows_at(o, 3 * it + quo(n, 4))
            g = jnp.where(ends, e_g, jnp.where(last, quo(n, 2), lax.div(n, n_m)))
            m = jnp.where(ends, e_m, jnp.where(last, rem(n, 2), m_lo + lax.rem(n, n_m)))
            k = jnp.where(ends, first_kb + rem(n, 4), jnp.where(last, first_kb + 3, kb))
            return k, m, g

        def six(fresh, j, c):
            if fresh:
                def one(t, c):
                    _, m, g = index(UNROLL * j + t)
                    wait_rows(m, g)
                    return c
                with jax.named_scope('w_rows'):
                    lax.fori_loop(0, UNROLL, one, 0)
            kb_p, rg_p = c
            for t in range(UNROLL):
                k, m, g = index(UNROLL * j + t)
                if fresh:
                    prepare_rows(m, g)
                bufs = (p0, d0, p1, d1) if t % 2 == 0 else (p1, d1, p0, d0)
                tile(k, m, g, kb_p, rg_p, *bufs, False)
                kb_p, rg_p = k, m * N_GRP + g
            return kb_p, rg_p

        def index_masked(n):
            n2 = quo(n, 2)
            half = quo(n_m, 2)
            e = n + skip
            w = pick(o < PASS_B, 2, 4)
            a = e - 2 * w
            b = e - 5 * w
            e_r = jnp.where(a < 0, quo(e, 2), jnp.where(b < 0, w + quo(jnp.maximum(a, 0), 3), 2 * w + quo(jnp.maximum(b, 0), 4)))
            e_k = jnp.where(a < 0, rem(e, 2), jnp.where(b < 0, rem(jnp.maximum(a, 0), 3), rem(jnp.maximum(b, 0), 4)))
            e_m, e_g = rows_at(o, e_r)
            g = jnp.where(ends, e_g, jnp.where(last, 2, g_lo + lax.div(n2, half)))
            m = jnp.where(ends, e_m, jnp.where(last, n, m_lo + 2 * lax.rem(n2, half) + rem(n, 2)))
            k = jnp.where(ends, 15 + e_k, jnp.where(last, 18, kb))
            return k, m, g

        def pair(j, c):
            kb_p, rg_p = c
            k_a, m_a, g_a = index_masked(2 * j)
            k_b, m_b, g_b = index_masked(2 * j + 1)
            tile(k_a, m_a, g_a, kb_p, rg_p, p0, d0, p1, d1, True)
            tile(k_b, m_b, g_b, k_a, m_a * N_GRP + g_a, p1, d1, p0, d0, True)
            return k_b, m_b * N_GRP + g_b

        with jax.named_scope('tiles'):
            carry = lax.fori_loop(0, jnp.where(first, n_full, 0), functools.partial(six, True), carry)
            carry = lax.fori_loop(0, jnp.where(first | masked, 0, n_full), functools.partial(six, False), carry)
            carry = lax.fori_loop(0, jnp.where(masked, n_pairs, 0), pair, carry)

        def put_kv(k, buf, ev):
            @pl.when(ev >= N_BUF)
            def _():
                wait_kv(buf)
            stage_kv(k, buf)
        done_kv(o, put_kv)

        def put_dq(m, g, r):
            @pl.when(r >= N_DQ)
            def _():
                wait_dq(rem(r, N_DQ))
            stage_dq(m, g, rem(r, N_DQ))
        done_dq(o, put_dq)
        return carry

    kb_p, rg_p = lax.fori_loop(0, N_OUTER, outer, (first_kb, jnp.int32(0)))
    done_dq(jnp.int32(N_OUTER - 1), lambda m, g, r: send_dq(m, g, rem(r, N_DQ)))
    done_kv(jnp.int32(N_OUTER - 1), lambda k, buf, ev: send_kv(k, buf))
    with jax.named_scope('flush'):
        flush(kb_p, rg_p)

    for r in range(2 * N_GRP):
        slot = (18 + r) % N_DQ
        if r < 3:
            wait_kv((16 + r) % N_BUF)
            stage_kv(first_kb + 1 + r, (16 + r) % N_BUF)
        wait_dq(slot)
        stage_dq(jnp.int32(1 - r % 2), jnp.int32(r // 2), slot)
        if r < 3:
            send_kv(first_kb + 1 + r, (16 + r) % N_BUF)
        if r > 0:
            send_dq(jnp.int32(1 - (r - 1) % 2), jnp.int32((r - 1) // 2), (17 + r) % N_DQ)
    send_dq(jnp.int32(0), jnp.int32(N_GRP - 1), (18 + 2 * N_GRP - 1) % N_DQ)

    for slot in range(N_DQ):
        wait_dq(slot)
    for buf in range(N_BUF):
        wait_kv(buf)
    with jax.named_scope('drain'):
        for m in range(1, N_DEV):
            for g in range(N_GRP):
                wait_local(st_v.at[m, g, pl.ds(0, 8), :], rows_ss.at[m, g, 2])
                wait_local(nd_v.at[m, g], rows_ss.at[m, g, 3])
                wait_local(q_v.at[m, g], rows_ss.at[m, g, 0])
                wait_local(do_v.at[m, g], rows_ss.at[m, g, 1])
            wait_local(k_v.at[pl.ds(0, KEYS_DEV), :], keys_ss.at[m, 0])
            wait_local(v_v.at[pl.ds(0, KEYS_DEV), :], keys_ss.at[m, 1])
            heads = pl.ds(0, GROUP)
            wait_local(dq_o.at[:, :, heads, :], dq_rs.at[m])
            wait_local(dkv_o.at[:, :, 0, 0, :], kv_rs.at[m])


def solution(mesh):
    row_spec = P(None, CP_AXES, 'heads', None)
    stat_spec = P(None, CP_AXES, 'heads')
    key_spec = P(CP_AXES, 'heads', None)
    any_ = pl.BlockSpec(memory_space=pl.ANY)

    def local_grads(queries, attn_out, grad_out, log_sum_exp, key_cache, value_cache):
        lse = (log_sum_exp * (-1.0 / SCALE)).reshape(N_GRP, 8, ROWS_DEV, N_DEV, GROUP)
        lse = jnp.transpose(lse, (3, 0, 1, 2, 4)).reshape(N_DEV, N_GRP, 8, DIM)
        keys = jnp.transpose(key_cache, (1, 0, 2))
        values = jnp.transpose(value_cache, (1, 0, 2))
        dma = pltpu.SemaphoreType.DMA
        rows_shape = (N_DEV, N_GRP, 8, ROWS_DEV, GROUP, DIM)
        n_rg = N_DEV * N_GRP
        grad_query, grad_keys = pl.pallas_call(
            kernel,
            name='attn_bwd',
            out_shape=(jax.ShapeDtypeStruct((N_SLICES, ROWS_DEV, N_DEV * GROUP, DIM), BF16),
                       jax.ShapeDtypeStruct((2, KEYS_DEV, N_DEV, 1, DIM), F32)),
            in_specs=[any_] * 6,
            out_specs=[any_] * 2,
            scratch_shapes=[
                pltpu.VMEM(rows_shape, BF16), pltpu.VMEM(rows_shape, BF16),
                pltpu.VMEM((n_rg, DIM, RB), BF16), pltpu.VMEM((n_rg, DIM, RB), BF16),
                pltpu.VMEM((N_DEV, N_GRP, 16, DIM), F32), pltpu.VMEM((N_DEV, N_GRP, DIM, DIM), BF16),
                pltpu.VMEM((KEYS, DIM), BF16), pltpu.VMEM((KEYS, DIM), BF16),
                pltpu.VMEM((n_rg, DIM, RB), F32),
                pltpu.VMEM((NKB, DIM, CB), F32), pltpu.VMEM((NKB, DIM, CB), F32),
                pltpu.VMEM((RB, CB), BF16), pltpu.VMEM((RB, CB), BF16),
                pltpu.VMEM((RB, CB), BF16), pltpu.VMEM((RB, CB), BF16),
                pltpu.VMEM((DIM, CB), jnp.int32),
                pltpu.VMEM((N_BUF, 2, CB, DIM), F32),
                pltpu.VMEM((N_DQ, 8, ROWS_DEV, GROUP, DIM), BF16),
                pltpu.VMEM((N_DEV, N_GRP, 8, DIM), F32),
                dma((N_DEV, N_GRP, 4)), dma((N_DEV, 2)), dma((N_DEV, N_GRP, 4)), dma((N_DEV, 2)),
                dma((N_BUF,)), dma((N_DEV,)), dma((N_DQ,)), dma((N_DEV,)),
            ],
            compiler_params=pltpu.CompilerParams(collective_id=0, has_side_effects=True, vmem_limit_bytes=67043328),
        )(queries, grad_out, attn_out, lse, keys, values)
        grad_keys = grad_keys.reshape(2, KEYS_DEV, N_DEV, DIM)
        return grad_query, grad_keys[0], grad_keys[1]

    return jax.shard_map(local_grads, mesh=mesh, in_specs=(row_spec, row_spec, row_spec, stat_spec, key_spec, key_spec),
                         out_specs=(row_spec, key_spec, key_spec), check_vma=False)
```

```python
import functools
import math

import jax
import jax.numpy as jnp
from jax import lax
from jax.experimental import pallas as pl
from jax.experimental.pallas import tpu as pltpu
from jax.sharding import PartitionSpec as P

CP_AXES = ('cpo', 'cp')
MESH = pl.DeviceIdType.MESH
BF16 = jnp.bfloat16
F32 = jnp.float32

N_DEV = 8
N_SLICES = 24
ROWS_DEV = 8
GROUP = 16
DIM = 128
KEYS = 9728
KEYS_DEV = KEYS // N_DEV
PREFIX = 8192
N_GRP = 3
RB = 1024
CB = 512
NKB = KEYS // CB
CHUNK = 64
SCALE = DIM ** -0.5
EXP_SCALE = SCALE * math.log2(math.e)

UNROLL = 6
N_BUF = 3
N_DQ = 12
N_OUTER = 53
AHEAD = 5


def dg(a, b, ca, cb):
    return lax.dot_general(a, b, (((ca,), (cb,)), ((), ())), preferred_element_type=F32)


def quo(a, b):
    return lax.div(a, jnp.int32(b))


def rem(a, b):
    return lax.rem(a, jnp.int32(b))


def pick(cond, a, b):
    return jnp.where(cond, jnp.int32(a), jnp.int32(b))


def xor3(a, b):
    out = jnp.int32(0)
    for bit in (1, 2, 4):
        out = out + bit * rem(rem(quo(a, bit), 2) + rem(quo(b, bit), 2), 2)
    return out


def kernel(q_h, do_h, o_h, l_h, k_h, v_h, dq_o, dkv_o,
           q_v, do_v, qt_v, dot_v, st_v, aug_v, k_v, v_v, dqt, dkt, dvt, p0, d0, p1, d1, x_v, okv, odq, nd_v,
           rows_ss, keys_ss, rows_rs, keys_rs, kv_ss, kv_rs, dq_ss, dq_rs):
    me = lax.axis_index('cpo') * 4 + lax.axis_index('cp')
    chip = quo(me, 2)
    first_kb = 5 * chip
    chips = [chip] + [quo(xor3(me, jnp.int32(2 * i)), 2) for i in (1, 2, 3)]

    edge = chip == 3
    edge_at = 3 - chip
    n_own = pick(edge, 2, 3)
    n_units = pick(edge, 15, 13)
    pass_1 = n_own + n_units
    pass_2 = pass_1 + 6
    pass_d = pass_2 + n_units
    pass_3 = pass_d + 2
    pass_b = pass_3 + n_units - 6
    pass_c = pass_b + 4
    n_outer = pass_c + pick(edge, 0, 1)

    def dev(e):
        return {'cpo': quo(e, 4), 'cp': rem(e, 4)}

    barrier = pltpu.get_barrier_semaphore()
    for m in range(1, N_DEV):
        pl.semaphore_signal(barrier, inc=1, device_id=dev(xor3(me, jnp.int32(m))), device_id_type=MESH)

    def zero_keys(i, c):
        dkt[i] = jnp.zeros((DIM, CB), F32)
        dvt[i] = jnp.zeros((DIM, CB), F32)
        return c
    lax.fori_loop(0, NKB, zero_keys, 0)

    def zero_rows(i, c):
        dqt[i] = jnp.zeros((DIM, RB), F32)
        return c
    lax.fori_loop(0, N_DEV * N_GRP, zero_rows, 0)
    p1[...] = jnp.zeros((RB, CB), BF16)
    d1[...] = jnp.zeros((RB, CB), BF16)
    x_v[...] = (lax.broadcasted_iota(jnp.int32, (DIM, CB), 1)
                - lax.broadcasted_iota(jnp.int32, (DIM, CB), 0) // GROUP)

    with jax.named_scope('barrier'):
        pl.semaphore_wait(barrier, N_DEV - 1)

    def row_copies(m, g):
        e = xor3(me, jnp.int32(m))
        heads = pl.ds(pl.multiple_of(e * GROUP, GROUP), GROUP)
        pairs = ((l_h.at[e, g], st_v.at[m, g, pl.ds(0, 8), :], 2),
                 (q_h.at[pl.ds(8 * g, 8), :, heads, :], q_v.at[m, g], 0),
                 (do_h.at[pl.ds(8 * g, 8), :, heads, :], do_v.at[m, g], 1))
        for src, dst, t in pairs:
            if m == 0:
                yield pltpu.make_async_copy(src, dst, rows_rs.at[m, g, t])
            else:
                yield pltpu.make_async_remote_copy(src, dst, rows_ss.at[m, g, t], rows_rs.at[m, g, t],
                                                   device_id=dev(e), device_id_type=MESH)

    def key_copies(e, m, local=False):
        rows = pl.ds(pl.multiple_of(me * KEYS_DEV, CHUNK), KEYS_DEV)
        for src, dst, t in ((k_h.at[e], k_v.at[rows, :], 0), (v_h.at[e], v_v.at[rows, :], 1)):
            if local:
                yield pltpu.make_async_copy(src, dst, keys_rs.at[m, t])
            else:
                yield pltpu.make_async_remote_copy(src, dst, keys_ss.at[m, t], keys_rs.at[m, t],
                                                   device_id=dev(e), device_id_type=MESH)

    for c in key_copies(me, jnp.int32(0), local=True):
        c.start()
    for c in key_copies(xor3(me, jnp.int32(1)), jnp.int32(1)):
        c.start()
    for g in range(N_GRP):
        for m in (0, 1):
            for c in row_copies(m, g):
                c.start()
    for ms in ((2, 4, 3, 5), (6, 7)):
        pairs = [list(key_copies(xor3(me, jnp.int32(m)), jnp.int32(m))) for m in ms]
        for t in (0, 1):
            for pair in pairs:
                pair[t].start()

    def block_copies(c):
        e = xor3(me, quo(c, N_GRP))
        src = (pl.ds(pl.multiple_of(8 * rem(c, N_GRP), 8), 8), slice(None), pl.ds(pl.multiple_of(e * GROUP, GROUP), GROUP), slice(None))
        for t, ref in ((0, o_h), (6, do_h)):
            slot = rem(c, 6) + t
            yield pltpu.make_async_copy(ref.at[src], odq.at[slot], dq_ss.at[slot])

    def delta(c, carry):
        @pl.when(c + AHEAD < N_DEV * N_GRP)
        def _():
            for copy in block_copies(c + AHEAD):
                copy.start()
        for copy in block_copies(c):
            copy.wait()
        x = odq[rem(c, 6)].reshape(RB, DIM).astype(F32) * odq[rem(c, 6) + 6].reshape(RB, DIM).astype(F32)
        hi = x.astype(BF16)
        lo = (x - hi.astype(F32)).astype(BF16)
        row = lax.broadcasted_iota(jnp.int32, (16, 2 * DIM), 0)
        acc = None
        for i in range(8):
            one = jnp.where(row == i, 1.0, 0.0).astype(BF16)
            part = dg(one, jnp.concatenate([hi[DIM * i:DIM * i + DIM], lo[DIM * i:DIM * i + DIM]], axis=1), 1, 1)
            acc = part if acc is None else part + acc
        nd = 0.0 - acc[:8]
        m, g = quo(c, N_GRP), rem(c, N_GRP)
        nd_v[m, g] = nd

        @pl.when(m == 0)
        def _():
            st_v[0, g, 8:16, :] = nd
        return carry

    for c in range(AHEAD):
        for copy in block_copies(jnp.int32(c)):
            copy.start()
    with jax.named_scope('delta'):
        lax.fori_loop(0, N_DEV * N_GRP, delta, 0)
    for m in range(1, N_DEV):
        for g in range(N_GRP):
            pltpu.make_async_remote_copy(nd_v.at[m, g], st_v.at[m, g, pl.ds(8, 8), :], rows_ss.at[m, g, 3], rows_rs.at[m, g, 3],
                                         device_id=dev(xor3(me, jnp.int32(m))), device_id_type=MESH).start()
    for ms in ((2, 4, 3, 5), (6, 7)):
        for g in range(N_GRP):
            for m in ms:
                for c in row_copies(m, g):
                    c.start()

    def keys_t(ref, kb):
        return jnp.concatenate([ref[pl.ds(pl.multiple_of(kb * CB + DIM * i, DIM), DIM), :] for i in range(CB // DIM)], axis=1)

    def tile(kb, m, g, kb_p, rg_p, bufs, diagonal=False, diagonal_p=False, fill=False):
        p_ref, d_ref, pp_ref, dp_ref = bufs
        slice_of = lax.broadcasted_iota(jnp.int32, (DIM, DIM), 1) % 8
        part_row = lax.broadcasted_iota(jnp.int32, (DIM, CB), 0)
        pick_l = jnp.where(part_row < 24, 1.0, 0.0).astype(BF16)
        pick_d = jnp.where((part_row >= 24) & (part_row < 48), 1.0, 0.0).astype(BF16)
        rhs_s = jnp.concatenate([keys_t(k_v, kb), pick_l], axis=0)
        rhs_d = jnp.concatenate([keys_t(v_v, kb), pick_d], axis=0)
        stats = aug_v[m, g]

        def width(rc):
            return 256 if diagonal and rc < 2 else CB

        def lhs(ref, rc):
            zero = jnp.zeros((), BF16)
            aug = jnp.concatenate([jnp.where(slice_of == 2 * rc, stats, zero),
                                   jnp.where(slice_of == 2 * rc + 1, stats, zero)], axis=0)
            return jnp.concatenate([ref[m, g, pl.ds(2 * rc, 2)].reshape(256, DIM), aug], axis=1)

        def score(rc):
            return dg(lhs(q_v, rc), rhs_s[:, :width(rc)], 1, 0)

        def grad(rc):
            return dg(lhs(do_v, rc), rhs_d[:, :width(rc)], 1, 0)

        def finish(rc, s, dp):
            w = width(rc)
            p = jnp.exp2(s * EXP_SCALE)
            if diagonal:
                limit = ROWS_DEV * xor3(me, m)
                p = jnp.concatenate([jnp.where(x_v[:, :w] <= limit + 64 * (2 * rc), p[:DIM], 0.0),
                                     jnp.where(x_v[:, :w] <= limit + 64 * (2 * rc + 1), p[DIM:], 0.0)], axis=0)
            rows = slice(256 * rc, 256 * rc + 256)
            p_ref[rows, :w] = p.astype(BF16)
            d_ref[rows, :w] = (p * dp).astype(BF16)
            if fill and w < CB:
                p_ref[rows, w:] = jnp.zeros((256, CB - w), BF16)
                d_ref[rows, w:] = jnp.zeros((256, CB - w), BF16)

        def dq_half(h, k):
            cols = slice(256 * k, 256 * k + 256)
            return dg(keys_t(k_v, kb_p)[:, cols], dp_ref[512 * h:512 * h + 512, cols], 1, 1)

        def part(ref, x_ref, i, w=CB):
            return dg(ref[rg_p][:, 256 * i:256 * i + 256], x_ref[256 * i:256 * i + 256, :w], 1, 0)

        def put_dq(h, x):
            dqt[rg_p, :, 512 * h:512 * h + 512] = x + dqt[rg_p, :, 512 * h:512 * h + 512]

        def put_keys(ref, low, full):
            if low is None:
                ref[kb_p] = full + ref[kb_p]
            else:
                ref[kb_p, :, :256] = low + full[:, :256] + ref[kb_p, :, :256]
                ref[kb_p, :, 256:] = full[:, 256:] + ref[kb_p, :, 256:]

        def keys_sum(ref, x_ref):
            if diagonal_p:
                low = part(ref, x_ref, 0, 256)
                yield None
                low = part(ref, x_ref, 1, 256) + low
                yield None
                full = part(ref, x_ref, 2)
                yield None
                yield low, part(ref, x_ref, 3) + full
            else:
                full = part(ref, x_ref, 0)
                for i in (1, 2):
                    yield None
                    full = part(ref, x_ref, i) + full
                yield None
                yield None, part(ref, x_ref, 3) + full

        s = score(0)
        dq = dq_half(0, 0)
        dp = grad(0)
        finish(0, s, dp)
        put_dq(0, dq if diagonal_p else dq_half(0, 1) + dq)
        s = score(1)
        dv = keys_sum(dot_v, pp_ref)
        next(dv)
        next(dv)
        dp = grad(1)
        finish(1, s, dp)
        next(dv)
        put_keys(dvt, *next(dv))
        s = score(2)
        dq = dq_half(1, 0)
        dp = grad(2)
        finish(2, s, dp)
        put_dq(1, dq_half(1, 1) + dq)
        s = score(3)
        dk = keys_sum(qt_v, dp_ref)
        next(dk)
        next(dk)
        dp = grad(3)
        finish(3, s, dp)
        next(dk)
        put_keys(dkt, *next(dk))

    def flush(kb_p, rg_p):
        dvt[kb_p] += dg(dot_v[rg_p], p1[...], 1, 0)
        dkt[kb_p] += dg(qt_v[rg_p], d1[...], 1, 0)
        dqt[rg_p] += dg(keys_t(k_v, kb_p), d1[...], 1, 1)

    def wait_local(ref, sem):
        pltpu.make_async_copy(ref, ref, sem).wait()

    def wait_rows(m, g):
        wait_local(st_v.at[m, g, pl.ds(0, 8), :], rows_rs.at[m, g, 2])
        wait_local(q_v.at[m, g], rows_rs.at[m, g, 0])
        wait_local(do_v.at[m, g], rows_rs.at[m, g, 1])

        @pl.when(m != 0)
        def _():
            wait_local(st_v.at[m, g, pl.ds(8, 8), :], rows_rs.at[m, g, 3])

    def prepare_rows(m, g):
        rg = m * N_GRP + g
        x = st_v[m, g]
        hi = x.astype(BF16).astype(F32)
        mid = (x - hi).astype(BF16).astype(F32)
        lo = (x - hi) - mid
        parts = [y[8 * t:8 * t + 8] for t in (0, 1) for y in (hi, mid, lo)]
        aug_v[m, g] = jnp.concatenate(parts + [jnp.zeros((80, DIM), F32)], axis=0).T.astype(BF16)
        qt_v[rg] = q_v[m, g].reshape(RB, DIM).T
        dot_v[rg] = do_v[m, g].reshape(RB, DIM).T

    def wait_keys(k):
        with jax.named_scope('w_keys'):
            for core in (0, 1):
                e = 2 * k + core
                m = xor3(me, e)
                rows = pl.ds(pl.multiple_of(e * KEYS_DEV, CHUNK), KEYS_DEV)
                wait_local(k_v.at[rows, :], keys_rs.at[m, 0])
                wait_local(v_v.at[rows, :], keys_rs.at[m, 1])

    def prepare_keys(kb):
        for i in range(CB // DIM):
            rows = pl.ds(pl.multiple_of(kb * CB + DIM * i, DIM), DIM)
            k_v[rows, :] = k_v[rows, :].T
            v_v[rows, :] = v_v[rows, :].T

    def stage_dq(m, g, slot):
        with jax.named_scope('s_dq'):
            odq[slot] = (dqt[m * N_GRP + g].T * SCALE).astype(BF16).reshape(8, ROWS_DEV, GROUP, DIM)

    def send_dq(m, g, slot):
        e = xor3(me, m)
        dst = dq_o.at[pl.ds(pl.multiple_of(8 * g, 8), 8), :, pl.ds(pl.multiple_of(me * GROUP, GROUP), GROUP), :]

        @pl.when(m == 0)
        def _():
            pltpu.make_async_copy(odq.at[slot], dst, dq_ss.at[slot]).start()

        @pl.when(m != 0)
        def _():
            pltpu.make_async_remote_copy(odq.at[slot], dst, dq_ss.at[slot], dq_rs.at[m],
                                         device_id=dev(e), device_id_type=MESH).start()

    def stage_kv(kb, buf):
        with jax.named_scope('s_kv'):
            okv[buf, 0] = dkt[kb].T * SCALE
            okv[buf, 1] = dvt[kb].T

    def send_kv(kb, buf):
        n_dev = KEYS_DEV // CHUNK
        e_lo = quo(8 * kb, n_dev)

        def piece(j, c):
            ck = 8 * kb + j
            over = ck >= n_dev * (e_lo + 1)
            e = jnp.where(over, e_lo + 1, e_lo)
            off = pl.multiple_of(CHUNK * (ck - n_dev * e), CHUNK)
            m = xor3(me, e)
            src = okv.at[buf, :, pl.ds(pl.multiple_of(CHUNK * j, CHUNK), CHUNK), :]
            dst = dkv_o.at[:, pl.ds(off, CHUNK), me, 0, :]

            @pl.when(m == 0)
            def _():
                pltpu.make_async_copy(src, dst, kv_ss.at[buf]).start()

            @pl.when(m != 0)
            def _():
                pltpu.make_async_remote_copy(src, dst, kv_ss.at[buf], kv_rs.at[m],
                                             device_id=dev(e), device_id_type=MESH).start()
            return c
        lax.fori_loop(0, CB // CHUNK, piece, 0)

    def wait_kv(buf):
        with jax.named_scope('w_kv'):
            wait_local(okv.at[buf], kv_ss.at[buf])

    def wait_dq(slot):
        with jax.named_scope('w_dq'):
            wait_local(odq.at[slot], dq_ss.at[slot])

    def between(o, lo, hi):
        return (o >= lo) & (o < hi)

    def chip_at(d):
        return jnp.where(d == 0, chips[0], jnp.where(d == 1, chips[1], jnp.where(d == 2, chips[2], chips[3])))

    from_2 = pick(edge_at == 1, 2, 4)
    from_3 = from_2 + pick(edge_at == 2, 2, 4)
    from_4 = from_3 + pick(edge_at == 3, 2, 4)

    def block_0(o):
        j = o - n_own
        d = pick(j >= from_3, 3, pick(j >= from_2, 2, 1))
        i = j - jnp.where(j >= from_3, from_3, jnp.where(j >= from_2, from_2, 0))
        kb = jnp.where(j >= from_4, 5 * (j - from_4) + 4, 5 * chip_at(d) + i)
        return jnp.where(j < 0, first_kb + o, kb)

    def unit(n):
        rest = jnp.maximum(n - 6, 0)
        one = pick(edge_at == 1, 2, 1)
        two = pick(edge_at == 3, 2, 3)
        turn = edge | (n < 6)
        d = jnp.where(turn, 1 + rem(n, 3), jnp.where(rem(rest, 2) == 0, one, two))
        i = jnp.where(turn, quo(n, 3), 2 + quo(rest, 2))
        n_whole = n_units - 3
        return jnp.where(n >= n_whole, 5 * (n - n_whole) + 4, 5 * chip_at(d) + i)

    def rows_d(r):
        return 6 + rem(r, 2), quo(r, 2)

    def rows_b(r):
        return 2 + 2 * rem(r, 2) + quo(rem(r, 4), 2), quo(r, 4)

    def rows_at(o, r):
        d_m, d_g = rows_d(r)
        b_m, b_g = rows_b(r)
        return jnp.where(o < pass_b, d_m, b_m), jnp.where(o < pass_b, d_g, b_g)

    def done_dq(o, act):
        @pl.when(o >= pass_d)
        def _():
            in_d = o <= pass_3
            base = jnp.where(in_d, pass_d, pass_b)
            n = pick(in_d, 6, 11)

            def one(t, c):
                r = 3 * (o - base) - 1 + t

                @pl.when((r >= 0) & (r < n))
                def _():
                    d_m, d_g = rows_d(r)
                    b_m, b_g = rows_b(r)
                    act(jnp.where(in_d, d_m, b_m), jnp.where(in_d, d_g, b_g), r + pick(in_d, 0, 6))
                return c
            lax.fori_loop(0, 3, one, 0)

    n_early = pick(edge, 6, 8)
    at_edge = edge_at + 2

    def done_kv(o, act):
        early = between(o, pass_2 + 1, pass_2 + 1 + n_early)

        @pl.when(early | between(o, pass_3 + 1, pass_b + 1))
        def _():
            e = o - pass_2 - 1
            at = jnp.where(edge | (e < at_edge), e, jnp.where(e < at_edge + 3, at_edge, e - 2))
            add = jnp.where(edge | (e < at_edge) | (e >= at_edge + 3), 0, e - at_edge)
            kb = jnp.where(early, unit(at) + add, unit(jnp.maximum(o - pass_3, 0) + 5))
            act(kb, jnp.where(early, e, n_early + o - pass_3 - 1))

    def put_kv(kb, ev):
        @pl.when(ev >= N_BUF)
        def _():
            wait_kv(rem(ev, N_BUF))
        stage_kv(kb, rem(ev, N_BUF))

    def put_dq(m, g, slot):
        wait_dq(slot)
        stage_dq(m, g, slot)

    def outer(o, carry):
        ends = between(o, pass_d, pass_3) | between(o, pass_b, pass_c)
        last = o >= pass_c
        n = jnp.where(o < pass_2, o - pass_1, jnp.where(o < pass_d, o - pass_2, o - pass_3 + 6))
        kb = jnp.where(o < pass_1, block_0(o), unit(jnp.clip(n, 0, n_units - 1)))
        cut = kb == 16
        m_lo = pick(o < pass_1, 0, pick(between(o, pass_2, pass_d), 6, 2))
        n_m = pick((o < pass_1) | between(o, pass_2, pass_d), 2, 4)
        it = jnp.where(o < pass_b, o - pass_d, o - pass_b)
        w = pick(o < pass_b, 2, 4)
        n_six = jnp.where(ends, pick(edge, 1, 2), jnp.where(last, pick(o == pass_c, 1, 0), quo(n_m, 2)))
        n_diag = jnp.where(ends, pick(edge & (it < quo(w, 2)), 1, 0), jnp.where(last, 0, jnp.where(cut, quo(n_m, 2), 0)))
        first = (o == 0) | (o == pass_1) | (o == pass_2)

        done_dq(o - 1, lambda m, g, ev: send_dq(m, g, rem(ev, N_DQ)))
        done_kv(o - 1, lambda k, ev: send_kv(k, rem(ev, N_BUF)))

        @pl.when(o < pass_1)
        def _():
            @pl.when(o == 0)
            def _():
                wait_keys(chip)
                for i in (1, 2, 3):
                    prepare_keys(first_kb + i)
            j = o - n_own

            @pl.when((j == 0) | (j == from_2) | (j == from_3))
            def _():
                wait_keys(chip_at(pick(j == from_3, 3, pick(j == from_2, 2, 1))))

            @pl.when((o == 0) | (j >= 0))
            def _():
                prepare_keys(kb)

            @pl.when(cut & (j >= 0))
            def _():
                prepare_keys(kb + 1)
                prepare_keys(kb + 2)

        def index(n):
            f = lax.div(n, n_m)
            k = jnp.where(cut, pick(f == 2, 17, 16), kb)
            m = m_lo + lax.rem(n, n_m)
            g = jnp.where(cut, pick(f == 0, 1, 2), f)
            e_r = 3 * it + quo(n, 4)
            e_k = first_kb + rem(n, 4)
            e = 6 * it + n
            e_a = jnp.maximum(e - w, 0)
            e_b = jnp.maximum(e - 3 * w, 0)
            x_r = jnp.where(e < w, e, jnp.where(e < 3 * w, w + quo(e_a, 2), 2 * w + quo(e_b, 3)))
            x_k = 15 + jnp.where(e < w, 0, jnp.where(e < 3 * w, rem(e_a, 2), rem(e_b, 3)))
            e_m, e_g = rows_at(o, jnp.where(edge, x_r, e_r))
            k = jnp.where(ends, jnp.where(edge, x_k, e_k), jnp.where(last, first_kb + 3, k))
            m = jnp.where(ends, e_m, jnp.where(last, rem(n, 2), m))
            g = jnp.where(ends, e_g, jnp.where(last, quo(n, 2), g))
            return k, m, g

        def index_diag(n):
            e_m, e_g = rows_at(o, 6 * it + n)
            g = jnp.where(ends, e_g, lax.div(n, n_m))
            m = jnp.where(ends, e_m, m_lo + lax.rem(n, n_m))
            return 16 + g, m, g

        def six(fresh, diagonal, j, c):
            if fresh:
                def one(t, c):
                    _, m, g = index(UNROLL * j + t)
                    wait_rows(m, g)
                    return c
                with jax.named_scope('w_rows'):
                    lax.fori_loop(0, UNROLL, one, 0)
            kb_p, rg_p = c
            for t in range(UNROLL):
                k, m, g = (index_diag if diagonal else index)(UNROLL * j + t)
                if fresh:
                    prepare_rows(m, g)
                bufs = (p0, d0, p1, d1) if t % 2 == 0 else (p1, d1, p0, d0)
                tile(k, m, g, kb_p, rg_p, bufs, diagonal, diagonal and t > 0, diagonal and t == UNROLL - 1)
                kb_p, rg_p = k, m * N_GRP + g
            return kb_p, rg_p

        with jax.named_scope('tiles'):
            carry = lax.fori_loop(0, jnp.where(first, n_six, 0), functools.partial(six, True, False), carry)
            carry = lax.fori_loop(0, jnp.where(first, 0, n_six), functools.partial(six, False, False), carry)
            carry = lax.fori_loop(0, n_diag, functools.partial(six, False, True), carry)

        done_kv(o, put_kv)

        def put(m, g, ev):
            @pl.when(ev >= N_DQ)
            def _():
                wait_dq(rem(ev, N_DQ))
            stage_dq(m, g, rem(ev, N_DQ))
        done_dq(o, put)
        return carry

    kb_p, rg_p = lax.fori_loop(0, N_OUTER, outer, (first_kb, jnp.int32(0)))
    done_dq(n_outer - 1, lambda m, g, ev: send_dq(m, g, rem(ev, N_DQ)))
    with jax.named_scope('flush'):
        flush(kb_p, rg_p)

    m_l, g_l = rows_b(jnp.int32(11))
    put_dq(m_l, g_l, 17 % N_DQ)
    for i in range(4):
        put_kv(first_kb + i, jnp.int32(15 + i))
        if i == 0:
            send_dq(m_l, g_l, 17 % N_DQ)
        else:
            send_kv(first_kb + i - 1, (14 + i) % N_BUF)
    own = [(jnp.int32(m), jnp.int32(g), (18 + 3 * (1 - m) + g) % N_DQ) for m in (1, 0) for g in range(N_GRP)]
    for r, (m, g, slot) in enumerate(own):
        put_dq(m, g, slot)
        if r == 0:
            send_kv(first_kb + 3, 18 % N_BUF)
        else:
            send_dq(*own[r - 1])
    send_dq(*own[-1])

    for slot in range(N_DQ):
        wait_dq(slot)
    for buf in range(N_BUF):
        wait_kv(buf)
    with jax.named_scope('drain'):
        for m in range(1, N_DEV):
            for g in range(N_GRP):
                wait_local(st_v.at[m, g, pl.ds(0, 8), :], rows_ss.at[m, g, 2])
                wait_local(nd_v.at[m, g], rows_ss.at[m, g, 3])
                wait_local(q_v.at[m, g], rows_ss.at[m, g, 0])
                wait_local(do_v.at[m, g], rows_ss.at[m, g, 1])
            wait_local(k_v.at[pl.ds(0, KEYS_DEV), :], keys_ss.at[m, 0])
            wait_local(v_v.at[pl.ds(0, KEYS_DEV), :], keys_ss.at[m, 1])
            heads = pl.ds(0, GROUP)
            wait_local(dq_o.at[:, :, heads, :], dq_rs.at[m])
            wait_local(dkv_o.at[:, :, 0, 0, :], kv_rs.at[m])


def solution(mesh):
    row_spec = P(None, CP_AXES, 'heads', None)
    stat_spec = P(None, CP_AXES, 'heads')
    key_spec = P(CP_AXES, 'heads', None)
    any_ = pl.BlockSpec(memory_space=pl.ANY)

    def local_grads(queries, attn_out, grad_out, log_sum_exp, key_cache, value_cache):
        lse = (log_sum_exp * (-1.0 / SCALE)).reshape(N_GRP, 8, ROWS_DEV, N_DEV, GROUP)
        lse = jnp.transpose(lse, (3, 0, 1, 2, 4)).reshape(N_DEV, N_GRP, 8, DIM)
        keys = jnp.transpose(key_cache, (1, 0, 2))
        values = jnp.transpose(value_cache, (1, 0, 2))
        dma = pltpu.SemaphoreType.DMA
        rows_shape = (N_DEV, N_GRP, 8, ROWS_DEV, GROUP, DIM)
        n_rg = N_DEV * N_GRP
        grad_query, grad_keys = pl.pallas_call(
            kernel,
            name='attn_bwd',
            out_shape=(jax.ShapeDtypeStruct((N_SLICES, ROWS_DEV, N_DEV * GROUP, DIM), BF16),
                       jax.ShapeDtypeStruct((2, KEYS_DEV, N_DEV, 1, DIM), F32)),
            in_specs=[any_] * 6,
            out_specs=[any_] * 2,
            scratch_shapes=[
                pltpu.VMEM(rows_shape, BF16), pltpu.VMEM(rows_shape, BF16),
                pltpu.VMEM((n_rg, DIM, RB), BF16), pltpu.VMEM((n_rg, DIM, RB), BF16),
                pltpu.VMEM((N_DEV, N_GRP, 16, DIM), F32), pltpu.VMEM((N_DEV, N_GRP, DIM, DIM), BF16),
                pltpu.VMEM((KEYS, DIM), BF16), pltpu.VMEM((KEYS, DIM), BF16),
                pltpu.VMEM((n_rg, DIM, RB), F32),
                pltpu.VMEM((NKB, DIM, CB), F32), pltpu.VMEM((NKB, DIM, CB), F32),
                pltpu.VMEM((RB, CB), BF16), pltpu.VMEM((RB, CB), BF16),
                pltpu.VMEM((RB, CB), BF16), pltpu.VMEM((RB, CB), BF16),
                pltpu.VMEM((DIM, CB), jnp.int32),
                pltpu.VMEM((N_BUF, 2, CB, DIM), F32),
                pltpu.VMEM((N_DQ, 8, ROWS_DEV, GROUP, DIM), BF16),
                pltpu.VMEM((N_DEV, N_GRP, 8, DIM), F32),
                dma((N_DEV, N_GRP, 4)), dma((N_DEV, 2)), dma((N_DEV, N_GRP, 4)), dma((N_DEV, 2)),
                dma((N_BUF,)), dma((N_DEV,)), dma((N_DQ,)), dma((N_DEV,)),
            ],
            compiler_params=pltpu.CompilerParams(collective_id=0, has_side_effects=True, vmem_limit_bytes=67043328),
        )(queries, grad_out, attn_out, lse, keys, values)
        grad_keys = grad_keys.reshape(2, KEYS_DEV, N_DEV, DIM)
        return grad_query, grad_keys[0], grad_keys[1]

    return jax.shard_map(local_grads, mesh=mesh, in_specs=(row_spec, row_spec, row_spec, stat_spec, key_spec, key_spec),
                         out_specs=(row_spec, key_spec, key_spec), check_vma=False)
```

```python
import functools
import math

import jax
import jax.numpy as jnp
from jax import lax
from jax.experimental import pallas as pl
from jax.experimental.pallas import tpu as pltpu
from jax.sharding import PartitionSpec as P

CP_AXES = ('cpo', 'cp')
MESH = pl.DeviceIdType.MESH
BF16 = jnp.bfloat16
F32 = jnp.float32

N_DEV = 8
N_SLICES = 24
ROWS_DEV = 8
GROUP = 16
DIM = 128
KEYS = 9728
KEYS_DEV = KEYS // N_DEV
PREFIX = 8192
N_GRP = 3
RB = 1024
CB = 512
NKB = KEYS // CB
CHUNK = 64
SCALE = DIM ** -0.5
EXP_SCALE = SCALE * math.log2(math.e)

UNROLL = 6
N_BUF = 3
N_DQ = 12
N_OUTER = 53
AHEAD = 5


def dg(a, b, ca, cb):
    return lax.dot_general(a, b, (((ca,), (cb,)), ((), ())), preferred_element_type=F32)


def quo(a, b):
    return lax.div(a, jnp.int32(b))


def rem(a, b):
    return lax.rem(a, jnp.int32(b))


def pick(cond, a, b):
    return jnp.where(cond, jnp.int32(a), jnp.int32(b))


def xor3(a, b):
    out = jnp.int32(0)
    for bit in (1, 2, 4):
        out = out + bit * rem(rem(quo(a, bit), 2) + rem(quo(b, bit), 2), 2)
    return out


def kernel(q_h, do_h, o_h, l_h, k_h, v_h, dq_o, dkv_o,
           q_v, do_v, qt_v, dot_v, st_v, aug_v, k_v, v_v, dqt, dkt, dvt, p0, d0, p1, d1, x_v, okv, odq, nd_v,
           rows_ss, keys_ss, rows_rs, keys_rs, kv_ss, kv_rs, dq_ss, dq_rs):
    me = lax.axis_index('cpo') * 4 + lax.axis_index('cp')
    chip = quo(me, 2)
    first_kb = 5 * chip
    chips = [chip] + [quo(xor3(me, jnp.int32(2 * i)), 2) for i in (1, 2, 3)]

    edge = chip == 3
    edge_at = 3 - chip
    n_own = pick(edge, 2, 3)
    n_units = pick(edge, 15, 13)
    pass_1 = n_own + n_units
    pass_2 = pass_1 + 6
    pass_d = pass_2 + n_units
    pass_3 = pass_d + 2
    pass_b = pass_3 + n_units - 6
    pass_c = pass_b + 4
    n_outer = pass_c + pick(edge, 0, 1)

    def dev(e):
        return {'cpo': quo(e, 4), 'cp': rem(e, 4)}

    barrier = pltpu.get_barrier_semaphore()
    for m in range(1, N_DEV):
        pl.semaphore_signal(barrier, inc=1, device_id=dev(xor3(me, jnp.int32(m))), device_id_type=MESH)

    def zero_keys(i, c):
        dkt[i] = jnp.zeros((DIM, CB), F32)
        dvt[i] = jnp.zeros((DIM, CB), F32)
        return c
    lax.fori_loop(0, NKB, zero_keys, 0)

    def zero_rows(i, c):
        dqt[i] = jnp.zeros((DIM, RB), F32)
        return c
    lax.fori_loop(0, N_DEV * N_GRP, zero_rows, 0)
    p1[...] = jnp.zeros((RB, CB), BF16)
    d1[...] = jnp.zeros((RB, CB), BF16)
    x_v[...] = (lax.broadcasted_iota(jnp.int32, (DIM, CB), 1)
                - lax.broadcasted_iota(jnp.int32, (DIM, CB), 0) // GROUP)

    with jax.named_scope('barrier'):
        pl.semaphore_wait(barrier, N_DEV - 1)

    def row_copies(m, g):
        e = xor3(me, jnp.int32(m))
        heads = pl.ds(pl.multiple_of(e * GROUP, GROUP), GROUP)
        pairs = ((l_h.at[e, g], st_v.at[m, g, pl.ds(0, 8), :], 2),
                 (q_h.at[pl.ds(8 * g, 8), :, heads, :], q_v.at[m, g], 0),
                 (do_h.at[pl.ds(8 * g, 8), :, heads, :], do_v.at[m, g], 1))
        for src, dst, t in pairs:
            if m == 0:
                yield pltpu.make_async_copy(src, dst, rows_rs.at[m, g, t])
            else:
                yield pltpu.make_async_remote_copy(src, dst, rows_ss.at[m, g, t], rows_rs.at[m, g, t],
                                                   device_id=dev(e), device_id_type=MESH)

    def key_copies(e, m, local=False):
        rows = pl.ds(pl.multiple_of(me * KEYS_DEV, CHUNK), KEYS_DEV)
        for src, dst, t in ((k_h.at[e], k_v.at[rows, :], 0), (v_h.at[e], v_v.at[rows, :], 1)):
            if local:
                yield pltpu.make_async_copy(src, dst, keys_rs.at[m, t])
            else:
                yield pltpu.make_async_remote_copy(src, dst, keys_ss.at[m, t], keys_rs.at[m, t],
                                                   device_id=dev(e), device_id_type=MESH)

    for c in key_copies(me, jnp.int32(0), local=True):
        c.start()
    for c in key_copies(xor3(me, jnp.int32(1)), jnp.int32(1)):
        c.start()
    for g in range(N_GRP):
        for m in (0, 1):
            for c in row_copies(m, g):
                c.start()
    for ms in ((2, 4, 3, 5), (6, 7)):
        pairs = [list(key_copies(xor3(me, jnp.int32(m)), jnp.int32(m))) for m in ms]
        for t in (0, 1):
            for pair in pairs:
                pair[t].start()

    def block_copies(c):
        e = xor3(me, quo(c, N_GRP))
        src = (pl.ds(pl.multiple_of(8 * rem(c, N_GRP), 8), 8), slice(None), pl.ds(pl.multiple_of(e * GROUP, GROUP), GROUP), slice(None))
        for t, ref in ((0, o_h), (6, do_h)):
            slot = rem(c, 6) + t
            yield pltpu.make_async_copy(ref.at[src], odq.at[slot], dq_ss.at[slot])

    def delta(c, carry):
        @pl.when(c + AHEAD < N_DEV * N_GRP)
        def _():
            for copy in block_copies(c + AHEAD):
                copy.start()
        for copy in block_copies(c):
            copy.wait()
        x = odq[rem(c, 6)].reshape(RB, DIM).astype(F32) * odq[rem(c, 6) + 6].reshape(RB, DIM).astype(F32)
        hi = x.astype(BF16)
        lo = (x - hi.astype(F32)).astype(BF16)
        row = lax.broadcasted_iota(jnp.int32, (16, 2 * DIM), 0)
        acc = None
        for i in range(8):
            one = jnp.where(row == i, 1.0, 0.0).astype(BF16)
            part = dg(one, jnp.concatenate([hi[DIM * i:DIM * i + DIM], lo[DIM * i:DIM * i + DIM]], axis=1), 1, 1)
            acc = part if acc is None else part + acc
        nd = 0.0 - acc[:8]
        m, g = quo(c, N_GRP), rem(c, N_GRP)
        nd_v[m, g] = nd

        @pl.when(m == 0)
        def _():
            st_v[0, g, 8:16, :] = nd
        return carry

    for c in range(AHEAD):
        for copy in block_copies(jnp.int32(c)):
            copy.start()
    with jax.named_scope('delta'):
        lax.fori_loop(0, N_DEV * N_GRP, delta, 0)
    for m in range(1, N_DEV):
        for g in range(N_GRP):
            pltpu.make_async_remote_copy(nd_v.at[m, g], st_v.at[m, g, pl.ds(8, 8), :], rows_ss.at[m, g, 3], rows_rs.at[m, g, 3],
                                         device_id=dev(xor3(me, jnp.int32(m))), device_id_type=MESH).start()
    for ms in ((2, 4, 3, 5), (6, 7)):
        for g in range(N_GRP):
            for m in ms:
                for c in row_copies(m, g):
                    c.start()

    def keys_t(ref, kb):
        return jnp.concatenate([ref[pl.ds(pl.multiple_of(kb * CB + DIM * i, DIM), DIM), :] for i in range(CB // DIM)], axis=1)

    def tile(kb, m, g, kb_p, rg_p, bufs, diagonal=False, diagonal_p=False, fill=False):
        p_ref, d_ref, pp_ref, dp_ref = bufs
        slice_of = lax.broadcasted_iota(jnp.int32, (DIM, DIM), 1) % 8
        part_row = lax.broadcasted_iota(jnp.int32, (DIM, CB), 0)
        pick_l = jnp.where(part_row < 24, 1.0, 0.0).astype(BF16)
        pick_d = jnp.where((part_row >= 24) & (part_row < 48), 1.0, 0.0).astype(BF16)
        rhs_s = jnp.concatenate([keys_t(k_v, kb), pick_l], axis=0)
        rhs_d = jnp.concatenate([keys_t(v_v, kb), pick_d], axis=0)
        stats = aug_v[m, g]

        def width(rc):
            return 256 if diagonal and rc < 2 else CB

        def lhs(ref, rc):
            zero = jnp.zeros((), BF16)
            aug = jnp.concatenate([jnp.where(slice_of == 2 * rc, stats, zero),
                                   jnp.where(slice_of == 2 * rc + 1, stats, zero)], axis=0)
            return jnp.concatenate([ref[m, g, pl.ds(2 * rc, 2)].reshape(256, DIM), aug], axis=1)

        def score(rc):
            return dg(lhs(q_v, rc), rhs_s[:, :width(rc)], 1, 0)

        def grad(rc):
            return dg(lhs(do_v, rc), rhs_d[:, :width(rc)], 1, 0)

        def finish(rc, s, dp):
            w = width(rc)
            p = jnp.exp2(s * EXP_SCALE)
            if diagonal:
                limit = ROWS_DEV * xor3(me, m)
                p = jnp.concatenate([jnp.where(x_v[:, :w] <= limit + 64 * (2 * rc), p[:DIM], 0.0),
                                     jnp.where(x_v[:, :w] <= limit + 64 * (2 * rc + 1), p[DIM:], 0.0)], axis=0)
            rows = slice(256 * rc, 256 * rc + 256)
            p_ref[rows, :w] = p.astype(BF16)
            d_ref[rows, :w] = (p * dp).astype(BF16)
            if fill and w < CB:
                p_ref[rows, w:] = jnp.zeros((256, CB - w), BF16)
                d_ref[rows, w:] = jnp.zeros((256, CB - w), BF16)

        def dq_half(h, k):
            cols = slice(256 * k, 256 * k + 256)
            return dg(keys_t(k_v, kb_p)[:, cols], dp_ref[512 * h:512 * h + 512, cols], 1, 1)

        def part(ref, x_ref, i, w=CB):
            return dg(ref[rg_p][:, 256 * i:256 * i + 256], x_ref[256 * i:256 * i + 256, :w], 1, 0)

        def put_dq(h, x):
            dqt[rg_p, :, 512 * h:512 * h + 512] = x + dqt[rg_p, :, 512 * h:512 * h + 512]

        def put_keys(ref, low, full):
            if low is None:
                ref[kb_p] = full + ref[kb_p]
            else:
                ref[kb_p, :, :256] = low + full[:, :256] + ref[kb_p, :, :256]
                ref[kb_p, :, 256:] = full[:, 256:] + ref[kb_p, :, 256:]

        def keys_sum(ref, x_ref):
            if diagonal_p:
                low = part(ref, x_ref, 0, 256)
                yield None
                low = part(ref, x_ref, 1, 256) + low
                yield None
                full = part(ref, x_ref, 2)
                yield None
                yield low, part(ref, x_ref, 3) + full
            else:
                full = part(ref, x_ref, 0)
                for i in (1, 2):
                    yield None
                    full = part(ref, x_ref, i) + full
                yield None
                yield None, part(ref, x_ref, 3) + full

        s = score(0)
        dq = dq_half(0, 0)
        dp = grad(0)
        finish(0, s, dp)
        put_dq(0, dq if diagonal_p else dq_half(0, 1) + dq)
        s = score(1)
        dv = keys_sum(dot_v, pp_ref)
        next(dv)
        next(dv)
        dp = grad(1)
        finish(1, s, dp)
        next(dv)
        put_keys(dvt, *next(dv))
        s = score(2)
        dq = dq_half(1, 0)
        dp = grad(2)
        finish(2, s, dp)
        put_dq(1, dq_half(1, 1) + dq)
        s = score(3)
        dk = keys_sum(qt_v, dp_ref)
        next(dk)
        next(dk)
        dp = grad(3)
        finish(3, s, dp)
        next(dk)
        put_keys(dkt, *next(dk))

    def flush(kb_p, rg_p):
        dvt[kb_p] += dg(dot_v[rg_p], p1[...], 1, 0)
        dkt[kb_p] += dg(qt_v[rg_p], d1[...], 1, 0)
        dqt[rg_p] += dg(keys_t(k_v, kb_p), d1[...], 1, 1)

    def wait_local(ref, sem):
        pltpu.make_async_copy(ref, ref, sem).wait()

    def wait_rows(m, g):
        wait_local(st_v.at[m, g, pl.ds(0, 8), :], rows_rs.at[m, g, 2])
        wait_local(q_v.at[m, g], rows_rs.at[m, g, 0])
        wait_local(do_v.at[m, g], rows_rs.at[m, g, 1])

        @pl.when(m != 0)
        def _():
            wait_local(st_v.at[m, g, pl.ds(8, 8), :], rows_rs.at[m, g, 3])

    def prepare_rows(m, g):
        rg = m * N_GRP + g
        x = st_v[m, g]
        hi = x.astype(BF16).astype(F32)
        mid = (x - hi).astype(BF16).astype(F32)
        lo = (x - hi) - mid
        parts = [y[8 * t:8 * t + 8] for t in (0, 1) for y in (hi, mid, lo)]
        aug_v[m, g] = jnp.concatenate(parts + [jnp.zeros((80, DIM), F32)], axis=0).T.astype(BF16)
        qt_v[rg] = q_v[m, g].reshape(RB, DIM).T
        dot_v[rg] = do_v[m, g].reshape(RB, DIM).T

    def wait_keys(k):
        with jax.named_scope('w_keys'):
            for core in (0, 1):
                e = 2 * k + core
                m = xor3(me, e)
                rows = pl.ds(pl.multiple_of(e * KEYS_DEV, CHUNK), KEYS_DEV)
                wait_local(k_v.at[rows, :], keys_rs.at[m, 0])
                wait_local(v_v.at[rows, :], keys_rs.at[m, 1])

    def prepare_keys(kb):
        for i in range(CB // DIM):
            rows = pl.ds(pl.multiple_of(kb * CB + DIM * i, DIM), DIM)
            k_v[rows, :] = k_v[rows, :].T
            v_v[rows, :] = v_v[rows, :].T

    def stage_dq(m, g, slot):
        with jax.named_scope('s_dq'):
            odq[slot] = (dqt[m * N_GRP + g].T * SCALE).astype(BF16).reshape(8, ROWS_DEV, GROUP, DIM)

    def send_dq(m, g, slot):
        e = xor3(me, m)
        dst = dq_o.at[pl.ds(pl.multiple_of(8 * g, 8), 8), :, pl.ds(pl.multiple_of(me * GROUP, GROUP), GROUP), :]

        @pl.when(m == 0)
        def _():
            pltpu.make_async_copy(odq.at[slot], dst, dq_ss.at[slot]).start()

        @pl.when(m != 0)
        def _():
            pltpu.make_async_remote_copy(odq.at[slot], dst, dq_ss.at[slot], dq_rs.at[m],
                                         device_id=dev(e), device_id_type=MESH).start()

    def stage_kv(kb, buf):
        with jax.named_scope('s_kv'):
            okv[buf, 0] = dkt[kb].T * SCALE
            okv[buf, 1] = dvt[kb].T

    def send_kv(kb, buf):
        n_dev = KEYS_DEV // CHUNK
        e_lo = quo(8 * kb, n_dev)

        def piece(j, c):
            ck = 8 * kb + j
            over = ck >= n_dev * (e_lo + 1)
            e = jnp.where(over, e_lo + 1, e_lo)
            off = pl.multiple_of(CHUNK * (ck - n_dev * e), CHUNK)
            m = xor3(me, e)
            src = okv.at[buf, :, pl.ds(pl.multiple_of(CHUNK * j, CHUNK), CHUNK), :]
            dst = dkv_o.at[:, pl.ds(off, CHUNK), me, 0, :]

            @pl.when(m == 0)
            def _():
                pltpu.make_async_copy(src, dst, kv_ss.at[buf]).start()

            @pl.when(m != 0)
            def _():
                pltpu.make_async_remote_copy(src, dst, kv_ss.at[buf], kv_rs.at[m],
                                             device_id=dev(e), device_id_type=MESH).start()
            return c
        lax.fori_loop(0, CB // CHUNK, piece, 0)

    def wait_kv(buf):
        with jax.named_scope('w_kv'):
            wait_local(okv.at[buf], kv_ss.at[buf])

    def wait_dq(slot):
        with jax.named_scope('w_dq'):
            wait_local(odq.at[slot], dq_ss.at[slot])

    def between(o, lo, hi):
        return (o >= lo) & (o < hi)

    def chip_at(d):
        return jnp.where(d == 0, chips[0], jnp.where(d == 1, chips[1], jnp.where(d == 2, chips[2], chips[3])))

    from_2 = pick(edge_at == 1, 2, 4)
    from_3 = from_2 + pick(edge_at == 2, 2, 4)
    from_4 = from_3 + pick(edge_at == 3, 2, 4)

    def block_0(o):
        j = o - n_own
        d = pick(j >= from_3, 3, pick(j >= from_2, 2, 1))
        i = j - jnp.where(j >= from_3, from_3, jnp.where(j >= from_2, from_2, 0))
        kb = jnp.where(j >= from_4, 5 * (j - from_4) + 4, 5 * chip_at(d) + i)
        return jnp.where(j < 0, first_kb + o, kb)

    def unit(n):
        rest = jnp.maximum(n - 6, 0)
        one = pick(edge_at == 1, 2, 1)
        two = pick(edge_at == 3, 2, 3)
        turn = edge | (n < 6)
        d = jnp.where(turn, 1 + rem(n, 3), jnp.where(rem(rest, 2) == 0, one, two))
        i = jnp.where(turn, quo(n, 3), 2 + quo(rest, 2))
        n_whole = n_units - 3
        return jnp.where(n >= n_whole, 5 * (n - n_whole) + 4, 5 * chip_at(d) + i)

    def rows_d(r):
        return 6 + rem(r, 2), quo(r, 2)

    def rows_b(r):
        return 2 + 2 * rem(r, 2) + quo(rem(r, 4), 2), quo(r, 4)

    def rows_at(o, r):
        d_m, d_g = rows_d(r)
        b_m, b_g = rows_b(r)
        return jnp.where(o < pass_b, d_m, b_m), jnp.where(o < pass_b, d_g, b_g)

    def done_dq(o, act):
        @pl.when(o >= pass_d)
        def _():
            in_d = o <= pass_3
            base = jnp.where(in_d, pass_d, pass_b)
            n = pick(in_d, 6, 11)

            def one(t, c):
                r = 3 * (o - base) - 1 + t

                @pl.when((r >= 0) & (r < n))
                def _():
                    d_m, d_g = rows_d(r)
                    b_m, b_g = rows_b(r)
                    act(jnp.where(in_d, d_m, b_m), jnp.where(in_d, d_g, b_g), r + pick(in_d, 0, 6))
                return c
            lax.fori_loop(0, 3, one, 0)

    def done_kv(o, act):
        i = o - pass_2 - 1
        late = jnp.logical_not(edge) & ((i == 8) | (i == 11))

        @pl.when(((i >= 0) & (i < 6)) | late | between(o, pass_3 + 1, pass_b + 1))
        def _():
            kb = jnp.where(late, pick(i == 8, 17, 18), unit(jnp.where(i < 6, jnp.clip(i, 0, 5), jnp.maximum(o - pass_3, 0) + 5)))
            act(kb, jnp.where(late, pick(i == 8, 6, 7), jnp.where(i < 6, i, pick(edge, 6, 8) + o - pass_3 - 1)))

    def put_kv(kb, ev):
        @pl.when(ev >= N_BUF)
        def _():
            wait_kv(rem(ev, N_BUF))
        stage_kv(kb, rem(ev, N_BUF))

    def put_dq(m, g, slot):
        wait_dq(slot)
        stage_dq(m, g, slot)

    def outer(o, carry):
        ends = between(o, pass_d, pass_3) | between(o, pass_b, pass_c)
        last = o >= pass_c
        n = jnp.where(o < pass_2, o - pass_1, jnp.where(o < pass_d, o - pass_2, o - pass_3 + 6))
        kb = jnp.where(o < pass_1, block_0(o), unit(jnp.clip(n, 0, n_units - 1)))
        cut = kb == 16
        m_lo = pick(o < pass_1, 0, pick(between(o, pass_2, pass_d), 6, 2))
        n_m = pick((o < pass_1) | between(o, pass_2, pass_d), 2, 4)
        it = jnp.where(o < pass_b, o - pass_d, o - pass_b)
        w = pick(o < pass_b, 2, 4)
        n_six = jnp.where(ends, pick(edge, 1, 2), jnp.where(last, pick(o == pass_c, 1, 0), quo(n_m, 2)))
        n_diag = jnp.where(ends, pick(edge & (it < quo(w, 2)), 1, 0), jnp.where(last, 0, jnp.where(cut, quo(n_m, 2), 0)))
        first = (o == 0) | (o == pass_1) | (o == pass_2)

        done_dq(o - 1, lambda m, g, ev: send_dq(m, g, rem(ev, N_DQ)))
        done_kv(o - 1, lambda k, ev: send_kv(k, rem(ev, N_BUF)))

        @pl.when(o < pass_1)
        def _():
            @pl.when(o == 0)
            def _():
                wait_keys(chip)
                for i in (1, 2, 3):
                    prepare_keys(first_kb + i)
            j = o - n_own

            @pl.when((j == 0) | (j == from_2) | (j == from_3))
            def _():
                wait_keys(chip_at(pick(j == from_3, 3, pick(j == from_2, 2, 1))))

            @pl.when((o == 0) | (j >= 0))
            def _():
                prepare_keys(kb)

            @pl.when(cut & (j >= 0))
            def _():
                prepare_keys(kb + 1)
                prepare_keys(kb + 2)

        def index(n):
            f = lax.div(n, n_m)
            k = jnp.where(cut, pick(f == 2, 17, 16), kb)
            m = m_lo + lax.rem(n, n_m)
            g = jnp.where(cut, pick(f == 0, 1, 2), f)
            e_r = 3 * it + quo(n, 4)
            e_k = first_kb + rem(n, 4)
            e = 6 * it + n
            e_a = jnp.maximum(e - w, 0)
            e_b = jnp.maximum(e - 3 * w, 0)
            x_r = jnp.where(e < w, e, jnp.where(e < 3 * w, w + quo(e_a, 2), 2 * w + quo(e_b, 3)))
            x_k = 15 + jnp.where(e < w, 0, jnp.where(e < 3 * w, rem(e_a, 2), rem(e_b, 3)))
            e_m, e_g = rows_at(o, jnp.where(edge, x_r, e_r))
            k = jnp.where(ends, jnp.where(edge, x_k, e_k), jnp.where(last, first_kb + 3, k))
            m = jnp.where(ends, e_m, jnp.where(last, rem(n, 2), m))
            g = jnp.where(ends, e_g, jnp.where(last, quo(n, 2), g))
            return k, m, g

        def index_diag(n):
            e_m, e_g = rows_at(o, 6 * it + n)
            g = jnp.where(ends, e_g, lax.div(n, n_m))
            m = jnp.where(ends, e_m, m_lo + lax.rem(n, n_m))
            return 16 + g, m, g

        def six(fresh, diagonal, j, c):
            if fresh:
                def one(t, c):
                    _, m, g = index(UNROLL * j + t)
                    wait_rows(m, g)
                    return c
                with jax.named_scope('w_rows'):
                    lax.fori_loop(0, UNROLL, one, 0)
            kb_p, rg_p = c
            for t in range(UNROLL):
                k, m, g = (index_diag if diagonal else index)(UNROLL * j + t)
                if fresh:
                    prepare_rows(m, g)
                bufs = (p0, d0, p1, d1) if t % 2 == 0 else (p1, d1, p0, d0)
                tile(k, m, g, kb_p, rg_p, bufs, diagonal, diagonal and t > 0, diagonal and t == UNROLL - 1)
                kb_p, rg_p = k, m * N_GRP + g
            return kb_p, rg_p

        with jax.named_scope('tiles'):
            carry = lax.fori_loop(0, jnp.where(first, n_six, 0), functools.partial(six, True, False), carry)
            carry = lax.fori_loop(0, jnp.where(first, 0, n_six), functools.partial(six, False, False), carry)
            carry = lax.fori_loop(0, n_diag, functools.partial(six, False, True), carry)

        done_kv(o, put_kv)

        def put(m, g, ev):
            @pl.when(ev >= N_DQ)
            def _():
                wait_dq(rem(ev, N_DQ))
            stage_dq(m, g, rem(ev, N_DQ))
        done_dq(o, put)
        return carry

    kb_p, rg_p = lax.fori_loop(0, N_OUTER, outer, (first_kb, jnp.int32(0)))
    done_dq(n_outer - 1, lambda m, g, ev: send_dq(m, g, rem(ev, N_DQ)))
    with jax.named_scope('flush'):
        flush(kb_p, rg_p)

    m_l, g_l = rows_b(jnp.int32(11))
    put_dq(m_l, g_l, 17 % N_DQ)
    for i in range(4):
        put_kv(first_kb + i, jnp.int32(15 + i))
        if i == 0:
            send_dq(m_l, g_l, 17 % N_DQ)
        else:
            send_kv(first_kb + i - 1, (14 + i) % N_BUF)
    own = [(jnp.int32(m), jnp.int32(g), (18 + 3 * (1 - m) + g) % N_DQ) for m in (1, 0) for g in range(N_GRP)]
    for r, (m, g, slot) in enumerate(own):
        put_dq(m, g, slot)
        if r == 0:
            send_kv(first_kb + 3, 18 % N_BUF)
        else:
            send_dq(*own[r - 1])
    send_dq(*own[-1])

    for slot in range(N_DQ):
        wait_dq(slot)
    for buf in range(N_BUF):
        wait_kv(buf)
    with jax.named_scope('drain'):
        for m in range(1, N_DEV):
            for g in range(N_GRP):
                wait_local(st_v.at[m, g, pl.ds(0, 8), :], rows_ss.at[m, g, 2])
                wait_local(nd_v.at[m, g], rows_ss.at[m, g, 3])
                wait_local(q_v.at[m, g], rows_ss.at[m, g, 0])
                wait_local(do_v.at[m, g], rows_ss.at[m, g, 1])
            wait_local(k_v.at[pl.ds(0, KEYS_DEV), :], keys_ss.at[m, 0])
            wait_local(v_v.at[pl.ds(0, KEYS_DEV), :], keys_ss.at[m, 1])
            heads = pl.ds(0, GROUP)
            wait_local(dq_o.at[:, :, heads, :], dq_rs.at[m])
            wait_local(dkv_o.at[:, :, 0, 0, :], kv_rs.at[m])


def solution(mesh):
    row_spec = P(None, CP_AXES, 'heads', None)
    stat_spec = P(None, CP_AXES, 'heads')
    key_spec = P(CP_AXES, 'heads', None)
    any_ = pl.BlockSpec(memory_space=pl.ANY)

    def local_grads(queries, attn_out, grad_out, log_sum_exp, key_cache, value_cache):
        lse = (log_sum_exp * (-1.0 / SCALE)).reshape(N_GRP, 8, ROWS_DEV, N_DEV, GROUP)
        lse = jnp.transpose(lse, (3, 0, 1, 2, 4)).reshape(N_DEV, N_GRP, 8, DIM)
        keys = jnp.transpose(key_cache, (1, 0, 2))
        values = jnp.transpose(value_cache, (1, 0, 2))
        dma = pltpu.SemaphoreType.DMA
        rows_shape = (N_DEV, N_GRP, 8, ROWS_DEV, GROUP, DIM)
        n_rg = N_DEV * N_GRP
        grad_query, grad_keys = pl.pallas_call(
            kernel,
            name='attn_bwd',
            out_shape=(jax.ShapeDtypeStruct((N_SLICES, ROWS_DEV, N_DEV * GROUP, DIM), BF16),
                       jax.ShapeDtypeStruct((2, KEYS_DEV, N_DEV, 1, DIM), F32)),
            in_specs=[any_] * 6,
            out_specs=[any_] * 2,
            scratch_shapes=[
                pltpu.VMEM(rows_shape, BF16), pltpu.VMEM(rows_shape, BF16),
                pltpu.VMEM((n_rg, DIM, RB), BF16), pltpu.VMEM((n_rg, DIM, RB), BF16),
                pltpu.VMEM((N_DEV, N_GRP, 16, DIM), F32), pltpu.VMEM((N_DEV, N_GRP, DIM, DIM), BF16),
                pltpu.VMEM((KEYS, DIM), BF16), pltpu.VMEM((KEYS, DIM), BF16),
                pltpu.VMEM((n_rg, DIM, RB), F32),
                pltpu.VMEM((NKB, DIM, CB), F32), pltpu.VMEM((NKB, DIM, CB), F32),
                pltpu.VMEM((RB, CB), BF16), pltpu.VMEM((RB, CB), BF16),
                pltpu.VMEM((RB, CB), BF16), pltpu.VMEM((RB, CB), BF16),
                pltpu.VMEM((DIM, CB), jnp.int32),
                pltpu.VMEM((N_BUF, 2, CB, DIM), F32),
                pltpu.VMEM((N_DQ, 8, ROWS_DEV, GROUP, DIM), BF16),
                pltpu.VMEM((N_DEV, N_GRP, 8, DIM), F32),
                dma((N_DEV, N_GRP, 4)), dma((N_DEV, 2)), dma((N_DEV, N_GRP, 4)), dma((N_DEV, 2)),
                dma((N_BUF,)), dma((N_DEV,)), dma((N_DQ,)), dma((N_DEV,)),
            ],
            compiler_params=pltpu.CompilerParams(collective_id=0, has_side_effects=True, vmem_limit_bytes=67043328),
        )(queries, grad_out, attn_out, lse, keys, values)
        grad_keys = grad_keys.reshape(2, KEYS_DEV, N_DEV, DIM)
        return grad_query, grad_keys[0], grad_keys[1]

    return jax.shard_map(local_grads, mesh=mesh, in_specs=(row_spec, row_spec, row_spec, stat_spec, key_spec, key_spec),
                         out_specs=(row_spec, key_spec, key_spec), check_vma=False)
```

```python
import functools
import math

import jax
import jax.numpy as jnp
from jax import lax
from jax.experimental import pallas as pl
from jax.experimental.pallas import tpu as pltpu
from jax.sharding import PartitionSpec as P

CP_AXES = ('cpo', 'cp')
MESH = pl.DeviceIdType.MESH
BF16 = jnp.bfloat16
F32 = jnp.float32

N_DEV = 8
N_SLICES = 24
ROWS_DEV = 8
GROUP = 16
DIM = 128
KEYS = 9728
KEYS_DEV = KEYS // N_DEV
PREFIX = 8192
N_GRP = 3
RB = 1024
CB = 512
NKB = KEYS // CB
CHUNK = 64
SCALE = DIM ** -0.5
EXP_SCALE = SCALE * math.log2(math.e)

UNROLL = 6
N_BUF = 3
N_DQ = 12
N_OUTER = 53
AHEAD = 5


def dg(a, b, ca, cb):
    return lax.dot_general(a, b, (((ca,), (cb,)), ((), ())), preferred_element_type=F32)


def quo(a, b):
    return lax.div(a, jnp.int32(b))


def rem(a, b):
    return lax.rem(a, jnp.int32(b))


def pick(cond, a, b):
    return jnp.where(cond, jnp.int32(a), jnp.int32(b))


def xor3(a, b):
    out = jnp.int32(0)
    for bit in (1, 2, 4):
        out = out + bit * rem(rem(quo(a, bit), 2) + rem(quo(b, bit), 2), 2)
    return out


def kernel(q_h, do_h, o_h, l_h, k_h, v_h, dq_o, dkv_o,
           q_v, do_v, qt_v, dot_v, st_v, aug_v, k_v, v_v, dqt, dkt, dvt, p0, d0, p1, d1, x_v, okv, odq, nd_v,
           rows_ss, keys_ss, rows_rs, keys_rs, kv_ss, kv_rs, dq_ss, dq_rs):
    me = lax.axis_index('cpo') * 4 + lax.axis_index('cp')
    chip = quo(me, 2)
    first_kb = 5 * chip
    core = rem(me, 2)
    chips = [chip, quo(xor3(me, 2 + 2 * core), 2), quo(xor3(me, 4 - 2 * core), 2), 3 - chip]

    edge = chip == 3
    edge_at = pick(chips[1] == 3, 1, pick(chips[2] == 3, 2, pick(edge, 0, 3)))
    n_own = pick(edge, 2, 3)
    n_units = pick(edge, 15, 13)
    pass_1 = n_own + n_units
    pass_2 = pass_1 + 6
    pass_d = pass_2 + n_units
    pass_3 = pass_d + 2
    pass_b = pass_3 + n_units - 6
    pass_c = pass_b + 4
    n_outer = pass_c + pick(edge, 0, 1)

    def dev(e):
        return {'cpo': quo(e, 4), 'cp': rem(e, 4)}

    barrier = pltpu.get_barrier_semaphore()
    for m in range(1, N_DEV):
        pl.semaphore_signal(barrier, inc=1, device_id=dev(xor3(me, jnp.int32(m))), device_id_type=MESH)

    def zero_keys(i, c):
        dkt[i] = jnp.zeros((DIM, CB), F32)
        dvt[i] = jnp.zeros((DIM, CB), F32)
        return c
    lax.fori_loop(0, NKB, zero_keys, 0)

    def zero_rows(i, c):
        dqt[i] = jnp.zeros((DIM, RB), F32)
        return c
    lax.fori_loop(0, N_DEV * N_GRP, zero_rows, 0)
    p1[...] = jnp.zeros((RB, CB), BF16)
    d1[...] = jnp.zeros((RB, CB), BF16)
    x_v[...] = (lax.broadcasted_iota(jnp.int32, (DIM, CB), 1)
                - lax.broadcasted_iota(jnp.int32, (DIM, CB), 0) // GROUP)

    with jax.named_scope('barrier'):
        pl.semaphore_wait(barrier, N_DEV - 1)

    def row_copies(m, g, local=False):
        e = xor3(me, m)
        heads = pl.ds(pl.multiple_of(e * GROUP, GROUP), GROUP)
        pairs = ((l_h.at[e, g], st_v.at[m, g, pl.ds(0, 8), :], 2),
                 (q_h.at[pl.ds(8 * g, 8), :, heads, :], q_v.at[m, g], 0),
                 (do_h.at[pl.ds(8 * g, 8), :, heads, :], do_v.at[m, g], 1))
        for src, dst, t in pairs:
            if local:
                yield pltpu.make_async_copy(src, dst, rows_rs.at[m, g, t])
            else:
                yield pltpu.make_async_remote_copy(src, dst, rows_ss.at[m, g, t], rows_rs.at[m, g, t],
                                                   device_id=dev(e), device_id_type=MESH)

    def key_copies(e, m, local=False):
        rows = pl.ds(pl.multiple_of(me * KEYS_DEV, CHUNK), KEYS_DEV)
        for src, dst, t in ((k_h.at[e], k_v.at[rows, :], 0), (v_h.at[e], v_v.at[rows, :], 1)):
            if local:
                yield pltpu.make_async_copy(src, dst, keys_rs.at[m, t])
            else:
                yield pltpu.make_async_remote_copy(src, dst, keys_ss.at[m, t], keys_rs.at[m, t],
                                                   device_id=dev(e), device_id_type=MESH)

    for c in key_copies(me, jnp.int32(0), local=True):
        c.start()
    for c in key_copies(xor3(me, jnp.int32(1)), jnp.int32(1)):
        c.start()
    for g in range(N_GRP):
        for m in (0, 1):
            for c in row_copies(jnp.int32(m), g, m == 0):
                c.start()
    turns = [jnp.where(core == 0, jnp.int32(a), jnp.int32(b)) for a, b in ((2, 4), (5, 3), (3, 5), (4, 2), (6, 7), (7, 6))]
    for m in turns:
        for c in key_copies(xor3(me, m), m):
            c.start()

    def block_copies(c):
        e = xor3(me, quo(c, N_GRP))
        src = (pl.ds(pl.multiple_of(8 * rem(c, N_GRP), 8), 8), slice(None), pl.ds(pl.multiple_of(e * GROUP, GROUP), GROUP), slice(None))
        for t, ref in ((0, o_h), (6, do_h)):
            slot = rem(c, 6) + t
            yield pltpu.make_async_copy(ref.at[src], odq.at[slot], dq_ss.at[slot])

    def delta(c, carry):
        @pl.when(c + AHEAD < N_DEV * N_GRP)
        def _():
            for copy in block_copies(c + AHEAD):
                copy.start()
        for copy in block_copies(c):
            copy.wait()
        x = odq[rem(c, 6)].reshape(RB, DIM).astype(F32) * odq[rem(c, 6) + 6].reshape(RB, DIM).astype(F32)
        hi = x.astype(BF16)
        lo = (x - hi.astype(F32)).astype(BF16)
        row = lax.broadcasted_iota(jnp.int32, (16, 2 * DIM), 0)
        acc = None
        for i in range(8):
            one = jnp.where(row == i, 1.0, 0.0).astype(BF16)
            part = dg(one, jnp.concatenate([hi[DIM * i:DIM * i + DIM], lo[DIM * i:DIM * i + DIM]], axis=1), 1, 1)
            acc = part if acc is None else part + acc
        nd = 0.0 - acc[:8]
        m, g = quo(c, N_GRP), rem(c, N_GRP)
        nd_v[m, g] = nd

        @pl.when(m == 0)
        def _():
            st_v[0, g, 8:16, :] = nd
        return carry

    for c in range(AHEAD):
        for copy in block_copies(jnp.int32(c)):
            copy.start()
    with jax.named_scope('delta'):
        lax.fori_loop(0, N_DEV * N_GRP, delta, 0)
    for m in range(1, N_DEV):
        for g in range(N_GRP):
            pltpu.make_async_remote_copy(nd_v.at[m, g], st_v.at[m, g, pl.ds(8, 8), :], rows_ss.at[m, g, 3], rows_rs.at[m, g, 3],
                                         device_id=dev(xor3(me, jnp.int32(m))), device_id_type=MESH).start()
    for ms in (turns[:4], turns[4:]):
        for g in range(N_GRP):
            for m in ms:
                for c in row_copies(m, g):
                    c.start()

    def keys_t(ref, kb):
        return jnp.concatenate([ref[pl.ds(pl.multiple_of(kb * CB + DIM * i, DIM), DIM), :] for i in range(CB // DIM)], axis=1)

    def tile(kb, m, g, kb_p, rg_p, bufs, diagonal=False, diagonal_p=False, fill=False):
        p_ref, d_ref, pp_ref, dp_ref = bufs
        slice_of = lax.broadcasted_iota(jnp.int32, (DIM, DIM), 1) % 8
        part_row = lax.broadcasted_iota(jnp.int32, (DIM, CB), 0)
        pick_l = jnp.where(part_row < 24, 1.0, 0.0).astype(BF16)
        pick_d = jnp.where((part_row >= 24) & (part_row < 48), 1.0, 0.0).astype(BF16)
        rhs_s = jnp.concatenate([keys_t(k_v, kb), pick_l], axis=0)
        rhs_d = jnp.concatenate([keys_t(v_v, kb), pick_d], axis=0)
        stats = aug_v[m, g]

        def width(rc):
            return 256 if diagonal and rc < 2 else CB

        def lhs(ref, rc):
            zero = jnp.zeros((), BF16)
            aug = jnp.concatenate([jnp.where(slice_of == 2 * rc, stats, zero),
                                   jnp.where(slice_of == 2 * rc + 1, stats, zero)], axis=0)
            return jnp.concatenate([ref[m, g, pl.ds(2 * rc, 2)].reshape(256, DIM), aug], axis=1)

        def score(rc):
            return dg(lhs(q_v, rc), rhs_s[:, :width(rc)], 1, 0)

        def grad(rc):
            return dg(lhs(do_v, rc), rhs_d[:, :width(rc)], 1, 0)

        def finish(rc, s, dp):
            w = width(rc)
            p = jnp.exp2(s * EXP_SCALE)
            if diagonal:
                limit = ROWS_DEV * xor3(me, m)
                p = jnp.concatenate([jnp.where(x_v[:, :w] <= limit + 64 * (2 * rc), p[:DIM], 0.0),
                                     jnp.where(x_v[:, :w] <= limit + 64 * (2 * rc + 1), p[DIM:], 0.0)], axis=0)
            rows = slice(256 * rc, 256 * rc + 256)
            p_ref[rows, :w] = p.astype(BF16)
            d_ref[rows, :w] = (p * dp).astype(BF16)
            if fill and w < CB:
                p_ref[rows, w:] = jnp.zeros((256, CB - w), BF16)
                d_ref[rows, w:] = jnp.zeros((256, CB - w), BF16)

        def dq_half(h, k):
            cols = slice(256 * k, 256 * k + 256)
            return dg(keys_t(k_v, kb_p)[:, cols], dp_ref[512 * h:512 * h + 512, cols], 1, 1)

        def part(ref, x_ref, i, w=CB):
            return dg(ref[rg_p][:, 256 * i:256 * i + 256], x_ref[256 * i:256 * i + 256, :w], 1, 0)

        def put_dq(h, x):
            dqt[rg_p, :, 512 * h:512 * h + 512] = x + dqt[rg_p, :, 512 * h:512 * h + 512]

        def put_keys(ref, low, full):
            if low is None:
                ref[kb_p] = full + ref[kb_p]
            else:
                ref[kb_p, :, :256] = low + full[:, :256] + ref[kb_p, :, :256]
                ref[kb_p, :, 256:] = full[:, 256:] + ref[kb_p, :, 256:]

        def keys_sum(ref, x_ref):
            if diagonal_p:
                low = part(ref, x_ref, 0, 256)
                yield None
                low = part(ref, x_ref, 1, 256) + low
                yield None
                full = part(ref, x_ref, 2)
                yield None
                yield low, part(ref, x_ref, 3) + full
            else:
                full = part(ref, x_ref, 0)
                for i in (1, 2):
                    yield None
                    full = part(ref, x_ref, i) + full
                yield None
                yield None, part(ref, x_ref, 3) + full

        s = score(0)
        dq = dq_half(0, 0)
        dp = grad(0)
        finish(0, s, dp)
        put_dq(0, dq if diagonal_p else dq_half(0, 1) + dq)
        s = score(1)
        dv = keys_sum(dot_v, pp_ref)
        next(dv)
        next(dv)
        dp = grad(1)
        finish(1, s, dp)
        next(dv)
        put_keys(dvt, *next(dv))
        s = score(2)
        dq = dq_half(1, 0)
        dp = grad(2)
        finish(2, s, dp)
        put_dq(1, dq_half(1, 1) + dq)
        s = score(3)
        dk = keys_sum(qt_v, dp_ref)
        next(dk)
        next(dk)
        dp = grad(3)
        finish(3, s, dp)
        next(dk)
        put_keys(dkt, *next(dk))

    def flush(kb_p, rg_p):
        dvt[kb_p] += dg(dot_v[rg_p], p1[...], 1, 0)
        dkt[kb_p] += dg(qt_v[rg_p], d1[...], 1, 0)
        dqt[rg_p] += dg(keys_t(k_v, kb_p), d1[...], 1, 1)

    def wait_local(ref, sem):
        pltpu.make_async_copy(ref, ref, sem).wait()

    def wait_rows(m, g):
        wait_local(st_v.at[m, g, pl.ds(0, 8), :], rows_rs.at[m, g, 2])
        wait_local(q_v.at[m, g], rows_rs.at[m, g, 0])
        wait_local(do_v.at[m, g], rows_rs.at[m, g, 1])

        @pl.when(m != 0)
        def _():
            wait_local(st_v.at[m, g, pl.ds(8, 8), :], rows_rs.at[m, g, 3])

    def prepare_rows(m, g):
        rg = m * N_GRP + g
        x = st_v[m, g]
        hi = x.astype(BF16).astype(F32)
        mid = (x - hi).astype(BF16).astype(F32)
        lo = (x - hi) - mid
        parts = [y[8 * t:8 * t + 8] for t in (0, 1) for y in (hi, mid, lo)]
        aug_v[m, g] = jnp.concatenate(parts + [jnp.zeros((80, DIM), F32)], axis=0).T.astype(BF16)
        qt_v[rg] = q_v[m, g].reshape(RB, DIM).T
        dot_v[rg] = do_v[m, g].reshape(RB, DIM).T

    def wait_keys(k):
        with jax.named_scope('w_keys'):
            for side in (0, 1):
                e = 2 * k + side
                m = xor3(me, e)
                rows = pl.ds(pl.multiple_of(e * KEYS_DEV, CHUNK), KEYS_DEV)
                wait_local(k_v.at[rows, :], keys_rs.at[m, 0])
                wait_local(v_v.at[rows, :], keys_rs.at[m, 1])

    def prepare_keys(kb):
        for i in range(CB // DIM):
            rows = pl.ds(pl.multiple_of(kb * CB + DIM * i, DIM), DIM)
            k_v[rows, :] = k_v[rows, :].T
            v_v[rows, :] = v_v[rows, :].T

    def stage_dq(m, g, slot):
        with jax.named_scope('s_dq'):
            odq[slot] = (dqt[m * N_GRP + g].T * SCALE).astype(BF16).reshape(8, ROWS_DEV, GROUP, DIM)

    def send_dq(m, g, slot):
        e = xor3(me, m)
        dst = dq_o.at[pl.ds(pl.multiple_of(8 * g, 8), 8), :, pl.ds(pl.multiple_of(me * GROUP, GROUP), GROUP), :]

        @pl.when(m == 0)
        def _():
            pltpu.make_async_copy(odq.at[slot], dst, dq_ss.at[slot]).start()

        @pl.when(m != 0)
        def _():
            pltpu.make_async_remote_copy(odq.at[slot], dst, dq_ss.at[slot], dq_rs.at[m],
                                         device_id=dev(e), device_id_type=MESH).start()

    def stage_kv(kb, buf):
        with jax.named_scope('s_kv'):
            okv[buf, 0] = dkt[kb].T * SCALE
            okv[buf, 1] = dvt[kb].T

    def send_kv(kb, buf):
        n_dev = KEYS_DEV // CHUNK
        e_lo = quo(8 * kb, n_dev)

        def piece(j, c):
            ck = 8 * kb + j
            over = ck >= n_dev * (e_lo + 1)
            e = jnp.where(over, e_lo + 1, e_lo)
            off = pl.multiple_of(CHUNK * (ck - n_dev * e), CHUNK)
            m = xor3(me, e)
            src = okv.at[buf, :, pl.ds(pl.multiple_of(CHUNK * j, CHUNK), CHUNK), :]
            dst = dkv_o.at[:, pl.ds(off, CHUNK), me, 0, :]

            @pl.when(m == 0)
            def _():
                pltpu.make_async_copy(src, dst, kv_ss.at[buf]).start()

            @pl.when(m != 0)
            def _():
                pltpu.make_async_remote_copy(src, dst, kv_ss.at[buf], kv_rs.at[m],
                                             device_id=dev(e), device_id_type=MESH).start()
            return c
        lax.fori_loop(0, CB // CHUNK, piece, 0)

    def wait_kv(buf):
        with jax.named_scope('w_kv'):
            wait_local(okv.at[buf], kv_ss.at[buf])

    def wait_dq(slot):
        with jax.named_scope('w_dq'):
            wait_local(odq.at[slot], dq_ss.at[slot])

    def between(o, lo, hi):
        return (o >= lo) & (o < hi)

    def chip_at(d):
        return jnp.where(d == 0, chips[0], jnp.where(d == 1, chips[1], jnp.where(d == 2, chips[2], chips[3])))

    from_2 = pick(edge_at == 1, 2, 4)
    from_3 = from_2 + pick(edge_at == 2, 2, 4)
    from_4 = from_3 + pick(edge_at == 3, 2, 4)

    def block_0(o):
        j = o - n_own
        d = pick(j >= from_3, 3, pick(j >= from_2, 2, 1))
        i = j - jnp.where(j >= from_3, from_3, jnp.where(j >= from_2, from_2, 0))
        kb = jnp.where(j >= from_4, 5 * (j - from_4) + 4, 5 * chip_at(d) + i)
        return jnp.where(j < 0, first_kb + o, kb)

    def unit(n):
        rest = jnp.maximum(n - 6, 0)
        one = pick(edge_at == 1, 2, 1)
        two = pick(edge_at == 3, 2, 3)
        turn = edge | (n < 6)
        d = jnp.where(turn, 1 + rem(n, 3), jnp.where(rem(rest, 2) == 0, one, two))
        i = jnp.where(turn, quo(n, 3), 2 + quo(rest, 2))
        n_whole = n_units - 3
        return jnp.where(n >= n_whole, 5 * (n - n_whole) + 4, 5 * chip_at(d) + i)

    def rows_d(r):
        return 6 + rem(r, 2), quo(r, 2)

    def rows_b(r):
        return 2 + 2 * rem(r + core, 2) + quo(rem(r, 4), 2), quo(r, 4)

    def rows_at(o, r):
        d_m, d_g = rows_d(r)
        b_m, b_g = rows_b(r)
        return jnp.where(o < pass_b, d_m, b_m), jnp.where(o < pass_b, d_g, b_g)

    def done_dq(o, act):
        @pl.when(o >= pass_d)
        def _():
            in_d = o <= pass_3
            base = jnp.where(in_d, pass_d, pass_b)
            n = pick(in_d, 6, 11)

            def one(t, c):
                r = 3 * (o - base) - 1 + t

                @pl.when((r >= 0) & (r < n))
                def _():
                    d_m, d_g = rows_d(r)
                    b_m, b_g = rows_b(r)
                    act(jnp.where(in_d, d_m, b_m), jnp.where(in_d, d_g, b_g), r + pick(in_d, 0, 6))
                return c
            lax.fori_loop(0, 3, one, 0)

    def done_kv(o, act):
        i = o - pass_2 - 1
        late = jnp.logical_not(edge) & ((i == 8) | (i == 11))

        @pl.when(((i >= 0) & (i < 6)) | late | between(o, pass_3 + 1, pass_b + 1))
        def _():
            kb = jnp.where(late, pick(i == 8, 17, 18), unit(jnp.where(i < 6, jnp.clip(i, 0, 5), jnp.maximum(o - pass_3, 0) + 5)))
            act(kb, jnp.where(late, pick(i == 8, 6, 7), jnp.where(i < 6, i, pick(edge, 6, 8) + o - pass_3 - 1)))

    def put_kv(kb, ev):
        @pl.when(ev >= N_BUF)
        def _():
            wait_kv(rem(ev, N_BUF))
        stage_kv(kb, rem(ev, N_BUF))

    def put_dq(m, g, slot):
        wait_dq(slot)
        stage_dq(m, g, slot)

    def outer(o, carry):
        ends = between(o, pass_d, pass_3) | between(o, pass_b, pass_c)
        last = o >= pass_c
        n = jnp.where(o < pass_2, o - pass_1, jnp.where(o < pass_d, o - pass_2, o - pass_3 + 6))
        kb = jnp.where(o < pass_1, block_0(o), unit(jnp.clip(n, 0, n_units - 1)))
        cut = kb == 16
        m_lo = pick(o < pass_1, 0, pick(between(o, pass_2, pass_d), 6, 2))
        n_m = pick((o < pass_1) | between(o, pass_2, pass_d), 2, 4)
        it = jnp.where(o < pass_b, o - pass_d, o - pass_b)
        w = pick(o < pass_b, 2, 4)
        n_six = jnp.where(ends, pick(edge, 1, 2), jnp.where(last, pick(o == pass_c, 1, 0), quo(n_m, 2)))
        n_diag = jnp.where(ends, pick(edge & (it < quo(w, 2)), 1, 0), jnp.where(last, 0, jnp.where(cut, quo(n_m, 2), 0)))
        first = (o == 0) | (o == pass_1) | (o == pass_2)

        done_dq(o - 1, lambda m, g, ev: send_dq(m, g, rem(ev, N_DQ)))
        done_kv(o - 1, lambda k, ev: send_kv(k, rem(ev, N_BUF)))

        @pl.when(o < pass_1)
        def _():
            @pl.when(o == 0)
            def _():
                wait_keys(chip)
                for i in (1, 2, 3):
                    prepare_keys(first_kb + i)
            j = o - n_own

            @pl.when((j == 0) | (j == from_2) | (j == from_3))
            def _():
                wait_keys(chip_at(pick(j == from_3, 3, pick(j == from_2, 2, 1))))

            @pl.when((o == 0) | (j >= 0))
            def _():
                prepare_keys(kb)

            @pl.when(cut & (j >= 0))
            def _():
                prepare_keys(kb + 1)
                prepare_keys(kb + 2)

        def index(n):
            f = lax.div(n, n_m)
            k = jnp.where(cut, pick(f == 2, 17, 16), kb)
            m = m_lo + lax.rem(n, n_m)
            g = jnp.where(cut, pick(f == 0, 1, 2), f)
            e_r = 3 * it + quo(n, 4)
            e_k = first_kb + rem(n, 4)
            e = 6 * it + n
            e_a = jnp.maximum(e - w, 0)
            e_b = jnp.maximum(e - 3 * w, 0)
            x_r = jnp.where(e < w, e, jnp.where(e < 3 * w, w + quo(e_a, 2), 2 * w + quo(e_b, 3)))
            x_k = 15 + jnp.where(e < w, 0, jnp.where(e < 3 * w, rem(e_a, 2), rem(e_b, 3)))
            e_m, e_g = rows_at(o, jnp.where(edge, x_r, e_r))
            k = jnp.where(ends, jnp.where(edge, x_k, e_k), jnp.where(last, first_kb + 3, k))
            m = jnp.where(ends, e_m, jnp.where(last, rem(n, 2), m))
            g = jnp.where(ends, e_g, jnp.where(last, quo(n, 2), g))
            return k, m, g

        def index_diag(n):
            e_m, e_g = rows_at(o, 6 * it + n)
            g = jnp.where(ends, e_g, lax.div(n, n_m))
            m = jnp.where(ends, e_m, m_lo + lax.rem(n, n_m))
            return 16 + g, m, g

        def six(fresh, diagonal, j, c):
            if fresh:
                def one(t, c):
                    _, m, g = index(UNROLL * j + t)
                    wait_rows(m, g)
                    return c
                with jax.named_scope('w_rows'):
                    lax.fori_loop(0, UNROLL, one, 0)
            kb_p, rg_p = c
            for t in range(UNROLL):
                k, m, g = (index_diag if diagonal else index)(UNROLL * j + t)
                if fresh:
                    prepare_rows(m, g)
                bufs = (p0, d0, p1, d1) if t % 2 == 0 else (p1, d1, p0, d0)
                tile(k, m, g, kb_p, rg_p, bufs, diagonal, diagonal and t > 0, diagonal and t == UNROLL - 1)
                kb_p, rg_p = k, m * N_GRP + g
            return kb_p, rg_p

        with jax.named_scope('tiles'):
            carry = lax.fori_loop(0, jnp.where(first, n_six, 0), functools.partial(six, True, False), carry)
            carry = lax.fori_loop(0, jnp.where(first, 0, n_six), functools.partial(six, False, False), carry)
            carry = lax.fori_loop(0, n_diag, functools.partial(six, False, True), carry)

        done_kv(o, put_kv)

        def put(m, g, ev):
            @pl.when(ev >= N_DQ)
            def _():
                wait_dq(rem(ev, N_DQ))
            stage_dq(m, g, rem(ev, N_DQ))
        done_dq(o, put)
        return carry

    kb_p, rg_p = lax.fori_loop(0, N_OUTER, outer, (first_kb, jnp.int32(0)))
    done_dq(n_outer - 1, lambda m, g, ev: send_dq(m, g, rem(ev, N_DQ)))
    with jax.named_scope('flush'):
        flush(kb_p, rg_p)

    m_l, g_l = rows_b(jnp.int32(11))
    put_dq(m_l, g_l, 17 % N_DQ)
    for i in range(4):
        put_kv(first_kb + i, jnp.int32(15 + i))
        if i == 0:
            send_dq(m_l, g_l, 17 % N_DQ)
        else:
            send_kv(first_kb + i - 1, (14 + i) % N_BUF)
    own = [(jnp.int32(m), jnp.int32(g), (18 + 3 * (1 - m) + g) % N_DQ) for m in (1, 0) for g in range(N_GRP)]
    for r, (m, g, slot) in enumerate(own):
        put_dq(m, g, slot)
        if r == 0:
            send_kv(first_kb + 3, 18 % N_BUF)
        else:
            send_dq(*own[r - 1])
    send_dq(*own[-1])

    for slot in range(N_DQ):
        wait_dq(slot)
    for buf in range(N_BUF):
        wait_kv(buf)
    with jax.named_scope('drain'):
        for m in range(1, N_DEV):
            for g in range(N_GRP):
                wait_local(st_v.at[m, g, pl.ds(0, 8), :], rows_ss.at[m, g, 2])
                wait_local(nd_v.at[m, g], rows_ss.at[m, g, 3])
                wait_local(q_v.at[m, g], rows_ss.at[m, g, 0])
                wait_local(do_v.at[m, g], rows_ss.at[m, g, 1])
            wait_local(k_v.at[pl.ds(0, KEYS_DEV), :], keys_ss.at[m, 0])
            wait_local(v_v.at[pl.ds(0, KEYS_DEV), :], keys_ss.at[m, 1])
            heads = pl.ds(0, GROUP)
            wait_local(dq_o.at[:, :, heads, :], dq_rs.at[m])
            wait_local(dkv_o.at[:, :, 0, 0, :], kv_rs.at[m])


def solution(mesh):
    row_spec = P(None, CP_AXES, 'heads', None)
    stat_spec = P(None, CP_AXES, 'heads')
    key_spec = P(CP_AXES, 'heads', None)
    any_ = pl.BlockSpec(memory_space=pl.ANY)

    def local_grads(queries, attn_out, grad_out, log_sum_exp, key_cache, value_cache):
        lse = (log_sum_exp * (-1.0 / SCALE)).reshape(N_GRP, 8, ROWS_DEV, N_DEV, GROUP)
        lse = jnp.transpose(lse, (3, 0, 1, 2, 4)).reshape(N_DEV, N_GRP, 8, DIM)
        keys = jnp.transpose(key_cache, (1, 0, 2))
        values = jnp.transpose(value_cache, (1, 0, 2))
        dma = pltpu.SemaphoreType.DMA
        rows_shape = (N_DEV, N_GRP, 8, ROWS_DEV, GROUP, DIM)
        n_rg = N_DEV * N_GRP
        grad_query, grad_keys = pl.pallas_call(
            kernel,
            name='attn_bwd',
            out_shape=(jax.ShapeDtypeStruct((N_SLICES, ROWS_DEV, N_DEV * GROUP, DIM), BF16),
                       jax.ShapeDtypeStruct((2, KEYS_DEV, N_DEV, 1, DIM), F32)),
            in_specs=[any_] * 6,
            out_specs=[any_] * 2,
            scratch_shapes=[
                pltpu.VMEM(rows_shape, BF16), pltpu.VMEM(rows_shape, BF16),
                pltpu.VMEM((n_rg, DIM, RB), BF16), pltpu.VMEM((n_rg, DIM, RB), BF16),
                pltpu.VMEM((N_DEV, N_GRP, 16, DIM), F32), pltpu.VMEM((N_DEV, N_GRP, DIM, DIM), BF16),
                pltpu.VMEM((KEYS, DIM), BF16), pltpu.VMEM((KEYS, DIM), BF16),
                pltpu.VMEM((n_rg, DIM, RB), F32),
                pltpu.VMEM((NKB, DIM, CB), F32), pltpu.VMEM((NKB, DIM, CB), F32),
                pltpu.VMEM((RB, CB), BF16), pltpu.VMEM((RB, CB), BF16),
                pltpu.VMEM((RB, CB), BF16), pltpu.VMEM((RB, CB), BF16),
                pltpu.VMEM((DIM, CB), jnp.int32),
                pltpu.VMEM((N_BUF, 2, CB, DIM), F32),
                pltpu.VMEM((N_DQ, 8, ROWS_DEV, GROUP, DIM), BF16),
                pltpu.VMEM((N_DEV, N_GRP, 8, DIM), F32),
                dma((N_DEV, N_GRP, 4)), dma((N_DEV, 2)), dma((N_DEV, N_GRP, 4)), dma((N_DEV, 2)),
                dma((N_BUF,)), dma((N_DEV,)), dma((N_DQ,)), dma((N_DEV,)),
            ],
            compiler_params=pltpu.CompilerParams(collective_id=0, has_side_effects=True, vmem_limit_bytes=67043328),
        )(queries, grad_out, attn_out, lse, keys, values)
        grad_keys = grad_keys.reshape(2, KEYS_DEV, N_DEV, DIM)
        return grad_query, grad_keys[0], grad_keys[1]

    return jax.shard_map(local_grads, mesh=mesh, in_specs=(row_spec, row_spec, row_spec, stat_spec, key_spec, key_spec),
                         out_specs=(row_spec, key_spec, key_spec), check_vma=False)
```

```python
import functools
import math

import jax
import jax.numpy as jnp
from jax import lax
from jax.experimental import pallas as pl
from jax.experimental.pallas import tpu as pltpu
from jax.sharding import PartitionSpec as P

CP_AXES = ('cpo', 'cp')
MESH = pl.DeviceIdType.MESH
BF16 = jnp.bfloat16
F32 = jnp.float32

N_DEV = 8
N_SLICES = 24
ROWS_DEV = 8
GROUP = 16
DIM = 128
KEYS = 9728
KEYS_DEV = KEYS // N_DEV
PREFIX = 8192
N_GRP = 3
RB = 1024
CB = 512
NKB = KEYS // CB
CHUNK = 64
SCALE = DIM ** -0.5
EXP_SCALE = SCALE * math.log2(math.e)

UNROLL = 6
N_BUF = 3
N_DQ = 12
N_OUTER = 54
AHEAD = 4


def dg(a, b, ca, cb):
    return lax.dot_general(a, b, (((ca,), (cb,)), ((), ())), preferred_element_type=F32)


def quo(a, b):
    return lax.div(a, jnp.int32(b))


def rem(a, b):
    return lax.rem(a, jnp.int32(b))


def pick(cond, a, b):
    return jnp.where(cond, jnp.int32(a), jnp.int32(b))


def xor3(a, b):
    out = jnp.int32(0)
    for bit in (1, 2, 4):
        out = out + bit * rem(rem(quo(a, bit), 2) + rem(quo(b, bit), 2), 2)
    return out


def kernel(q_h, do_h, o_h, l_h, k_h, v_h, dq_o, dkv_o,
           q_v, do_v, qt_v, dot_v, st_v, aug_v, k_v, v_v, dqt, dkt, dvt, p0, d0, p1, d1, x_v, okv, odq, nd_v,
           rows_ss, keys_ss, rows_rs, keys_rs, kv_ss, kv_rs, dq_ss, dq_rs):
    me = lax.axis_index('cpo') * 4 + lax.axis_index('cp')
    chip = quo(me, 2)
    first_kb = 5 * chip
    core = rem(me, 2)
    chips = [chip, quo(xor3(me, 2 + 2 * core), 2), quo(xor3(me, 4 - 2 * core), 2), 3 - chip]

    edge = chip == 3
    edge_at = pick(chips[1] == 3, 1, pick(chips[2] == 3, 2, pick(edge, 0, 3)))
    n_own = 2
    n_units = pick(edge, 15, 13)
    pass_1 = n_own + n_units
    pass_2 = pass_1 + 6
    pass_d = pass_2 + n_units
    pass_3 = pass_d + 2
    pass_b = pass_3 + n_units - 6
    pass_c = pass_b + 4

    def dev(e):
        return {'cpo': quo(e, 4), 'cp': rem(e, 4)}

    barrier = pltpu.get_barrier_semaphore()
    for m in range(1, N_DEV):
        pl.semaphore_signal(barrier, inc=1, device_id=dev(xor3(me, jnp.int32(m))), device_id_type=MESH)

    def zero_keys(i, c):
        dkt[i] = jnp.zeros((DIM, CB), F32)
        dvt[i] = jnp.zeros((DIM, CB), F32)
        return c
    lax.fori_loop(0, NKB, zero_keys, 0)

    def zero_rows(i, c):
        dqt[i] = jnp.zeros((DIM, RB), F32)
        return c
    lax.fori_loop(0, N_DEV * N_GRP, zero_rows, 0)
    p1[...] = jnp.zeros((RB, CB), BF16)
    d1[...] = jnp.zeros((RB, CB), BF16)
    x_v[...] = (lax.broadcasted_iota(jnp.int32, (DIM, CB), 1)
                - lax.broadcasted_iota(jnp.int32, (DIM, CB), 0) // GROUP)

    with jax.named_scope('barrier'):
        pl.semaphore_wait(barrier, N_DEV - 1)

    def row_copies(m, g, local=False):
        e = xor3(me, m)
        heads = pl.ds(pl.multiple_of(e * GROUP, GROUP), GROUP)
        pairs = ((l_h.at[e, g], st_v.at[m, g, pl.ds(0, 8), :], 2),
                 (q_h.at[pl.ds(8 * g, 8), :, heads, :], q_v.at[m, g], 0),
                 (do_h.at[pl.ds(8 * g, 8), :, heads, :], do_v.at[m, g], 1))
        for src, dst, t in pairs:
            if local:
                yield pltpu.make_async_copy(src, dst, rows_rs.at[m, g, t])
            else:
                yield pltpu.make_async_remote_copy(src, dst, rows_ss.at[m, g, t], rows_rs.at[m, g, t],
                                                   device_id=dev(e), device_id_type=MESH)

    def key_copies(e, m, local=False):
        rows = pl.ds(pl.multiple_of(me * KEYS_DEV, CHUNK), KEYS_DEV)
        for src, dst, t in ((k_h.at[e], k_v.at[rows, :], 0), (v_h.at[e], v_v.at[rows, :], 1)):
            if local:
                yield pltpu.make_async_copy(src, dst, keys_rs.at[m, t])
            else:
                yield pltpu.make_async_remote_copy(src, dst, keys_ss.at[m, t], keys_rs.at[m, t],
                                                   device_id=dev(e), device_id_type=MESH)

    for c in key_copies(me, jnp.int32(0), local=True):
        c.start()
    for c in key_copies(xor3(me, jnp.int32(1)), jnp.int32(1)):
        c.start()
    for g in range(N_GRP):
        for m in (0, 1):
            for c in row_copies(jnp.int32(m), g, m == 0):
                c.start()
    turns = [jnp.where(core == 0, jnp.int32(a), jnp.int32(b)) for a, b in ((2, 4), (5, 3), (3, 5), (4, 2), (6, 7), (7, 6))]

    def send_keys(ms):
        for m in ms:
            for c in key_copies(xor3(me, m), m):
                c.start()

    def send_rows(ms):
        for g in range(N_GRP):
            for m in ms:
                for c in row_copies(m, g):
                    c.start()

    send_keys(turns[:4])

    def block_copies(c):
        e = xor3(me, quo(c, N_GRP))
        src = (pl.ds(pl.multiple_of(8 * rem(c, N_GRP), 8), 8), slice(None), pl.ds(pl.multiple_of(e * GROUP, GROUP), GROUP), slice(None))
        for t, ref in ((0, o_h), (6, do_h)):
            slot = rem(c, 6) + t
            yield pltpu.make_async_copy(ref.at[src], odq.at[slot], dq_ss.at[slot])

    def delta(step, carry):
        for c in (2 * step, 2 * step + 1):
            @pl.when(c + AHEAD < N_DEV * N_GRP)
            def _():
                for copy in block_copies(c + AHEAD):
                    copy.start()
        for c in (2 * step, 2 * step + 1):
            for copy in block_copies(c):
                copy.wait()
        row = lax.broadcasted_iota(jnp.int32, (16, 2 * DIM), 0)
        for c in (2 * step, 2 * step + 1):
            x = odq[rem(c, 6)].reshape(RB, DIM).astype(F32) * odq[rem(c, 6) + 6].reshape(RB, DIM).astype(F32)
            hi = x.astype(BF16)
            lo = (x - hi.astype(F32)).astype(BF16)
            acc = None
            for i in range(8):
                one = jnp.where(row == i, 1.0, 0.0).astype(BF16)
                part = dg(one, jnp.concatenate([hi[DIM * i:DIM * i + DIM], lo[DIM * i:DIM * i + DIM]], axis=1), 1, 1)
                acc = part if acc is None else part + acc
            nd_v[quo(c, N_GRP), rem(c, N_GRP)] = 0.0 - acc[:8]
        return carry

    for c in range(AHEAD):
        for copy in block_copies(jnp.int32(c)):
            copy.start()
    with jax.named_scope('delta'):
        lax.fori_loop(0, N_DEV * N_GRP // 2, delta, 0)
    for g in range(N_GRP):
        st_v[0, g, 8:16, :] = nd_v[0, g]
    for m in range(1, N_DEV):
        for g in range(N_GRP):
            pltpu.make_async_remote_copy(nd_v.at[m, g], st_v.at[m, g, pl.ds(8, 8), :], rows_ss.at[m, g, 3], rows_rs.at[m, g, 3],
                                         device_id=dev(xor3(me, jnp.int32(m))), device_id_type=MESH).start()

    def keys_t(ref, kb):
        return jnp.concatenate([ref[pl.ds(pl.multiple_of(kb * CB + DIM * i, DIM), DIM), :] for i in range(CB // DIM)], axis=1)

    def tile(kb, m, g, kb_p, rg_p, bufs, diagonal=False, diagonal_p=False, fill=False):
        p_ref, d_ref, pp_ref, dp_ref = bufs
        slice_of = lax.broadcasted_iota(jnp.int32, (DIM, DIM), 1) % 8
        part_row = lax.broadcasted_iota(jnp.int32, (DIM, CB), 0)
        pick_l = jnp.where(part_row < 24, 1.0, 0.0).astype(BF16)
        pick_d = jnp.where((part_row >= 24) & (part_row < 48), 1.0, 0.0).astype(BF16)
        rhs_s = jnp.concatenate([keys_t(k_v, kb), pick_l], axis=0)
        rhs_d = jnp.concatenate([keys_t(v_v, kb), pick_d], axis=0)
        stats = aug_v[m, g]

        def width(rc):
            return 256 if diagonal and rc < 2 else CB

        def lhs(ref, rc):
            zero = jnp.zeros((), BF16)
            aug = jnp.concatenate([jnp.where(slice_of == 2 * rc, stats, zero),
                                   jnp.where(slice_of == 2 * rc + 1, stats, zero)], axis=0)
            return jnp.concatenate([ref[m, g, pl.ds(2 * rc, 2)].reshape(256, DIM), aug], axis=1)

        def score(rc):
            return dg(lhs(q_v, rc), rhs_s[:, :width(rc)], 1, 0)

        def grad(rc):
            return dg(lhs(do_v, rc), rhs_d[:, :width(rc)], 1, 0)

        def finish(rc, s, dp):
            w = width(rc)
            p = jnp.exp2(s * EXP_SCALE)
            if diagonal:
                limit = ROWS_DEV * xor3(me, m)
                p = jnp.concatenate([jnp.where(x_v[:, :w] <= limit + 64 * (2 * rc), p[:DIM], 0.0),
                                     jnp.where(x_v[:, :w] <= limit + 64 * (2 * rc + 1), p[DIM:], 0.0)], axis=0)
            rows = slice(256 * rc, 256 * rc + 256)
            p_ref[rows, :w] = p.astype(BF16)
            d_ref[rows, :w] = (p * dp).astype(BF16)
            if fill and w < CB:
                p_ref[rows, w:] = jnp.zeros((256, CB - w), BF16)
                d_ref[rows, w:] = jnp.zeros((256, CB - w), BF16)

        def dq_half(h, k):
            cols = slice(256 * k, 256 * k + 256)
            return dg(keys_t(k_v, kb_p)[:, cols], dp_ref[512 * h:512 * h + 512, cols], 1, 1)

        def part(ref, x_ref, i, w=CB):
            return dg(ref[rg_p][:, 256 * i:256 * i + 256], x_ref[256 * i:256 * i + 256, :w], 1, 0)

        def put_dq(h, x):
            dqt[rg_p, :, 512 * h:512 * h + 512] = x + dqt[rg_p, :, 512 * h:512 * h + 512]

        def put_keys(ref, low, full):
            if low is None:
                ref[kb_p] = full + ref[kb_p]
            else:
                ref[kb_p, :, :256] = low + full[:, :256] + ref[kb_p, :, :256]
                ref[kb_p, :, 256:] = full[:, 256:] + ref[kb_p, :, 256:]

        def keys_sum(ref, x_ref):
            if diagonal_p:
                low = part(ref, x_ref, 0, 256)
                yield None
                low = part(ref, x_ref, 1, 256) + low
                yield None
                full = part(ref, x_ref, 2)
                yield None
                yield low, part(ref, x_ref, 3) + full
            else:
                full = part(ref, x_ref, 0)
                for i in (1, 2):
                    yield None
                    full = part(ref, x_ref, i) + full
                yield None
                yield None, part(ref, x_ref, 3) + full

        s = score(0)
        dq = dq_half(0, 0)
        dp = grad(0)
        finish(0, s, dp)
        put_dq(0, dq if diagonal_p else dq_half(0, 1) + dq)
        s = score(1)
        dv = keys_sum(dot_v, pp_ref)
        next(dv)
        next(dv)
        dp = grad(1)
        finish(1, s, dp)
        next(dv)
        put_keys(dvt, *next(dv))
        s = score(2)
        dq = dq_half(1, 0)
        dp = grad(2)
        finish(2, s, dp)
        put_dq(1, dq_half(1, 1) + dq)
        s = score(3)
        dk = keys_sum(qt_v, dp_ref)
        next(dk)
        next(dk)
        dp = grad(3)
        finish(3, s, dp)
        next(dk)
        put_keys(dkt, *next(dk))

    def flush(kb_p, rg_p):
        dvt[kb_p] += dg(dot_v[rg_p], p1[...], 1, 0)
        dkt[kb_p] += dg(qt_v[rg_p], d1[...], 1, 0)
        dqt[rg_p] += dg(keys_t(k_v, kb_p), d1[...], 1, 1)

    def wait_local(ref, sem):
        pltpu.make_async_copy(ref, ref, sem).wait()

    def wait_rows(m, g):
        wait_local(st_v.at[m, g, pl.ds(0, 8), :], rows_rs.at[m, g, 2])
        wait_local(q_v.at[m, g], rows_rs.at[m, g, 0])
        wait_local(do_v.at[m, g], rows_rs.at[m, g, 1])

        @pl.when(m != 0)
        def _():
            wait_local(st_v.at[m, g, pl.ds(8, 8), :], rows_rs.at[m, g, 3])

    def prepare_rows(m, g):
        rg = m * N_GRP + g
        x = st_v[m, g]
        hi = x.astype(BF16).astype(F32)
        mid = (x - hi).astype(BF16).astype(F32)
        lo = (x - hi) - mid
        parts = [y[8 * t:8 * t + 8] for t in (0, 1) for y in (hi, mid, lo)]
        aug_v[m, g] = jnp.concatenate(parts + [jnp.zeros((80, DIM), F32)], axis=0).T.astype(BF16)
        qt_v[rg] = q_v[m, g].reshape(RB, DIM).T
        dot_v[rg] = do_v[m, g].reshape(RB, DIM).T

    def wait_keys(k):
        with jax.named_scope('w_keys'):
            for side in (0, 1):
                e = 2 * k + side
                m = xor3(me, e)
                rows = pl.ds(pl.multiple_of(e * KEYS_DEV, CHUNK), KEYS_DEV)
                wait_local(k_v.at[rows, :], keys_rs.at[m, 0])
                wait_local(v_v.at[rows, :], keys_rs.at[m, 1])

    def prepare_keys(kb):
        blocks = [(ref, pl.ds(pl.multiple_of(kb * CB + DIM * i, DIM), DIM)) for ref in (k_v, v_v) for i in range(CB // DIM)]
        turned = [ref[rows, :].T for ref, rows in blocks]
        for (ref, rows), x in zip(blocks, turned):
            ref[rows, :] = x

    def stage_dq(m, g, slot):
        with jax.named_scope('s_dq'):
            odq[slot] = (dqt[m * N_GRP + g].T * SCALE).astype(BF16).reshape(8, ROWS_DEV, GROUP, DIM)

    def send_dq(m, g, slot):
        e = xor3(me, m)
        dst = dq_o.at[pl.ds(pl.multiple_of(8 * g, 8), 8), :, pl.ds(pl.multiple_of(me * GROUP, GROUP), GROUP), :]

        @pl.when(m == 0)
        def _():
            pltpu.make_async_copy(odq.at[slot], dst, dq_ss.at[slot]).start()

        @pl.when(m != 0)
        def _():
            pltpu.make_async_remote_copy(odq.at[slot], dst, dq_ss.at[slot], dq_rs.at[m],
                                         device_id=dev(e), device_id_type=MESH).start()

    def stage_kv(kb, buf):
        with jax.named_scope('s_kv'):
            okv[buf, 0] = dkt[kb].T * SCALE
            okv[buf, 1] = dvt[kb].T

    def send_kv(kb, buf):
        n_dev = KEYS_DEV // CHUNK
        e_lo = quo(8 * kb, n_dev)

        def piece(j, c):
            ck = 8 * kb + j
            over = ck >= n_dev * (e_lo + 1)
            e = jnp.where(over, e_lo + 1, e_lo)
            off = pl.multiple_of(CHUNK * (ck - n_dev * e), CHUNK)
            m = xor3(me, e)
            src = okv.at[buf, :, pl.ds(pl.multiple_of(CHUNK * j, CHUNK), CHUNK), :]
            dst = dkv_o.at[:, pl.ds(off, CHUNK), me, 0, :]

            @pl.when(m == 0)
            def _():
                pltpu.make_async_copy(src, dst, kv_ss.at[buf]).start()

            @pl.when(m != 0)
            def _():
                pltpu.make_async_remote_copy(src, dst, kv_ss.at[buf], kv_rs.at[m],
                                             device_id=dev(e), device_id_type=MESH).start()
            return c
        lax.fori_loop(0, CB // CHUNK, piece, 0)

    def wait_kv(buf):
        with jax.named_scope('w_kv'):
            wait_local(okv.at[buf], kv_ss.at[buf])

    def wait_dq(slot):
        with jax.named_scope('w_dq'):
            wait_local(odq.at[slot], dq_ss.at[slot])

    def between(o, lo, hi):
        return (o >= lo) & (o < hi)

    def chip_at(d):
        return jnp.where(d == 0, chips[0], jnp.where(d == 1, chips[1], jnp.where(d == 2, chips[2], chips[3])))

    from_2 = pick(edge_at == 1, 2, 4)
    from_3 = from_2 + pick(edge_at == 2, 2, 4)
    from_4 = from_3 + pick(edge_at == 3, 2, 4)

    def block_0(o):
        j = o - n_own
        d = pick(j >= from_3, 3, pick(j >= from_2, 2, 1))
        i = j - jnp.where(j >= from_3, from_3, jnp.where(j >= from_2, from_2, 0))
        kb = jnp.where(j >= from_4, 5 * (j - from_4) + 4, 5 * chip_at(d) + i)
        return jnp.where(j < 0, first_kb + o, kb)

    def unit(n):
        rest = jnp.maximum(n - 6, 0)
        one = pick(edge_at == 1, 2, 1)
        two = pick(edge_at == 3, 2, 3)
        turn = edge | (n < 6)
        d = jnp.where(turn, 1 + rem(n, 3), jnp.where(rem(rest, 2) == 0, one, two))
        i = jnp.where(turn, quo(n, 3), 2 + quo(rest, 2))
        n_whole = n_units - 3
        return jnp.where(n >= n_whole, 5 * (n - n_whole) + 4, 5 * chip_at(d) + i)

    def rows_d(r):
        return 6 + rem(r, 2), quo(r, 2)

    def rows_b(r):
        return 2 + 2 * rem(r + core, 2) + quo(rem(r, 4), 2), quo(r, 4)

    def rows_at(o, r):
        d_m, d_g = rows_d(r)
        b_m, b_g = rows_b(r)
        return jnp.where(o < pass_b, d_m, b_m), jnp.where(o < pass_b, d_g, b_g)

    def done_dq(o, act):
        @pl.when(o >= pass_d)
        def _():
            in_d = o <= pass_3
            it = jnp.where(in_d, o - pass_d, o - pass_b)

            def complete(i):
                fast = jnp.where(in_d, 4 + i, jnp.where(i < 2, 5 + 3 * i, jnp.where(i == 2, 9, 11 + i - 3)))
                n = jnp.where(edge, fast, 3 * i + 2)
                return jnp.where(i < 0, 0, jnp.minimum(n, pick(in_d, 6, 12)))

            def one(r, c):
                d_m, d_g = rows_d(r)
                b_m, b_g = rows_b(r)
                act(jnp.where(in_d, d_m, b_m), jnp.where(in_d, d_g, b_g), r + pick(in_d, 0, 6))
                return c
            lax.fori_loop(complete(it - 1), complete(it), one, 0)

    def done_kv(o, act):
        i = o - pass_2 - 1
        late = jnp.logical_not(edge) & ((i == 8) | (i == 11))
        own = o == pass_c

        @pl.when(((i >= 0) & (i < 6)) | late | between(o, pass_3 + 1, pass_b + 1) | own)
        def _():
            kb = jnp.where(late, pick(i == 8, 17, 18), unit(jnp.where(i < 6, jnp.clip(i, 0, 5), jnp.clip(o - pass_3 + 5, 6, n_units - 1))))
            ev = jnp.where(late, pick(i == 8, 6, 7), jnp.where(i < 6, i, pick(edge, 6, 8) + o - pass_3 - 1))
            act(jnp.where(own, first_kb, kb), jnp.where(own, 15, ev))

    def put_kv(kb, ev):
        @pl.when(ev >= N_BUF)
        def _():
            wait_kv(rem(ev, N_BUF))
        stage_kv(kb, rem(ev, N_BUF))

    def put_dq(m, g, slot):
        wait_dq(slot)
        stage_dq(m, g, slot)

    def outer(o, carry):
        ends = between(o, pass_d, pass_3) | between(o, pass_b, pass_c)
        last = o >= pass_c
        n = jnp.where(o < pass_2, o - pass_1, jnp.where(o < pass_d, o - pass_2, o - pass_3 + 6))
        kb = jnp.where(o < pass_1, block_0(o), unit(jnp.clip(n, 0, n_units - 1)))
        cut = kb == 16
        m_lo = pick((o < pass_1) | last, 0, pick(between(o, pass_2, pass_d), 6, 2))
        n_m = pick((o < pass_1) | between(o, pass_2, pass_d) | last, 2, 4)
        it = jnp.where(o < pass_b, o - pass_d, o - pass_b)
        w = pick(o < pass_b, 2, 4)
        n_six = jnp.where(ends, pick(edge, 1, 2), jnp.where(last, pick((o < pass_c + 2) & jnp.logical_not(edge), 1, 0), quo(n_m, 2)))
        n_diag = jnp.where(ends, pick(edge & (it < quo(w, 2)), 1, 0), jnp.where(last, pick(edge & (o == pass_c), 1, 0), jnp.where(cut & (o != 1), quo(n_m, 2), 0)))
        first = (o == 0) | (o == pass_1) | (o == pass_2)

        done_dq(o - 1, lambda m, g, ev: send_dq(m, g, rem(ev, N_DQ)))
        done_kv(o - 1, lambda k, ev: send_kv(k, rem(ev, N_BUF)))

        @pl.when(o < pass_1)
        def _():
            @pl.when(o == 0)
            def _():
                wait_keys(chip)
                for i in (1, 2, 3):
                    prepare_keys(first_kb + i)

            @pl.when(o == 2)
            def _():
                send_keys(turns[4:])
                send_rows(turns[:4])

            @pl.when(o == 12)
            def _():
                send_rows(turns[4:])
            j = o - n_own

            @pl.when((j == 0) | (j == from_2) | (j == from_3))
            def _():
                wait_keys(chip_at(pick(j == from_3, 3, pick(j == from_2, 2, 1))))

            @pl.when((o == 0) | (j >= 0))
            def _():
                prepare_keys(kb)

            @pl.when(cut & (j >= 0))
            def _():
                prepare_keys(kb + 1)
                prepare_keys(kb + 2)

        def index(n):
            f = lax.div(n, n_m)
            k = jnp.where(cut, pick(f == 2, 17, 16), kb)
            m = m_lo + lax.rem(n, n_m)
            g = jnp.where(cut, pick(f == 0, 1, 2), f)
            e_r = 3 * it + quo(n, 4)
            e_k = first_kb + rem(n, 4)
            e = 6 * it + n
            e_a = jnp.maximum(e - w, 0)
            e_b = jnp.maximum(e - 3 * w, 0)
            x_r = jnp.where(e < w, e, jnp.where(e < 3 * w, w + quo(e_a, 2), 2 * w + quo(e_b, 3)))
            x_k = 15 + jnp.where(e < w, 0, jnp.where(e < 3 * w, rem(e_a, 2), rem(e_b, 3)))
            e_m, e_g = rows_at(o, jnp.where(edge, x_r, e_r))
            own = n + 6 * (o - pass_c)
            k = jnp.where(ends, jnp.where(edge, x_k, e_k), jnp.where(last, first_kb + 2 + rem(n, 2), k))
            m = jnp.where(ends, e_m, jnp.where(last, rem(quo(own, 2), 2), m))
            g = jnp.where(ends, e_g, jnp.where(last, quo(own, 4), g))
            return k, m, g

        def index_diag(n):
            e_m, e_g = rows_at(o, 6 * it + n)
            g = jnp.where(ends, e_g, lax.div(n, n_m))
            m = jnp.where(ends, e_m, m_lo + lax.rem(n, n_m))
            return 16 + g, m, g

        def six(fresh, diagonal, j, c):
            if fresh:
                def one(t, c):
                    _, m, g = index(UNROLL * j + t)
                    wait_rows(m, g)
                    return c
                with jax.named_scope('w_rows'):
                    lax.fori_loop(0, UNROLL, one, 0)
            kb_p, rg_p = c
            for t in range(UNROLL):
                k, m, g = (index_diag if diagonal else index)(UNROLL * j + t)
                if fresh:
                    prepare_rows(m, g)
                bufs = (p0, d0, p1, d1) if t % 2 == 0 else (p1, d1, p0, d0)
                tile(k, m, g, kb_p, rg_p, bufs, diagonal, diagonal and t > 0, diagonal and t == UNROLL - 1)
                kb_p, rg_p = k, m * N_GRP + g
            return kb_p, rg_p

        with jax.named_scope('tiles'):
            carry = lax.fori_loop(0, jnp.where(first, n_six, 0), functools.partial(six, True, False), carry)
            carry = lax.fori_loop(0, jnp.where(first, 0, n_six), functools.partial(six, False, False), carry)
            carry = lax.fori_loop(0, n_diag, functools.partial(six, False, True), carry)

        done_kv(o, put_kv)

        def put(m, g, ev):
            @pl.when(ev >= N_DQ)
            def _():
                wait_dq(rem(ev, N_DQ))
            stage_dq(m, g, rem(ev, N_DQ))
        done_dq(o, put)
        return carry

    kb_p, rg_p = lax.fori_loop(0, N_OUTER, outer, (first_kb, jnp.int32(0)))
    done_dq(jnp.int32(N_OUTER - 1), lambda m, g, ev: send_dq(m, g, rem(ev, N_DQ)))
    done_kv(jnp.int32(N_OUTER - 1), lambda k, ev: send_kv(k, rem(ev, N_BUF)))
    with jax.named_scope('flush'):
        flush(kb_p, rg_p)

    own = [(jnp.int32(m), jnp.int32(g), (18 + 3 * (1 - m) + g) % N_DQ) for m in (1, 0) for g in range(N_GRP)]
    for r, (m, g, slot) in enumerate(own):
        if r < 3:
            put_kv(first_kb + 1 + r, jnp.int32(16 + r))
        put_dq(m, g, slot)
        if r < 3:
            send_kv(first_kb + 1 + r, (16 + r) % N_BUF)
        if r > 0:
            send_dq(*own[r - 1])
    send_dq(*own[-1])

    for slot in range(N_DQ):
        wait_dq(slot)
    for buf in range(N_BUF):
        wait_kv(buf)
    with jax.named_scope('drain'):
        for m in range(1, N_DEV):
            for g in range(N_GRP):
                wait_local(st_v.at[m, g, pl.ds(0, 8), :], rows_ss.at[m, g, 2])
                wait_local(nd_v.at[m, g], rows_ss.at[m, g, 3])
                wait_local(q_v.at[m, g], rows_ss.at[m, g, 0])
                wait_local(do_v.at[m, g], rows_ss.at[m, g, 1])
            wait_local(k_v.at[pl.ds(0, KEYS_DEV), :], keys_ss.at[m, 0])
            wait_local(v_v.at[pl.ds(0, KEYS_DEV), :], keys_ss.at[m, 1])
            heads = pl.ds(0, GROUP)
            wait_local(dq_o.at[:, :, heads, :], dq_rs.at[m])
            wait_local(dkv_o.at[:, :, 0, 0, :], kv_rs.at[m])


def solution(mesh):
    row_spec = P(None, CP_AXES, 'heads', None)
    stat_spec = P(None, CP_AXES, 'heads')
    key_spec = P(CP_AXES, 'heads', None)
    any_ = pl.BlockSpec(memory_space=pl.ANY)

    def local_grads(queries, attn_out, grad_out, log_sum_exp, key_cache, value_cache):
        lse = (log_sum_exp * (-1.0 / SCALE)).reshape(N_GRP, 8, ROWS_DEV, N_DEV, GROUP)
        lse = jnp.transpose(lse, (3, 0, 1, 2, 4)).reshape(N_DEV, N_GRP, 8, DIM)
        keys = jnp.transpose(key_cache, (1, 0, 2))
        values = jnp.transpose(value_cache, (1, 0, 2))
        dma = pltpu.SemaphoreType.DMA
        rows_shape = (N_DEV, N_GRP, 8, ROWS_DEV, GROUP, DIM)
        n_rg = N_DEV * N_GRP
        grad_query, grad_keys = pl.pallas_call(
            kernel,
            name='attn_bwd',
            out_shape=(jax.ShapeDtypeStruct((N_SLICES, ROWS_DEV, N_DEV * GROUP, DIM), BF16),
                       jax.ShapeDtypeStruct((2, KEYS_DEV, N_DEV, 1, DIM), F32)),
            in_specs=[any_] * 6,
            out_specs=[any_] * 2,
            scratch_shapes=[
                pltpu.VMEM(rows_shape, BF16), pltpu.VMEM(rows_shape, BF16),
                pltpu.VMEM((n_rg, DIM, RB), BF16), pltpu.VMEM((n_rg, DIM, RB), BF16),
                pltpu.VMEM((N_DEV, N_GRP, 16, DIM), F32), pltpu.VMEM((N_DEV, N_GRP, DIM, DIM), BF16),
                pltpu.VMEM((KEYS, DIM), BF16), pltpu.VMEM((KEYS, DIM), BF16),
                pltpu.VMEM((n_rg, DIM, RB), F32),
                pltpu.VMEM((NKB, DIM, CB), F32), pltpu.VMEM((NKB, DIM, CB), F32),
                pltpu.VMEM((RB, CB), BF16), pltpu.VMEM((RB, CB), BF16),
                pltpu.VMEM((RB, CB), BF16), pltpu.VMEM((RB, CB), BF16),
                pltpu.VMEM((DIM, CB), jnp.int32),
                pltpu.VMEM((N_BUF, 2, CB, DIM), F32),
                pltpu.VMEM((N_DQ, 8, ROWS_DEV, GROUP, DIM), BF16),
                pltpu.VMEM((N_DEV, N_GRP, 8, DIM), F32),
                dma((N_DEV, N_GRP, 4)), dma((N_DEV, 2)), dma((N_DEV, N_GRP, 4)), dma((N_DEV, 2)),
                dma((N_BUF,)), dma((N_DEV,)), dma((N_DQ,)), dma((N_DEV,)),
            ],
            compiler_params=pltpu.CompilerParams(collective_id=0, has_side_effects=True, vmem_limit_bytes=67043328),
        )(queries, grad_out, attn_out, lse, keys, values)
        grad_keys = grad_keys.reshape(2, KEYS_DEV, N_DEV, DIM)
        return grad_query, grad_keys[0], grad_keys[1]

    return jax.shard_map(local_grads, mesh=mesh, in_specs=(row_spec, row_spec, row_spec, stat_spec, key_spec, key_spec),
                         out_specs=(row_spec, key_spec, key_spec), check_vma=False)
```

```python
import functools
import math

import jax
import jax.numpy as jnp
from jax import lax
from jax.experimental import pallas as pl
from jax.experimental.pallas import tpu as pltpu
from jax.sharding import PartitionSpec as P

CP_AXES = ('cpo', 'cp')
MESH = pl.DeviceIdType.MESH
BF16 = jnp.bfloat16
F32 = jnp.float32

N_DEV = 8
N_SLICES = 24
ROWS_DEV = 8
GROUP = 16
DIM = 128
KEYS = 9728
KEYS_DEV = KEYS // N_DEV
PREFIX = 8192
N_GRP = 3
RB = 1024
CB = 512
NKB = KEYS // CB
CHUNK = 64
SCALE = DIM ** -0.5
EXP_SCALE = SCALE * math.log2(math.e)

UNROLL = 6
N_BUF = 3
N_DQ = 12
N_OUTER = 54
AHEAD = 4


def dg(a, b, ca, cb):
    return lax.dot_general(a, b, (((ca,), (cb,)), ((), ())), preferred_element_type=F32)


def quo(a, b):
    return lax.div(a, jnp.int32(b))


def rem(a, b):
    return lax.rem(a, jnp.int32(b))


def pick(cond, a, b):
    return jnp.where(cond, jnp.int32(a), jnp.int32(b))


def xor3(a, b):
    out = jnp.int32(0)
    for bit in (1, 2, 4):
        out = out + bit * rem(rem(quo(a, bit), 2) + rem(quo(b, bit), 2), 2)
    return out


def kernel(q_h, do_h, o_h, l_h, k_h, v_h, dq_o, dkv_o,
           q_v, do_v, qt_v, dot_v, st_v, aug_v, k_v, v_v, dqt, dkt, dvt, p0, d0, p1, d1, x_v, okv, odq, nd_v,
           rows_ss, keys_ss, rows_rs, keys_rs, kv_ss, kv_rs, dq_ss, dq_rs):
    me = lax.axis_index('cpo') * 4 + lax.axis_index('cp')
    chip = quo(me, 2)
    first_kb = 5 * chip
    core = rem(me, 2)
    chips = [chip, quo(xor3(me, 2 + 2 * core), 2), quo(xor3(me, 4 - 2 * core), 2), 3 - chip]

    edge = chip == 3
    edge_at = pick(chips[1] == 3, 1, pick(chips[2] == 3, 2, pick(edge, 0, 3)))
    n_own = pick(edge, 2, 3)
    n_units = pick(edge, 15, 13)
    pass_1 = n_own + n_units
    pass_2 = pass_1 + 6
    pass_d = pass_2 + n_units
    pass_3 = pass_d + 2
    pass_b = pass_3 + n_units - 6
    pass_c = pass_b + 4

    def dev(e):
        return {'cpo': quo(e, 4), 'cp': rem(e, 4)}

    barrier = pltpu.get_barrier_semaphore()
    for m in range(1, N_DEV):
        pl.semaphore_signal(barrier, inc=1, device_id=dev(xor3(me, jnp.int32(m))), device_id_type=MESH)

    def zero_keys(i, c):
        dkt[i] = jnp.zeros((DIM, CB), F32)
        dvt[i] = jnp.zeros((DIM, CB), F32)
        return c
    lax.fori_loop(0, NKB, zero_keys, 0)

    def zero_rows(i, c):
        dqt[i] = jnp.zeros((DIM, RB), F32)
        return c
    lax.fori_loop(0, N_DEV * N_GRP, zero_rows, 0)
    p1[...] = jnp.zeros((RB, CB), BF16)
    d1[...] = jnp.zeros((RB, CB), BF16)
    x_v[...] = (lax.broadcasted_iota(jnp.int32, (DIM, CB), 1)
                - lax.broadcasted_iota(jnp.int32, (DIM, CB), 0) // GROUP)

    with jax.named_scope('barrier'):
        pl.semaphore_wait(barrier, N_DEV - 1)

    def row_copies(m, g, local=False):
        e = xor3(me, m)
        pairs = ((l_h.at[e, g], st_v.at[m, g, pl.ds(0, 8), :], 2),
                 (q_h.at[pl.ds(8 * g, 8), :, e], q_v.at[m, g], 0),
                 (do_h.at[pl.ds(8 * g, 8), :, e], do_v.at[m, g], 1))
        for src, dst, t in pairs:
            if local:
                yield pltpu.make_async_copy(src, dst, rows_rs.at[m, g, t])
            else:
                yield pltpu.make_async_remote_copy(src, dst, rows_ss.at[m, g, t], rows_rs.at[m, g, t],
                                                   device_id=dev(e), device_id_type=MESH)

    def key_copies(e, m, local=False):
        rows = pl.ds(pl.multiple_of(me * KEYS_DEV, CHUNK), KEYS_DEV)
        for src, dst, t in ((k_h.at[e], k_v.at[rows, :], 0), (v_h.at[e], v_v.at[rows, :], 1)):
            if local:
                yield pltpu.make_async_copy(src, dst, keys_rs.at[m, t])
            else:
                yield pltpu.make_async_remote_copy(src, dst, keys_ss.at[m, t], keys_rs.at[m, t],
                                                   device_id=dev(e), device_id_type=MESH)

    for c in key_copies(me, jnp.int32(0), local=True):
        c.start()
    for c in key_copies(xor3(me, jnp.int32(1)), jnp.int32(1)):
        c.start()
    for g in range(N_GRP):
        for m in (0, 1):
            for c in row_copies(jnp.int32(m), g, m == 0):
                c.start()
    turns = [jnp.where(core == 0, jnp.int32(a), jnp.int32(b)) for a, b in ((2, 4), (5, 3), (3, 5), (4, 2), (6, 7), (7, 6))]

    def send_keys(ms):
        for m in ms:
            for c in key_copies(xor3(me, m), m):
                c.start()

    def send_rows(ms, g):
        for m in ms:
            for c in row_copies(m, g):
                c.start()

    send_keys(turns[:4])

    def slice_copies(j):
        for t, ref in ((0, o_h), (6, do_h)):
            slot = rem(j, 6) + t
            yield pltpu.make_async_copy(ref.at[j], odq.at[slot], dq_ss.at[slot])

    def delta(step, carry):
        for j in (2 * step, 2 * step + 1):
            @pl.when(j + AHEAD < N_SLICES)
            def _():
                for copy in slice_copies(j + AHEAD):
                    copy.start()
        for j in (2 * step, 2 * step + 1):
            for copy in slice_copies(j):
                copy.wait()
        row = lax.broadcasted_iota(jnp.int32, (16, 2 * DIM), 0)
        for j in (2 * step, 2 * step + 1):
            x = odq[rem(j, 6)].astype(F32) * odq[rem(j, 6) + 6].astype(F32)
            hi = x.astype(BF16)
            lo = (x - hi.astype(F32)).astype(BF16)
            acc = None
            for e in range(N_DEV):
                one = jnp.where(row == e, 1.0, 0.0).astype(BF16)
                both = jnp.concatenate([hi[:, e].reshape(DIM, DIM), lo[:, e].reshape(DIM, DIM)], axis=1)
                part = dg(one, both, 1, 1)
                acc = part if acc is None else part + acc
            for e in range(N_DEV):
                nd_v[e, quo(j, 8), pl.ds(rem(j, 8), 1), :] = 0.0 - acc[e:e + 1]
        return carry

    for j in range(AHEAD):
        for copy in slice_copies(jnp.int32(j)):
            copy.start()
    with jax.named_scope('delta'):
        lax.fori_loop(0, N_SLICES // 2, delta, 0)
    for g in range(N_GRP):
        st_v[0, g, 8:16, :] = nd_v[me, g]
    for m in range(1, N_DEV):
        for g in range(N_GRP):
            e = xor3(me, jnp.int32(m))
            pltpu.make_async_remote_copy(nd_v.at[e, g], st_v.at[m, g, pl.ds(8, 8), :], rows_ss.at[m, g, 3], rows_rs.at[m, g, 3],
                                         device_id=dev(e), device_id_type=MESH).start()

    def keys_t(ref, kb):
        return jnp.concatenate([ref[pl.ds(pl.multiple_of(kb * CB + DIM * i, DIM), DIM), :] for i in range(CB // DIM)], axis=1)

    def tile(kb, m, g, kb_p, rg_p, bufs, diagonal=False, diagonal_p=False, fill=False):
        p_ref, d_ref, pp_ref, dp_ref = bufs
        slice_of = lax.broadcasted_iota(jnp.int32, (DIM, DIM), 1) % 8
        part_row = lax.broadcasted_iota(jnp.int32, (DIM, CB), 0)
        pick_l = jnp.where(part_row < 24, 1.0, 0.0).astype(BF16)
        pick_d = jnp.where((part_row >= 24) & (part_row < 48), 1.0, 0.0).astype(BF16)
        rhs_s = jnp.concatenate([keys_t(k_v, kb), pick_l], axis=0)
        rhs_d = jnp.concatenate([keys_t(v_v, kb), pick_d], axis=0)
        stats = aug_v[m, g]

        def width(rc):
            return 256 if diagonal and rc < 2 else CB

        def lhs(ref, rc):
            zero = jnp.zeros((), BF16)
            aug = jnp.concatenate([jnp.where(slice_of == 2 * rc, stats, zero),
                                   jnp.where(slice_of == 2 * rc + 1, stats, zero)], axis=0)
            return jnp.concatenate([ref[m, g, pl.ds(2 * rc, 2)].reshape(256, DIM), aug], axis=1)

        def score(rc):
            return dg(lhs(q_v, rc), rhs_s[:, :width(rc)], 1, 0)

        def grad(rc):
            return dg(lhs(do_v, rc), rhs_d[:, :width(rc)], 1, 0)

        def finish(rc, s, dp):
            w = width(rc)
            p = jnp.exp2(s * EXP_SCALE)
            if diagonal:
                limit = ROWS_DEV * xor3(me, m)
                p = jnp.concatenate([jnp.where(x_v[:, :w] <= limit + 64 * (2 * rc), p[:DIM], 0.0),
                                     jnp.where(x_v[:, :w] <= limit + 64 * (2 * rc + 1), p[DIM:], 0.0)], axis=0)
            rows = slice(256 * rc, 256 * rc + 256)
            p_ref[rows, :w] = p.astype(BF16)
            d_ref[rows, :w] = (p * dp).astype(BF16)
            if fill and w < CB:
                p_ref[rows, w:] = jnp.zeros((256, CB - w), BF16)
                d_ref[rows, w:] = jnp.zeros((256, CB - w), BF16)

        def dq_half(h, k):
            cols = slice(256 * k, 256 * k + 256)
            return dg(keys_t(k_v, kb_p)[:, cols], dp_ref[512 * h:512 * h + 512, cols], 1, 1)

        def part(ref, x_ref, i, w=CB):
            return dg(ref[rg_p][:, 256 * i:256 * i + 256], x_ref[256 * i:256 * i + 256, :w], 1, 0)

        def put_dq(h, x):
            dqt[rg_p, :, 512 * h:512 * h + 512] = x + dqt[rg_p, :, 512 * h:512 * h + 512]

        def put_keys(ref, low, full):
            if low is None:
                ref[kb_p] = full + ref[kb_p]
            else:
                ref[kb_p, :, :256] = low + full[:, :256] + ref[kb_p, :, :256]
                ref[kb_p, :, 256:] = full[:, 256:] + ref[kb_p, :, 256:]

        def keys_sum(ref, x_ref):
            if diagonal_p:
                low = part(ref, x_ref, 0, 256)
                yield None
                low = part(ref, x_ref, 1, 256) + low
                yield None
                full = part(ref, x_ref, 2)
                yield None
                yield low, part(ref, x_ref, 3) + full
            else:
                full = part(ref, x_ref, 0)
                for i in (1, 2):
                    yield None
                    full = part(ref, x_ref, i) + full
                yield None
                yield None, part(ref, x_ref, 3) + full

        s = score(0)
        dq = dq_half(0, 0)
        dp = grad(0)
        finish(0, s, dp)
        put_dq(0, dq if diagonal_p else dq_half(0, 1) + dq)
        s = score(1)
        dv = keys_sum(dot_v, pp_ref)
        next(dv)
        next(dv)
        dp = grad(1)
        finish(1, s, dp)
        next(dv)
        put_keys(dvt, *next(dv))
        s = score(2)
        dq = dq_half(1, 0)
        dp = grad(2)
        finish(2, s, dp)
        put_dq(1, dq_half(1, 1) + dq)
        s = score(3)
        dk = keys_sum(qt_v, dp_ref)
        next(dk)
        next(dk)
        dp = grad(3)
        finish(3, s, dp)
        next(dk)
        put_keys(dkt, *next(dk))

    def flush(kb_p, rg_p):
        dvt[kb_p] += dg(dot_v[rg_p], p1[...], 1, 0)
        dkt[kb_p] += dg(qt_v[rg_p], d1[...], 1, 0)
        dqt[rg_p] += dg(keys_t(k_v, kb_p), d1[...], 1, 1)

    def wait_local(ref, sem):
        pltpu.make_async_copy(ref, ref, sem).wait()

    def wait_rows(m, g):
        wait_local(st_v.at[m, g, pl.ds(0, 8), :], rows_rs.at[m, g, 2])
        wait_local(q_v.at[m, g], rows_rs.at[m, g, 0])
        wait_local(do_v.at[m, g], rows_rs.at[m, g, 1])

        @pl.when(m != 0)
        def _():
            wait_local(st_v.at[m, g, pl.ds(8, 8), :], rows_rs.at[m, g, 3])

    def prepare_rows(m, g):
        rg = m * N_GRP + g
        x = jnp.concatenate([st_v[m, g, 0:8] * (-1.0 / SCALE), st_v[m, g, 8:16]], axis=0)
        hi = x.astype(BF16).astype(F32)
        mid = (x - hi).astype(BF16).astype(F32)
        lo = (x - hi) - mid
        parts = [y[8 * t:8 * t + 8] for t in (0, 1) for y in (hi, mid, lo)]
        aug_v[m, g] = jnp.concatenate(parts + [jnp.zeros((80, DIM), F32)], axis=0).T.astype(BF16)
        qt_v[rg] = q_v[m, g].reshape(RB, DIM).T
        dot_v[rg] = do_v[m, g].reshape(RB, DIM).T

    def wait_keys(k):
        with jax.named_scope('w_keys'):
            for side in (0, 1):
                e = 2 * k + side
                m = xor3(me, e)
                rows = pl.ds(pl.multiple_of(e * KEYS_DEV, CHUNK), KEYS_DEV)
                wait_local(k_v.at[rows, :], keys_rs.at[m, 0])
                wait_local(v_v.at[rows, :], keys_rs.at[m, 1])

    def prepare_keys(kb):
        blocks = [(ref, pl.ds(pl.multiple_of(kb * CB + DIM * i, DIM), DIM)) for ref in (k_v, v_v) for i in range(CB // DIM)]
        turned = [ref[rows, :].T for ref, rows in blocks]
        for (ref, rows), x in zip(blocks, turned):
            ref[rows, :] = x

    def stage_dq(m, g, slot):
        with jax.named_scope('s_dq'):
            odq[slot] = (dqt[m * N_GRP + g].T * SCALE).astype(BF16).reshape(8, ROWS_DEV, GROUP, DIM)

    def send_dq(m, g, slot):
        e = xor3(me, m)
        dst = dq_o.at[pl.ds(pl.multiple_of(8 * g, 8), 8), :, pl.ds(pl.multiple_of(me * GROUP, GROUP), GROUP), :]

        @pl.when(m == 0)
        def _():
            pltpu.make_async_copy(odq.at[slot], dst, dq_ss.at[slot]).start()

        @pl.when(m != 0)
        def _():
            pltpu.make_async_remote_copy(odq.at[slot], dst, dq_ss.at[slot], dq_rs.at[m],
                                         device_id=dev(e), device_id_type=MESH).start()

    def stage_kv(kb, buf):
        with jax.named_scope('s_kv'):
            okv[buf, 0] = dkt[kb].T * SCALE
            okv[buf, 1] = dvt[kb].T

    def send_kv(kb, buf):
        n_dev = KEYS_DEV // CHUNK
        e_lo = quo(8 * kb, n_dev)
        whole = 8 * kb + 8 <= n_dev * (e_lo + 1)

        def send(j, n, e):
            off = pl.multiple_of(CHUNK * (8 * kb + j - n_dev * e), CHUNK)
            m = xor3(me, e)
            src = okv.at[buf, :, pl.ds(pl.multiple_of(CHUNK * j, CHUNK), n), :]
            dst = dkv_o.at[:, pl.ds(off, n), me, 0, :]

            @pl.when(m == 0)
            def _():
                pltpu.make_async_copy(src, dst, kv_ss.at[buf]).start()

            @pl.when(m != 0)
            def _():
                pltpu.make_async_remote_copy(src, dst, kv_ss.at[buf], kv_rs.at[m],
                                             device_id=dev(e), device_id_type=MESH).start()

        def piece(j, c):
            send(j, CHUNK, jnp.where(8 * kb + j >= n_dev * (e_lo + 1), e_lo + 1, e_lo))
            return c

        @pl.when(whole)
        def _():
            send(0, CB, e_lo)

        @pl.when(jnp.logical_not(whole))
        def _():
            lax.fori_loop(0, CB // CHUNK, piece, 0)

    def wait_kv(buf):
        with jax.named_scope('w_kv'):
            wait_local(okv.at[buf], kv_ss.at[buf])

    def wait_dq(slot):
        with jax.named_scope('w_dq'):
            wait_local(odq.at[slot], dq_ss.at[slot])

    def between(o, lo, hi):
        return (o >= lo) & (o < hi)

    def chip_at(d):
        return jnp.where(d == 0, chips[0], jnp.where(d == 1, chips[1], jnp.where(d == 2, chips[2], chips[3])))

    from_2 = pick(edge_at == 1, 2, 4)
    from_3 = from_2 + pick(edge_at == 2, 2, 4)
    from_4 = from_3 + pick(edge_at == 3, 2, 4)

    def block_0(o):
        j = o - n_own
        d = pick(j >= from_3, 3, pick(j >= from_2, 2, 1))
        i = j - jnp.where(j >= from_3, from_3, jnp.where(j >= from_2, from_2, 0))
        kb = jnp.where(j >= from_4, 5 * (j - from_4) + 4, 5 * chip_at(d) + i)
        return jnp.where(j < 0, first_kb + o, kb)

    def unit(n):
        rest = jnp.maximum(n - 6, 0)
        one = pick(edge_at == 1, 2, 1)
        two = pick(edge_at == 3, 2, 3)
        turn = edge | (n < 6)
        d = jnp.where(turn, 1 + rem(n, 3), jnp.where(rem(rest, 2) == 0, one, two))
        i = jnp.where(turn, quo(n, 3), 2 + quo(rest, 2))
        n_whole = n_units - 3
        return jnp.where(n >= n_whole, 5 * (n - n_whole) + 4, 5 * chip_at(d) + i)

    def rows_d(r):
        return 6 + rem(r, 2), quo(r, 2)

    def rows_b(r):
        return 2 + 2 * rem(r + core, 2) + quo(rem(r, 4), 2), quo(r, 4)

    def rows_at(o, r):
        d_m, d_g = rows_d(r)
        b_m, b_g = rows_b(r)
        return jnp.where(o < pass_b, d_m, b_m), jnp.where(o < pass_b, d_g, b_g)

    def done_dq(o, act):
        @pl.when(o >= pass_d)
        def _():
            in_d = o <= pass_3
            it = jnp.where(in_d, o - pass_d, o - pass_b)

            def complete(i):
                fast = jnp.where(in_d, 4 + i, jnp.where(i < 2, 5 + 3 * i, jnp.where(i == 2, 9, 11 + i - 3)))
                n = jnp.where(edge, fast, 3 * i + 2)
                return jnp.where(i < 0, 0, jnp.minimum(n, pick(in_d, 6, 12)))

            def one(r, c):
                d_m, d_g = rows_d(r)
                b_m, b_g = rows_b(r)
                act(jnp.where(in_d, d_m, b_m), jnp.where(in_d, d_g, b_g), r + pick(in_d, 0, 6))
                return c
            lax.fori_loop(complete(it - 1), complete(it), one, 0)

    def done_kv(o, act):
        i = o - pass_2 - 1
        late = jnp.logical_not(edge) & ((i == 8) | (i == 11))
        own = o == pass_c

        @pl.when(((i >= 0) & (i < 6)) | late | between(o, pass_3 + 1, pass_b + 1) | own)
        def _():
            kb = jnp.where(late, pick(i == 8, 17, 18), unit(jnp.where(i < 6, jnp.clip(i, 0, 5), jnp.clip(o - pass_3 + 5, 6, n_units - 1))))
            ev = jnp.where(late, pick(i == 8, 6, 7), jnp.where(i < 6, i, pick(edge, 6, 8) + o - pass_3 - 1))
            act(jnp.where(own, first_kb, kb), jnp.where(own, 15, ev))

    def put_kv(kb, ev):
        @pl.when(ev >= N_BUF)
        def _():
            wait_kv(rem(ev, N_BUF))
        stage_kv(kb, rem(ev, N_BUF))

    def put_dq(m, g, slot):
        wait_dq(slot)
        stage_dq(m, g, slot)

    def outer(o, carry):
        ends = between(o, pass_d, pass_3) | between(o, pass_b, pass_c)
        last = o >= pass_c
        n = jnp.where(o < pass_2, o - pass_1, jnp.where(o < pass_d, o - pass_2, o - pass_3 + 6))
        kb = jnp.where(o < pass_1, block_0(o), unit(jnp.clip(n, 0, n_units - 1)))
        cut = kb == 16
        m_lo = pick((o < pass_1) | last, 0, pick(between(o, pass_2, pass_d), 6, 2))
        n_m = pick((o < pass_1) | between(o, pass_2, pass_d) | last, 2, 4)
        it = jnp.where(o < pass_b, o - pass_d, o - pass_b)
        w = pick(o < pass_b, 2, 4)
        n_six = jnp.where(ends, pick(edge, 1, 2), jnp.where(last, pick((o == pass_c) & jnp.logical_not(edge), 1, 0), quo(n_m, 2)))
        n_diag = jnp.where(ends, pick(edge & (it < quo(w, 2)), 1, 0), jnp.where(last, pick(edge & (o == pass_c), 1, 0), jnp.where(cut & (o != 1), quo(n_m, 2), 0)))
        first = (o == 0) | (o == pass_1) | (o == pass_2)

        done_dq(o - 1, lambda m, g, ev: send_dq(m, g, rem(ev, N_DQ)))
        done_kv(o - 1, lambda k, ev: send_kv(k, rem(ev, N_BUF)))

        @pl.when(o < pass_1)
        def _():
            @pl.when(o == 0)
            def _():
                wait_keys(chip)
                for i in (1, 2, 3):
                    prepare_keys(first_kb + i)

            @pl.when(o == 2)
            def _():
                send_keys(turns[4:])

            for g in range(N_GRP):
                @pl.when(o == (4, 8, 11)[g])
                def _():
                    send_rows(turns[:4], g)

            @pl.when(o == 14)
            def _():
                for g in range(N_GRP):
                    send_rows(turns[4:], g)
            j = o - n_own

            @pl.when((j == 0) | (j == from_2) | (j == from_3))
            def _():
                wait_keys(chip_at(pick(j == from_3, 3, pick(j == from_2, 2, 1))))

            @pl.when((o == 0) | (j >= 0))
            def _():
                prepare_keys(kb)

            @pl.when(cut & (j >= 0))
            def _():
                prepare_keys(kb + 1)
                prepare_keys(kb + 2)

        def index(n):
            f = lax.div(n, n_m)
            hit = cut & jnp.logical_not(last)
            k = jnp.where(hit, pick(f == 2, 17, 16), kb)
            m = m_lo + lax.rem(n, n_m)
            g = jnp.where(hit, pick(f == 0, 1, 2), f)
            e_r = 3 * it + quo(n, 4)
            e_k = first_kb + rem(n, 4)
            e = 6 * it + n
            e_a = jnp.maximum(e - w, 0)
            e_b = jnp.maximum(e - 3 * w, 0)
            x_r = jnp.where(e < w, e, jnp.where(e < 3 * w, w + quo(e_a, 2), 2 * w + quo(e_b, 3)))
            x_k = 15 + jnp.where(e < w, 0, jnp.where(e < 3 * w, rem(e_a, 2), rem(e_b, 3)))
            e_m, e_g = rows_at(o, jnp.where(edge, x_r, e_r))
            k = jnp.where(ends, jnp.where(edge, x_k, e_k), jnp.where(last, first_kb + 3, k))
            m = jnp.where(ends, e_m, m)
            g = jnp.where(ends, e_g, g)
            return k, m, g

        def index_diag(n):
            e_m, e_g = rows_at(o, 6 * it + n)
            g = jnp.where(ends, e_g, lax.div(n, n_m))
            m = jnp.where(ends, e_m, m_lo + lax.rem(n, n_m))
            return 16 + g, m, g

        def six(fresh, diagonal, j, c):
            if fresh:
                def one(t, c):
                    _, m, g = index(UNROLL * j + t)
                    wait_rows(m, g)
                    return c
                with jax.named_scope('w_rows'):
                    lax.fori_loop(0, UNROLL, one, 0)
            kb_p, rg_p = c
            for t in range(UNROLL):
                k, m, g = (index_diag if diagonal else index)(UNROLL * j + t)
                if fresh:
                    prepare_rows(m, g)
                bufs = (p0, d0, p1, d1) if t % 2 == 0 else (p1, d1, p0, d0)
                tile(k, m, g, kb_p, rg_p, bufs, diagonal, diagonal and t > 0, diagonal and t == UNROLL - 1)
                kb_p, rg_p = k, m * N_GRP + g
            return kb_p, rg_p

        with jax.named_scope('tiles'):
            carry = lax.fori_loop(0, jnp.where(first, n_six, 0), functools.partial(six, True, False), carry)
            carry = lax.fori_loop(0, jnp.where(first, 0, n_six), functools.partial(six, False, False), carry)
            carry = lax.fori_loop(0, n_diag, functools.partial(six, False, True), carry)

        done_kv(o, put_kv)

        def put(m, g, ev):
            @pl.when(ev >= N_DQ)
            def _():
                wait_dq(rem(ev, N_DQ))
            stage_dq(m, g, rem(ev, N_DQ))
        done_dq(o, put)
        return carry

    kb_p, rg_p = lax.fori_loop(0, N_OUTER, outer, (first_kb, jnp.int32(0)))
    done_dq(jnp.int32(N_OUTER - 1), lambda m, g, ev: send_dq(m, g, rem(ev, N_DQ)))
    done_kv(jnp.int32(N_OUTER - 1), lambda k, ev: send_kv(k, rem(ev, N_BUF)))
    with jax.named_scope('flush'):
        flush(kb_p, rg_p)

    own = [(jnp.int32(m), jnp.int32(g), (18 + 3 * (1 - m) + g) % N_DQ) for m in (1, 0) for g in range(N_GRP)]
    for r, (m, g, slot) in enumerate(own):
        if r < 3:
            put_kv(first_kb + 1 + r, jnp.int32(16 + r))
        put_dq(m, g, slot)
        if r < 3:
            send_kv(first_kb + 1 + r, (16 + r) % N_BUF)
        if r > 0:
            send_dq(*own[r - 1])
    send_dq(*own[-1])

    for slot in range(N_DQ):
        wait_dq(slot)
    for buf in range(N_BUF):
        wait_kv(buf)
    with jax.named_scope('drain'):
        for m in range(1, N_DEV):
            for g in range(N_GRP):
                wait_local(st_v.at[m, g, pl.ds(0, 8), :], rows_ss.at[m, g, 2])
                wait_local(nd_v.at[m, g], rows_ss.at[m, g, 3])
                wait_local(q_v.at[m, g], rows_ss.at[m, g, 0])
                wait_local(do_v.at[m, g], rows_ss.at[m, g, 1])
            wait_local(k_v.at[pl.ds(0, KEYS_DEV), :], keys_ss.at[m, 0])
            wait_local(v_v.at[pl.ds(0, KEYS_DEV), :], keys_ss.at[m, 1])
            heads = pl.ds(0, GROUP)
            wait_local(dq_o.at[:, :, heads, :], dq_rs.at[m])
            wait_local(dkv_o.at[:, :, 0, 0, :], kv_rs.at[m])


def solution(mesh):
    row_spec = P(None, CP_AXES, 'heads', None)
    stat_spec = P(None, CP_AXES, 'heads')
    key_spec = P(CP_AXES, 'heads', None)
    any_ = pl.BlockSpec(memory_space=pl.ANY)

    def local_grads(queries, attn_out, grad_out, log_sum_exp, key_cache, value_cache):
        lse = log_sum_exp.reshape(N_GRP, 8, ROWS_DEV, N_DEV, GROUP)
        lse = jnp.transpose(lse, (3, 0, 1, 2, 4)).reshape(N_DEV, N_GRP, 8, DIM)
        keys = jnp.transpose(key_cache, (1, 0, 2))
        values = jnp.transpose(value_cache, (1, 0, 2))
        dma = pltpu.SemaphoreType.DMA
        rows_shape = (N_DEV, N_GRP, 8, ROWS_DEV, GROUP, DIM)
        n_rg = N_DEV * N_GRP
        grad_query, grad_keys = pl.pallas_call(
            kernel,
            name='attn_bwd',
            out_shape=(jax.ShapeDtypeStruct((N_SLICES, ROWS_DEV, N_DEV * GROUP, DIM), BF16),
                       jax.ShapeDtypeStruct((2, KEYS_DEV, N_DEV, 1, DIM), F32)),
            in_specs=[any_] * 6,
            out_specs=[any_] * 2,
            scratch_shapes=[
                pltpu.VMEM(rows_shape, BF16), pltpu.VMEM(rows_shape, BF16),
                pltpu.VMEM((n_rg, DIM, RB), BF16), pltpu.VMEM((n_rg, DIM, RB), BF16),
                pltpu.VMEM((N_DEV, N_GRP, 16, DIM), F32), pltpu.VMEM((N_DEV, N_GRP, DIM, DIM), BF16),
                pltpu.VMEM((KEYS, DIM), BF16), pltpu.VMEM((KEYS, DIM), BF16),
                pltpu.VMEM((n_rg, DIM, RB), F32),
                pltpu.VMEM((NKB, DIM, CB), F32), pltpu.VMEM((NKB, DIM, CB), F32),
                pltpu.VMEM((RB, CB), BF16), pltpu.VMEM((RB, CB), BF16),
                pltpu.VMEM((RB, CB), BF16), pltpu.VMEM((RB, CB), BF16),
                pltpu.VMEM((DIM, CB), jnp.int32),
                pltpu.VMEM((N_BUF, 2, CB, DIM), F32),
                pltpu.VMEM((N_DQ, 8, ROWS_DEV, GROUP, DIM), BF16),
                pltpu.VMEM((N_DEV, N_GRP, 8, DIM), F32),
                dma((N_DEV, N_GRP, 4)), dma((N_DEV, 2)), dma((N_DEV, N_GRP, 4)), dma((N_DEV, 2)),
                dma((N_BUF,)), dma((N_DEV,)), dma((N_DQ,)), dma((N_DEV,)),
            ],
            compiler_params=pltpu.CompilerParams(collective_id=0, has_side_effects=True, vmem_limit_bytes=67043328),
        )(*(x.reshape(N_SLICES, ROWS_DEV, N_DEV, GROUP, DIM) for x in (queries, grad_out, attn_out)), lse, keys, values)
        grad_keys = grad_keys.reshape(2, KEYS_DEV, N_DEV, DIM)
        return grad_query, grad_keys[0], grad_keys[1]

    return jax.shard_map(local_grads, mesh=mesh, in_specs=(row_spec, row_spec, row_spec, stat_spec, key_spec, key_spec),
                         out_specs=(row_spec, key_spec, key_spec), check_vma=False)
```
